32 devices in a mesh: dp: 8 (over z, core), seq: 4 (over y, x).
Axes of the slice: x: 2, y: 2, z: 4, core: 2. Of those that a mesh axis runs over, the one named last changes fastest.
Arguments:
- frames: bfloat16 [8192, 1024], P(('dp', 'seq')), may hold values from -6 to 6
- out_grad: bfloat16 [8192, 1024], P(('dp', 'seq')), may hold values from -6 to 6
- time_emb: float32 [24, 1024], P('dp'), may hold values from -6 to 6
- clip_len: int32 [8, 3], P('dp'), may hold values from 1 to 512, 1024 in all within a row
- pad_len: int32 [8, 3], P('dp'), may hold values from 0 to 127
- w_qkv: float32 [3, 1024, 1024], P(None, 'seq'), may hold values from -0.21875 to 0.21875
- mom_qkv: float32 [3, 1024, 1024], P(None, 'seq'), may hold values from -28 to 28
- var_qkv: float32 [3, 1024, 1024], P(None, 'seq'), may hold values from 0.8192 to 24.576
- w_out: float32 [1024, 1024], P('seq'), may hold values from -0.875 to 0.875
- mom_out: float32 [1024, 1024], P('seq'), may hold values from -28 to 28
- var_out: float32 [1024, 1024], P('seq'), may hold values from 0.8192 to 24.576
- w_up: float32 [1024, 2048], P('seq'), may hold values from -0.21875 to 0.21875
- mom_up: float32 [1024, 2048], P('seq'), may hold values from -28 to 28
- var_up: float32 [1024, 2048], P('seq'), may hold values from 0.8192 to 24.576
- w_down: float32 [2048, 1024], P('seq'), may hold values from -0.15467961 to 0.15467961
- mom_down: float32 [2048, 1024], P('seq'), may hold values from -28 to 28
- var_down: float32 [2048, 1024], P('seq'), may hold values from 0.8192 to 24.576
- w_mod: float32 [1024, 6144], P('seq'), may hold values from -0.21875 to 0.21875
- mom_mod: float32 [1024, 6144], P('seq'), may hold values from -28 to 28
- var_mod: float32 [1024, 6144], P('seq'), may hold values from 0.8192 to 24.576
- b_mod: float32 [6144], P('seq'), may hold values from -3.5 to 3.5
- mom_bias: float32 [6144], P('seq'), may hold values from -28 to 28
- var_bias: float32 [6144], P('seq'), may hold values from 0.8192 to 24.576
Outputs:
- output: bfloat16 [8192, 1024], P(('dp', 'seq'))
- input_grad: float32 [8192, 1024], P(('dp', 'seq'))
- time_grad: float32 [24, 1024], P('dp')
- grad_qkv: float32 [3, 1024, 1024], P(None, 'seq')
- master_qkv: float32 [3, 1024, 1024], P(None, 'seq')
- moment_qkv: float32 [3, 1024, 1024], P(None, 'seq')
- second_qkv: float32 [3, 1024, 1024], P(None, 'seq')
- grad_out: float32 [1024, 1024], P('seq')
- master_out: float32 [1024, 1024], P('seq')
- moment_out: float32 [1024, 1024], P('seq')
- second_out: float32 [1024, 1024], P('seq')
- grad_up: float32 [1024, 2048], P('seq')
- master_up: float32 [1024, 2048], P('seq')
- moment_up: float32 [1024, 2048], P('seq')
- second_up: float32 [1024, 2048], P('seq')
- grad_down: float32 [2048, 1024], P('seq')
- master_down: float32 [2048, 1024], P('seq')
- moment_down: float32 [2048, 1024], P('seq')
- second_down: float32 [2048, 1024], P('seq')
- grad_mod: float32 [1024, 6144], P('seq')
- master_mod: float32 [1024, 6144], P('seq')
- moment_mod: float32 [1024, 6144], P('seq')
- second_mod: float32 [1024, 6144], P('seq')
- grad_bias: float32 [6144], P('seq')
- master_bias: float32 [6144], P('seq')
- moment_bias: float32 [6144], P('seq')
- second_bias: float32 [6144], P('seq')
The draws below stay inside these ranges and needn't reach their ends.
Inputs may be any that keep to these rules, and one draw needn't show every extreme that they name: `clip_len`: row g lists the lengths of the 3 clips of data group g in frame order; each row sums to 1024, and the longest clip of every row has exactly 512 frames.
All inputs are finite; a program needn't handle non-finite values.
Results may differ from the reference program's by a relative error of at most 0.03.
The reference program's roundings to bfloat16 on the way count: a program that leaves them out, or rounds other values in their place, can miss the bound.
Values may be sent and summed in bfloat16 or wider, within the bound.
A program may use at most 256 MiB of HBM per device.

```python
import math
import jax
import jax.numpy as jnp
import numpy as np
from jax import lax

D = 1024
HEADS = 16
HEAD_DIM = 64
FF = 2048
GROUP = 1024
TOKENS = 8192
MAXLEN = 512
CLIPS = 3
CLIPS_ALL = 24
N_DP = 8


def rising_rows(key, shape, row_axis, scale_base):
    rows = shape[row_axis]
    position = jnp.arange(rows, dtype=jnp.float32) / max(rows - 1, 1)
    row_scale = jnp.power(jnp.float32(3.0), position) / 1.8
    view = [1] * len(shape)
    view[row_axis] = rows
    row_scale = row_scale.reshape(view)
    values = jax.random.truncated_normal(key, -4.0, 4.0, shape, jnp.float32)
    return (values * row_scale * scale_base).astype(jnp.float32)


def draw_w_qkv(key, part):
    return rising_rows(jax.random.fold_in(key, 101), (3, D, D), 1, D ** (-0.5))


def draw_w_out(key, part):
    return rising_rows(jax.random.fold_in(key, 102), (D, D), 0, (D // 16) ** (-0.5))


def draw_w_up(key, part):
    return rising_rows(jax.random.fold_in(key, 103), (D, FF), 0, D ** (-0.5))


def draw_w_down(key, part):
    return rising_rows(jax.random.fold_in(key, 104), (FF, D), 0, FF ** (-0.5))


def draw_w_mod(key, part):
    return rising_rows(jax.random.fold_in(key, 105), (D, 6 * D), 0, D ** (-0.5))


def draw_b_mod(key, part):
    return rising_rows(jax.random.fold_in(key, 106), (6 * D,), 0, 0.5)


def plant(entries, stream_key, least, top_value):
    longest = entries.shape.index(max(entries.shape))
    spots = []
    for shift in (0, 1):
        where = [jax.random.randint(jax.random.fold_in(stream_key, axis), (), 0, length) for axis, length in enumerate(entries.shape)]
        where[longest] = (where[longest] + shift) % entries.shape[longest]
        spots.append(tuple(where))
    return entries.at[spots[0]].set(least).at[spots[1]].set(top_value)


def shard_levels(key, extent, cuts, least, largest):
    factor_of, own = 1.0, jax.random.fold_in(key, 6)
    for dim, blocks in cuts:
        draws = jnp.exp(jax.random.uniform(jax.random.fold_in(own, dim), (blocks,), jnp.float32, least / len(cuts), largest / len(cuts)))
        factor_of = factor_of * jnp.repeat(draws, extent[dim] // blocks).reshape([-1 if axis == dim else 1 for axis in range(len(extent))])
    return factor_of


def length_profile(amount, total, reach, skew):
    loads = [(1 << 20) // math.isqrt(grade ** skew) + 1 for grade in range(2, amount + 1)]
    spare, given = total - reach - (amount - 1), [1] * (amount - 1)
    while spare > 0:
        free = [i for i in range(amount - 1) if given[i] < reach]
        whole, budget = sum([loads[i] for i in free]), spare
        for i in free:
            more = min(reach - given[i], max(1, budget * loads[i] // whole), spare)
            given[i] = given[i] + more
            spare = spare - more
    return np.array([reach] + given)


def ragged_sizes(own_key, count, total, bound, lean):
    if count == 2:
        one = jax.random.randint(own_key, (), max(1, total - bound), min(bound, total - 1) + 1)
        return jnp.stack([one, total - one])
    sizes = jnp.asarray(length_profile(count, total, bound, lean), jnp.int32)
    twos = (count - 1) // 2
    source_of, sink = sizes[1:1 + 2 * twos:2], sizes[2:2 + 2 * twos:2]
    room = jnp.minimum(source_of - 1, bound - sink)
    shifted = jax.random.randint(jax.random.fold_in(own_key, 1), (twos,), 0, 1 << 20) % (room + 1)
    sizes = sizes.at[1:1 + 2 * twos:2].set(source_of - shifted).at[2:2 + 2 * twos:2].set(sink + shifted)
    return sizes[jax.random.permutation(jax.random.fold_in(own_key, 2), count)]


def normal_values(own_key, dims, scale, reach, cuts=(), kind=jnp.bfloat16):
    gain = shard_levels(own_key, dims, cuts, -0.22, 0.18) if cuts else 1.0
    values = jax.random.normal(own_key, dims, jnp.float32) * scale * gain
    return jnp.minimum(jnp.maximum(values, -reach), reach).astype(kind)


def setup_inputs(seed: int = 0) -> dict:
    splits = jax.random.split(jax.random.key(seed), 24)
    return {
        "frames": normal_values(splits[0], (TOKENS, D), 1.0, 6.0, ((0, 32),)),
        "out_grad": normal_values(splits[1], (TOKENS, D), 1.0, 6.0, ((0, 32),)),
        "time_emb": normal_values(splits[2], (CLIPS_ALL, D), 1.0, 6.0, ((0, 8),), jnp.float32),
        "clip_len": jax.vmap(lambda own: ragged_sizes(own, CLIPS, GROUP, MAXLEN, 2))(jax.random.split(splits[3], N_DP)).reshape((N_DP, CLIPS)).astype(jnp.int32),
        "pad_len": plant(jax.random.randint(splits[4], (N_DP, CLIPS), 0, MAXLEN // 4), jax.random.fold_in(splits[4], 1), 0, (MAXLEN // 4) - 1).astype(jnp.int32),
        "w_qkv": draw_w_qkv(jax.random.fold_in(splits[23], 71), 0),
        "mom_qkv": normal_values(splits[6], (3, D, D), (0.05 * TOKENS ** 0.5), 28.0, ((1, 4),), jnp.float32),
        "var_qkv": jnp.clip(jnp.exp(math.log(24.576) - 3.4011974 * jax.random.uniform(splits[7], (3, D, D), jnp.float32) ** shard_levels(splits[7], (3, D, D), ((1, 4),), -0.2, 0.2)), 0.8192, 24.576),
        "w_out": draw_w_out(jax.random.fold_in(splits[23], 71), 0),
        "mom_out": normal_values(splits[9], (D, D), (0.05 * TOKENS ** 0.5), 28.0, ((0, 4),), jnp.float32),
        "var_out": jnp.clip(jnp.exp(math.log(24.576) - 3.4011974 * jax.random.uniform(splits[10], (D, D), jnp.float32) ** shard_levels(splits[10], (D, D), ((0, 4),), -0.2, 0.2)), 0.8192, 24.576),
        "w_up": draw_w_up(jax.random.fold_in(splits[23], 71), 0),
        "mom_up": normal_values(splits[12], (D, FF), (0.05 * TOKENS ** 0.5), 28.0, ((0, 4),), jnp.float32),
        "var_up": jnp.clip(jnp.exp(math.log(24.576) - 3.4011974 * jax.random.uniform(splits[13], (D, FF), jnp.float32) ** shard_levels(splits[13], (D, FF), ((0, 4),), -0.2, 0.2)), 0.8192, 24.576),
        "w_down": draw_w_down(jax.random.fold_in(splits[23], 71), 0),
        "mom_down": normal_values(splits[15], (FF, D), (0.05 * TOKENS ** 0.5), 28.0, ((0, 4),), jnp.float32),
        "var_down": jnp.clip(jnp.exp(math.log(24.576) - 3.4011974 * jax.random.uniform(splits[16], (FF, D), jnp.float32) ** shard_levels(splits[16], (FF, D), ((0, 4),), -0.2, 0.2)), 0.8192, 24.576),
        "w_mod": draw_w_mod(jax.random.fold_in(splits[23], 71), 0),
        "mom_mod": normal_values(splits[18], (D, 6 * D), (0.05 * TOKENS ** 0.5), 28.0, ((0, 4),), jnp.float32),
        "var_mod": jnp.clip(jnp.exp(math.log(24.576) - 3.4011974 * jax.random.uniform(splits[19], (D, 6 * D), jnp.float32) ** shard_levels(splits[19], (D, 6 * D), ((0, 4),), -0.2, 0.2)), 0.8192, 24.576),
        "b_mod": draw_b_mod(jax.random.fold_in(splits[23], 71), 0),
        "mom_bias": normal_values(splits[21], (6 * D,), (0.05 * TOKENS ** 0.5), 28.0, ((0, 4),), jnp.float32),
        "var_bias": jnp.clip(jnp.exp(math.log(24.576) - 3.4011974 * jax.random.uniform(splits[22], (6 * D,), jnp.float32) ** shard_levels(splits[22], (6 * D,), ((0, 4),), -0.2, 0.2)), 0.8192, 24.576),
    }


@jax.custom_vjp
def low(v):
    return lax.optimization_barrier(v.astype(jnp.bfloat16)).astype(jnp.float32)

@jax.custom_vjp
def low_back(v):
    return v

def low_keep(v):
    return (low(v), None)

def low_pass(kept, grad):
    return (grad,)

def back_keep(v):
    return (v, None)

def back_low(kept, grad):
    return (low(grad),)
low.defvjp(low_keep, low_pass)
low_back.defvjp(back_keep, back_low)
precise = lax.Precision.HIGHEST
norm_eps = 1e-06
masked_score = -1e+30
beta_one = 0.9
beta_two = 0.999
adam_eps = 1e-08
weight_decay = 0.01
step_rate = 1.0
step_count = 10

def layer_norm(values):
    center = values - lax.optimization_barrier(jnp.mean(values, axis=-1, keepdims=True))
    spread = lax.optimization_barrier(jnp.mean(center * center, axis=-1, keepdims=True))
    return center * lax.rsqrt(spread + norm_eps)

def rotate(values, places, turn_sign):
    frame_count = values.shape[0]
    half_dim = HEAD_DIM // 2
    exponent = jnp.arange(half_dim, dtype=jnp.float32) * (-2.0 / HEAD_DIM)
    frequency = jnp.power(jnp.float32(10000.0), exponent)
    angles = places.astype(jnp.float32)[:, None] * frequency[None, :]
    cos_table = jnp.cos(angles)[:, None, :]
    sin_table = turn_sign * jnp.sin(angles)[:, None, :]
    paired = values.reshape(frame_count, values.shape[1] // HEAD_DIM, half_dim, 2)
    even_part = paired[..., 0]
    odd_part = paired[..., 1]
    turned = jnp.stack([even_part * cos_table - odd_part * sin_table, odd_part * cos_table + even_part * sin_table], axis=-1)
    return turned.reshape(frame_count, values.shape[1])

def clip_tables(lengths, padding, frame_ids):
    lengths = lengths.astype(jnp.int32)
    starts = (jnp.cumsum(lengths) - lengths).astype(jnp.int32)
    finish = starts + lengths
    inside = (frame_ids[:, None] >= starts[None, :]) & (frame_ids[:, None] < finish[None, :])
    clip_ids = jnp.arange(lengths.shape[0], dtype=jnp.int32)
    owners = lax.optimization_barrier(jnp.sum(jnp.where(inside, clip_ids[None, :], 0), axis=1)).astype(jnp.int32)
    begins = lax.optimization_barrier(jnp.sum(jnp.where(inside, starts[None, :], 0), axis=1)).astype(jnp.int32)
    kept_len = jnp.maximum(lengths - padding.astype(jnp.int32), 1)
    limits = lax.optimization_barrier(jnp.sum(jnp.where(inside, kept_len[None, :], 0), axis=1)).astype(jnp.int32)
    places = (frame_ids - begins).astype(jnp.int32)
    return (inside.astype(jnp.float32), owners, places, places < limits)

def attention(queries, keys_all, values, owners, usable):
    frame_count = queries.shape[0]
    block_rows = min(512, frame_count)
    blocks = frame_count // block_rows
    score_scale = HEAD_DIM ** (-0.5)
    query_blocks = queries.reshape(blocks, block_rows, HEADS, HEAD_DIM)
    owner_blocks = owners.reshape(blocks, block_rows)
    keys_three = keys_all.reshape(frame_count, HEADS, HEAD_DIM)
    values_three = values.reshape(frame_count, HEADS, HEAD_DIM)

    def one_block(pair):
        query_rows, query_owner = pair
        raw = jnp.einsum('qhd,khd->hqk', query_rows, keys_three, precision=precise) * score_scale
        scores = low_back(raw)
        allowed = (query_owner[:, None] == owners[None, :]) & usable[None, :]
        masked = jnp.where(allowed[None], scores, masked_score)
        row_max = lax.optimization_barrier(jnp.max(masked, axis=-1, keepdims=True))
        expo = jnp.exp(masked - row_max)
        probs_low = low(expo / lax.optimization_barrier(jnp.sum(expo, axis=-1, keepdims=True)))
        return jnp.einsum('hqk,khd->qhd', probs_low, values_three, precision=precise)
    outcome = lax.map(jax.checkpoint(one_block), (query_blocks, owner_blocks))
    return outcome.reshape(frame_count, HEADS * HEAD_DIM)

def group_layer(weights, inputs, times, lengths, padding):
    w_qkv, w_out, w_up, w_down, w_mod, b_mod = [low(weight) for weight in weights]
    frame_count = inputs.shape[0]
    inside, owners, places, usable = clip_tables(lengths, padding, jnp.arange(frame_count, dtype=jnp.int32))
    silu_low = low(jax.nn.silu(times))
    modulation = jnp.dot(silu_low, w_mod, precision=precise) + b_mod
    mod_rows = jnp.dot(inside, modulation, precision=precise)
    shift_attn, scale_attn, gate_attn, shift_ff, scale_ff, gate_ff = jnp.split(mod_rows, 6, axis=1)
    hidden = low(layer_norm(inputs) * (1.0 + scale_attn) + shift_attn)
    query_lin = low_back(jnp.dot(hidden, w_qkv[0], precision=precise))
    key_lin = low_back(jnp.dot(hidden, w_qkv[1], precision=precise))
    value_lin = jnp.dot(hidden, w_qkv[2], precision=precise)
    queries = low(low_back(rotate(query_lin, places, 1.0)))
    keys_all = low(low_back(rotate(key_lin, places, 1.0)))
    values = low(low_back(value_lin))
    attended = low(low_back(attention(queries, keys_all, values, owners, usable)))
    attn_proj = low_back(jnp.dot(attended, w_out, precision=precise))
    mid = inputs + gate_attn * attn_proj
    hidden_ff = low(layer_norm(mid) * (1.0 + scale_ff) + shift_ff)
    pre_act = low_back(jnp.dot(hidden_ff, w_up, precision=precise))
    active = low(jax.nn.gelu(pre_act, approximate=True))
    ff_proj = low_back(jnp.dot(active, w_down, precision=precise))
    return mid + gate_ff * ff_proj

def lamb(weight, moment, second, grad, axes):
    moment_new = beta_one * moment + (1.0 - beta_one) * grad
    second_new = beta_two * second + (1.0 - beta_two) * grad * grad
    corrected = moment_new / (1.0 - beta_one ** step_count)
    scaled = second_new / (1.0 - beta_two ** step_count)
    direction = corrected / (jnp.sqrt(scaled) + adam_eps) + weight_decay * weight
    weight_sq = lax.optimization_barrier(jnp.sum(weight * weight, axis=axes, keepdims=True))
    update_sq = lax.optimization_barrier(jnp.sum(direction * direction, axis=axes, keepdims=True))
    ratio = jnp.sqrt(weight_sq) * lax.rsqrt(update_sq + 1e-06)
    return (weight - step_rate * ratio * direction, moment_new, second_new)

def reference(frames, out_grad, time_emb, clip_len, pad_len, w_qkv, mom_qkv, var_qkv, w_out, mom_out, var_out, w_up, mom_up, var_up, w_down, mom_down, var_down, w_mod, mom_mod, var_mod, b_mod, mom_bias, var_bias):
    masters = (w_qkv, w_out, w_up, w_down, w_mod, b_mod)
    inputs = frames.astype(jnp.float32)

    def forward(weights, rows, times):

        def one_group(unused_carry, group_data):
            rows_group, times_group, lengths, padding = group_data
            return (unused_carry, group_layer(weights, rows_group, times_group, lengths, padding))
        unused_carry, result = lax.scan(one_group, jnp.float32(0.0), (rows.reshape(N_DP, GROUP, D), times.reshape(N_DP, CLIPS, D), clip_len, pad_len))
        return result.reshape(N_DP * GROUP, D)
    result, pullback = jax.vjp(forward, masters, inputs, time_emb)
    grads, input_grad, time_grad = pullback(out_grad.astype(jnp.float32))
    master_qkv, moment_qkv, second_qkv = lamb(w_qkv, mom_qkv, var_qkv, grads[0], (1, 2))
    master_out, moment_out, second_out = lamb(w_out, mom_out, var_out, grads[1], None)
    master_up, moment_up, second_up = lamb(w_up, mom_up, var_up, grads[2], None)
    master_down, moment_down, second_down = lamb(w_down, mom_down, var_down, grads[3], None)
    master_mod, moment_mod, second_mod = lamb(w_mod, mom_mod, var_mod, grads[4], None)
    master_bias, moment_bias, second_bias = lamb(b_mod, mom_bias, var_bias, grads[5], None)
    return (result.astype(jnp.bfloat16), input_grad, time_grad, grads[0], master_qkv, moment_qkv, second_qkv, grads[1], master_out, moment_out, second_out, grads[2], master_up, moment_up, second_up, grads[3], master_down, moment_down, second_down, grads[4], master_mod, moment_mod, second_mod, grads[5], master_bias, moment_bias, second_bias)
```

```python
import jax
import jax.numpy as jnp
from jax import lax
from jax.sharding import PartitionSpec as P

HEAD_DIM = 64


precise = lax.Precision.HIGHEST
norm_eps = 1e-06
masked_score = -1e30
beta_one = 0.9
beta_two = 0.999
adam_eps = 1e-08
weight_decay = 0.01
step_rate = 1.0
step_count = 10


def layer_norm(values):
    center = values - jnp.mean(values, axis=-1, keepdims=True)
    spread = jnp.mean(center * center, axis=-1, keepdims=True)
    return center * lax.rsqrt(spread + norm_eps)


def modulate(values, shift, scale):
    return layer_norm(values) * (1.0 + scale) + shift


def gelu_tanh(values):
    return jax.nn.gelu(values, approximate=True)


def rotate(values, places, turn_sign):
    frame_count = values.shape[0]
    half_dim = HEAD_DIM // 2
    exponent = jnp.arange(half_dim, dtype=jnp.float32) * (-2.0 / HEAD_DIM)
    frequency = jnp.power(jnp.float32(10000.0), exponent)
    angles = places.astype(jnp.float32)[:, None] * frequency[None, :]
    cos_table = jnp.cos(angles)[:, None, :]
    sin_table = turn_sign * jnp.sin(angles)[:, None, :]
    paired = values.reshape(frame_count, values.shape[1] // HEAD_DIM, half_dim, 2)
    even_part = paired[..., 0]
    odd_part = paired[..., 1]
    turned = jnp.stack(
        [
            even_part * cos_table - odd_part * sin_table,
            odd_part * cos_table + even_part * sin_table,
        ],
        axis=-1,
    )
    return turned.reshape(frame_count, values.shape[1])


def clip_tables(lengths, padding, frame_ids):
    starts = jnp.cumsum(lengths) - lengths
    finish = starts + lengths
    inside = (frame_ids[:, None] >= starts[None, :]) & (frame_ids[:, None] < finish[None, :])
    clip_ids = jnp.arange(lengths.shape[0], dtype=jnp.int32)
    owners = jnp.sum(jnp.where(inside, clip_ids[None, :], 0), axis=1)
    begins = jnp.sum(jnp.where(inside, starts[None, :], 0), axis=1)
    kept_len = jnp.maximum(lengths - padding, 1)
    limits = jnp.sum(jnp.where(inside, kept_len[None, :], 0), axis=1)
    places = frame_ids - begins
    return (inside.astype(jnp.float32), owners, places, places < limits)


def key_window(block_index, block_rows, span, frame_count):
    return jnp.clip(block_index * block_rows - (span - block_rows) // 2, 0, frame_count - span)


def block_inputs(queries, keys_all, values, owners, usable, block_index, block_rows, span):
    frame_count, columns = queries.shape
    heads_here = columns // HEAD_DIM
    row_start = block_index * block_rows
    window = key_window(block_index, block_rows, span, frame_count)
    query_rows = lax.dynamic_slice_in_dim(queries, row_start, block_rows, 0).reshape(
        block_rows, heads_here, HEAD_DIM
    )
    keys_win = keys_all.reshape(span, heads_here, HEAD_DIM)
    values_win = values.reshape(span, heads_here, HEAD_DIM)
    query_owner = lax.dynamic_slice_in_dim(owners, row_start, block_rows, 0)
    score_scale = HEAD_DIM ** (-0.5)
    scores = (
        jnp.einsum("qhd,khd->hqk", query_rows, keys_win, preferred_element_type=jnp.float32)
        * score_scale
    )
    allowed = (query_owner[:, None] == owners[None, :]) & usable[None, :]
    masked = jnp.where(allowed[None], scores, masked_score)
    return (row_start, window, query_rows, keys_win, values_win, masked)


def attend_forward(queries, keys_all, values, owners, usable, span):
    frame_count, columns = queries.shape
    block_rows = min(512, frame_count)

    def one_block(block_index):
        row_start, window, query_rows, keys_win, values_win, masked = block_inputs(
            queries, keys_all, values, owners, usable, block_index, block_rows, span
        )
        row_max = jnp.max(masked, axis=-1, keepdims=True)
        row_total = jnp.sum(jnp.exp(masked - row_max), axis=-1, keepdims=True)
        log_total = row_max + jnp.log(row_total)
        probs_low = jnp.exp(masked - log_total).astype(jnp.bfloat16)
        attended = jnp.einsum(
            "hqk,khd->qhd", probs_low, values_win, preferred_element_type=jnp.float32
        )
        return (attended.astype(jnp.bfloat16).reshape(block_rows, columns), log_total)

    outcome, log_totals = lax.map(one_block, jnp.arange(frame_count // block_rows, dtype=jnp.int32))
    return (outcome.reshape(frame_count, columns), log_totals)


def attend_backward(queries, keys_all, values, grad_attended, log_totals, owners, usable, span):
    frame_count, columns = queries.shape
    heads_here = columns // HEAD_DIM
    block_rows = min(512, frame_count)
    score_scale = HEAD_DIM ** (-0.5)

    def one_block(sums, block_data):
        key_sum, value_sum = sums
        block_index, log_total = block_data
        row_start, window, query_rows, keys_win, values_win, masked = block_inputs(
            queries, keys_all, values, owners, usable, block_index, block_rows, span
        )
        grad_rows = lax.dynamic_slice_in_dim(grad_attended, row_start, block_rows, 0).reshape(
            block_rows, heads_here, HEAD_DIM
        )
        probs_full = jnp.exp(masked - log_total)
        probs_low = probs_full.astype(jnp.bfloat16)
        grad_probs = jnp.einsum(
            "qhd,khd->hqk", grad_rows, values_win, preferred_element_type=jnp.float32
        )
        row_delta = jnp.sum(probs_full * grad_probs, axis=-1, keepdims=True)
        grad_scores = (probs_full * (grad_probs - row_delta)).astype(jnp.bfloat16)
        grad_query = (
            jnp.einsum("hqk,khd->qhd", grad_scores, keys_win, preferred_element_type=jnp.float32)
            * score_scale
        )
        grad_key = (
            jnp.einsum("hqk,qhd->khd", grad_scores, query_rows, preferred_element_type=jnp.float32)
            * score_scale
        )
        grad_value = jnp.einsum(
            "hqk,qhd->khd", probs_low, grad_rows, preferred_element_type=jnp.float32
        )
        old_keys = key_sum
        key_sum = old_keys + grad_key.reshape(span, columns)
        old_values = value_sum
        value_sum = old_values + grad_value.reshape(span, columns)
        return ((key_sum, value_sum), grad_query.astype(jnp.bfloat16).reshape(block_rows, columns))

    zeros = jnp.zeros((frame_count, columns), jnp.float32)
    indices = jnp.arange(frame_count // block_rows, dtype=jnp.int32)
    (key_sum, value_sum), grad_queries = lax.scan(one_block, (zeros, zeros), (indices, log_totals))
    return (
        grad_queries.reshape(frame_count, columns),
        key_sum.astype(jnp.bfloat16),
        value_sum.astype(jnp.bfloat16),
    )


def adam_direction(weight, moment, second, grad):
    moment_new = beta_one * moment + (1.0 - beta_one) * grad
    second_new = beta_two * second + (1.0 - beta_two) * grad * grad
    corrected = moment_new / (1.0 - beta_one**step_count)
    scaled = second_new / (1.0 - beta_two**step_count)
    direction = corrected / (jnp.sqrt(scaled) + adam_eps) + weight_decay * weight
    return (moment_new, second_new, direction)


def local(
    frames,
    out_grad,
    time_emb,
    clip_len,
    pad_len,
    w_qkv,
    mom_qkv,
    var_qkv,
    w_out,
    mom_out,
    var_out,
    w_up,
    mom_up,
    var_up,
    w_down,
    mom_down,
    var_down,
    w_mod,
    mom_mod,
    var_mod,
    b_mod,
    mom_bias,
    var_bias,
):
    seq_count = lax.axis_size("seq")
    seq_rank = lax.axis_index("seq")
    frame_rows = frames.shape[0]
    group_frames = frame_rows * seq_count
    qkv_full, out_full, up_full, down_full, bias_full = (
        lax.all_gather(w_qkv.astype(jnp.bfloat16), "seq", axis=1, tiled=True),
        lax.all_gather(w_out.astype(jnp.bfloat16), "seq", axis=0, tiled=True),
        lax.all_gather(w_up.astype(jnp.bfloat16), "seq", axis=0, tiled=True),
        lax.all_gather(w_down.astype(jnp.bfloat16), "seq", axis=0, tiled=True),
        lax.all_gather(b_mod.astype(jnp.bfloat16), "seq", axis=0, tiled=True),
    )
    mod_low = w_mod.astype(jnp.bfloat16)
    mod_rows_here = w_mod.shape[0]
    mod_first = seq_rank * mod_rows_here
    inside_all, owners_all, places_all, usable_all = clip_tables(
        clip_len[0], pad_len[0], jnp.arange(group_frames, dtype=jnp.int32)
    )
    row_first = seq_rank * frame_rows
    inside_own = lax.dynamic_slice_in_dim(inside_all, row_first, frame_rows, 0)
    places_own = lax.dynamic_slice_in_dim(places_all, row_first, frame_rows, 0)
    silu_low = jax.nn.silu(time_emb).astype(jnp.bfloat16)
    silu_part = lax.dynamic_slice_in_dim(silu_low, mod_first, mod_rows_here, 1)
    modulation = lax.psum(
        jnp.dot(silu_part, mod_low, preferred_element_type=jnp.float32), "seq"
    ) + bias_full.astype(jnp.float32)
    mod_rows = jnp.dot(inside_own, modulation, precision=precise)
    shift_attn, scale_attn, gate_attn, shift_ff, scale_ff, gate_ff = jnp.split(mod_rows, 6, axis=1)
    inputs = frames.astype(jnp.float32)
    hidden, attn_norm_back = jax.vjp(modulate, inputs, shift_attn, scale_attn)
    hidden_low = hidden.astype(jnp.bfloat16)
    query_lin = jnp.dot(hidden_low, qkv_full[0], preferred_element_type=jnp.float32)
    key_lin = jnp.dot(hidden_low, qkv_full[1], preferred_element_type=jnp.float32)
    value_lin = jnp.dot(hidden_low, qkv_full[2], preferred_element_type=jnp.float32)
    query_send = rotate(query_lin, places_own, 1.0).astype(jnp.bfloat16)
    key_send = rotate(key_lin, places_own, 1.0).astype(jnp.bfloat16)
    value_send = value_lin.astype(jnp.bfloat16)
    query_heads, key_heads, value_heads = (
        lax.all_to_all(query_send, "seq", split_axis=1, concat_axis=0, tiled=True),
        lax.all_to_all(key_send, "seq", split_axis=1, concat_axis=0, tiled=True),
        lax.all_to_all(value_send, "seq", split_axis=1, concat_axis=0, tiled=True),
    )
    attended_heads, log_totals = attend_forward(
        query_heads, key_heads, value_heads, owners_all, usable_all, group_frames
    )
    attended = lax.all_to_all(attended_heads, "seq", split_axis=0, concat_axis=1, tiled=True)
    attn_proj = jnp.dot(attended, out_full, preferred_element_type=jnp.float32)
    mid = inputs + gate_attn * attn_proj
    hidden_ff, ff_norm_back = jax.vjp(modulate, mid, shift_ff, scale_ff)
    hidden_ff_low = hidden_ff.astype(jnp.bfloat16)
    pre_act = jnp.dot(hidden_ff_low, up_full, preferred_element_type=jnp.float32)
    active, gelu_back = jax.vjp(gelu_tanh, pre_act)
    active_low = active.astype(jnp.bfloat16)
    ff_proj = jnp.dot(active_low, down_full, preferred_element_type=jnp.float32)
    result = mid + gate_ff * ff_proj
    grad_result = out_grad.astype(jnp.float32)
    grad_gate_ff = grad_result * ff_proj
    grad_ff = (grad_result * gate_ff).astype(jnp.bfloat16)
    grad_down_local = jnp.einsum(
        "nf,nd->fd", active_low, grad_ff, preferred_element_type=jnp.float32
    )
    grad_active = jnp.einsum("nd,fd->nf", grad_ff, down_full, preferred_element_type=jnp.float32)
    (grad_pre,) = gelu_back(grad_active)
    grad_pre_low = grad_pre.astype(jnp.bfloat16)
    grad_up_local = jnp.einsum(
        "nd,nf->df", hidden_ff_low, grad_pre_low, preferred_element_type=jnp.float32
    )
    grad_hidden_ff = jnp.einsum(
        "nf,df->nd", grad_pre_low, up_full, preferred_element_type=jnp.float32
    )
    grad_mid_norm, grad_shift_ff, grad_scale_ff = ff_norm_back(grad_hidden_ff)
    grad_mid = grad_result + grad_mid_norm
    grad_gate_attn = grad_mid * attn_proj
    grad_proj = (grad_mid * gate_attn).astype(jnp.bfloat16)
    grad_out_local = jnp.einsum(
        "nd,ne->de", attended, grad_proj, preferred_element_type=jnp.float32
    )
    grad_attended = jnp.einsum(
        "ne,de->nd", grad_proj, out_full, preferred_element_type=jnp.float32
    ).astype(jnp.bfloat16)
    grad_heads = lax.all_to_all(grad_attended, "seq", split_axis=1, concat_axis=0, tiled=True)
    grad_query_heads, grad_key_heads, grad_value_heads = attend_backward(
        query_heads,
        key_heads,
        value_heads,
        grad_heads,
        log_totals,
        owners_all,
        usable_all,
        group_frames,
    )
    grad_query_rows, grad_key_rows, grad_value_rows = (
        lax.all_to_all(grad_query_heads, "seq", split_axis=0, concat_axis=1, tiled=True),
        lax.all_to_all(grad_key_heads, "seq", split_axis=0, concat_axis=1, tiled=True),
        lax.all_to_all(grad_value_heads, "seq", split_axis=0, concat_axis=1, tiled=True),
    )
    grad_query_lin = rotate(grad_query_rows.astype(jnp.float32), places_own, -1.0).astype(
        jnp.bfloat16
    )
    grad_key_lin = rotate(grad_key_rows.astype(jnp.float32), places_own, -1.0).astype(jnp.bfloat16)
    grad_qkv_local = jnp.stack(
        [
            jnp.einsum("nd,ne->de", hidden_low, grad_query_lin, preferred_element_type=jnp.float32),
            jnp.einsum("nd,ne->de", hidden_low, grad_key_lin, preferred_element_type=jnp.float32),
            jnp.einsum(
                "nd,ne->de", hidden_low, grad_value_rows, preferred_element_type=jnp.float32
            ),
        ]
    )
    grad_hidden = jnp.einsum(
        "ne,de->nd", grad_query_lin, qkv_full[0], preferred_element_type=jnp.float32
    )
    grad_hidden = grad_hidden + jnp.einsum(
        "ne,de->nd", grad_key_lin, qkv_full[1], preferred_element_type=jnp.float32
    )
    grad_hidden = grad_hidden + jnp.einsum(
        "ne,de->nd", grad_value_rows, qkv_full[2], preferred_element_type=jnp.float32
    )
    grad_input_norm, grad_shift_attn, grad_scale_attn = attn_norm_back(grad_hidden)
    input_grad = grad_mid + grad_input_norm
    grad_mod_rows = jnp.concatenate(
        [
            grad_shift_attn,
            grad_scale_attn,
            grad_gate_attn,
            grad_shift_ff,
            grad_scale_ff,
            grad_gate_ff,
        ],
        axis=1,
    )
    grad_mod_clip = lax.psum(
        jnp.einsum("nc,ne->ce", inside_own, grad_mod_rows, precision=precise), "seq"
    )
    grad_mod_all = lax.all_gather(grad_mod_clip, "dp", axis=0, tiled=True)
    silu_all = lax.all_gather(silu_part, "dp", axis=0, tiled=True)
    bias_cols = b_mod.shape[0]
    grad_bias_share = jnp.sum(
        lax.dynamic_slice_in_dim(grad_mod_all, seq_rank * bias_cols, bias_cols, 1), axis=0
    )
    grad_mod_share = jnp.einsum(
        "cd,ce->de", silu_all.astype(jnp.float32), grad_mod_all, precision=precise
    )
    grad_silu_part = jnp.einsum(
        "ce,de->cd", grad_mod_clip, mod_low.astype(jnp.float32), precision=precise
    )
    grad_silu = lax.all_gather(grad_silu_part, "seq", axis=1, tiled=True)
    time_grad = jax.vjp(jax.nn.silu, time_emb)[1](grad_silu)[0]
    shares = (
        lax.psum_scatter(
            grad_qkv_local.astype(jnp.bfloat16), "seq", scatter_dimension=1, tiled=True
        ).astype(jnp.float32),
        lax.psum_scatter(
            grad_out_local.astype(jnp.bfloat16), "seq", scatter_dimension=0, tiled=True
        ).astype(jnp.float32),
        lax.psum_scatter(
            grad_up_local.astype(jnp.bfloat16), "seq", scatter_dimension=0, tiled=True
        ).astype(jnp.float32),
        lax.psum_scatter(
            grad_down_local.astype(jnp.bfloat16), "seq", scatter_dimension=0, tiled=True
        ).astype(jnp.float32),
    )
    totals = (
        lax.psum(shares[0].astype(jnp.bfloat16), "dp").astype(jnp.float32),
        lax.psum(shares[1].astype(jnp.bfloat16), "dp").astype(jnp.float32),
        lax.psum(shares[2].astype(jnp.bfloat16), "dp").astype(jnp.float32),
        lax.psum(shares[3].astype(jnp.bfloat16), "dp").astype(jnp.float32),
        grad_mod_share,
        grad_bias_share,
    )
    masters = (w_qkv, w_out, w_up, w_down, w_mod, b_mod)
    moments = (mom_qkv, mom_out, mom_up, mom_down, mom_mod, mom_bias)
    seconds = (var_qkv, var_out, var_up, var_down, var_mod, var_bias)
    new_moments = []
    new_seconds = []
    directions = []
    weight_sums = []
    update_sums = []
    for param in range(6):
        moment_new, second_new, direction = adam_direction(
            masters[param], moments[param], seconds[param], totals[param]
        )
        sum_axes = (1, 2) if param == 0 else None
        new_moments.append(moment_new)
        new_seconds.append(second_new)
        directions.append(direction)
        weight_sums.append(jnp.sum(masters[param] * masters[param], axis=sum_axes, keepdims=True))
        update_sums.append(jnp.sum(direction * direction, axis=sum_axes, keepdims=True))
    norm_sums = lax.psum(
        (
            weight_sums[0],
            weight_sums[1],
            weight_sums[2],
            weight_sums[3],
            weight_sums[4],
            weight_sums[5],
            update_sums[0],
            update_sums[1],
            update_sums[2],
            update_sums[3],
            update_sums[4],
            update_sums[5],
        ),
        "seq",
    )
    new_masters = []
    for param in range(6):
        ratio = jnp.sqrt(norm_sums[param]) * lax.rsqrt(norm_sums[param + 6] + 1e-06)
        new_masters.append(masters[param] - step_rate * ratio * directions[param])
    return (
        result.astype(jnp.bfloat16),
        input_grad,
        time_grad,
        totals[0],
        new_masters[0],
        new_moments[0],
        new_seconds[0],
        totals[1],
        new_masters[1],
        new_moments[1],
        new_seconds[1],
        totals[2],
        new_masters[2],
        new_moments[2],
        new_seconds[2],
        totals[3],
        new_masters[3],
        new_moments[3],
        new_seconds[3],
        totals[4],
        new_masters[4],
        new_moments[4],
        new_seconds[4],
        totals[5],
        new_masters[5],
        new_moments[5],
        new_seconds[5],
    )


def solution(mesh):
    return jax.shard_map(
        local,
        mesh=mesh,
        in_specs=(
            P(("dp", "seq"), None),
            P(("dp", "seq"), None),
            P("dp", None),
            P("dp", None),
            P("dp", None),
            P(None, "seq", None),
            P(None, "seq", None),
            P(None, "seq", None),
            P("seq", None),
            P("seq", None),
            P("seq", None),
            P("seq", None),
            P("seq", None),
            P("seq", None),
            P("seq", None),
            P("seq", None),
            P("seq", None),
            P("seq", None),
            P("seq", None),
            P("seq", None),
            P("seq"),
            P("seq"),
            P("seq"),
        ),
        out_specs=(
            P(("dp", "seq"), None),
            P(("dp", "seq"), None),
            P("dp", None),
            P(None, "seq", None),
            P(None, "seq", None),
            P(None, "seq", None),
            P(None, "seq", None),
            P("seq", None),
            P("seq", None),
            P("seq", None),
            P("seq", None),
            P("seq", None),
            P("seq", None),
            P("seq", None),
            P("seq", None),
            P("seq", None),
            P("seq", None),
            P("seq", None),
            P("seq", None),
            P("seq", None),
            P("seq", None),
            P("seq", None),
            P("seq", None),
            P("seq"),
            P("seq"),
            P("seq"),
            P("seq"),
        ),
        check_vma=False,
    )
```

```python
import jax
import jax.numpy as jnp
from jax import lax
from jax.sharding import Mesh, PartitionSpec as P

HEAD_DIM = 64


precise = lax.Precision.HIGHEST
norm_eps = 1e-06
masked_score = -1e30
beta_one = 0.9
beta_two = 0.999
adam_eps = 1e-08
weight_decay = 0.01
step_rate = 1.0
step_count = 10


def layer_norm(values):
    center = values - jnp.mean(values, axis=-1, keepdims=True)
    spread = jnp.mean(center * center, axis=-1, keepdims=True)
    return center * lax.rsqrt(spread + norm_eps)


def modulate(values, shift, scale):
    return layer_norm(values) * (1.0 + scale) + shift


def gelu_tanh(values):
    return jax.nn.gelu(values, approximate=True)


def rotate(values, places, turn_sign):
    frame_count = values.shape[0]
    half_dim = HEAD_DIM // 2
    exponent = jnp.arange(half_dim, dtype=jnp.float32) * (-2.0 / HEAD_DIM)
    frequency = jnp.power(jnp.float32(10000.0), exponent)
    angles = places.astype(jnp.float32)[:, None] * frequency[None, :]
    cos_table = jnp.cos(angles)[:, None, :]
    sin_table = turn_sign * jnp.sin(angles)[:, None, :]
    paired = values.reshape(frame_count, values.shape[1] // HEAD_DIM, half_dim, 2)
    even_part = paired[..., 0]
    odd_part = paired[..., 1]
    turned = jnp.stack(
        [
            even_part * cos_table - odd_part * sin_table,
            odd_part * cos_table + even_part * sin_table,
        ],
        axis=-1,
    )
    return turned.reshape(frame_count, values.shape[1])


def clip_tables(lengths, padding, frame_ids):
    starts = jnp.cumsum(lengths) - lengths
    finish = starts + lengths
    inside = (frame_ids[:, None] >= starts[None, :]) & (frame_ids[:, None] < finish[None, :])
    clip_ids = jnp.arange(lengths.shape[0], dtype=jnp.int32)
    owners = jnp.sum(jnp.where(inside, clip_ids[None, :], 0), axis=1)
    begins = jnp.sum(jnp.where(inside, starts[None, :], 0), axis=1)
    kept_len = jnp.maximum(lengths - padding, 1)
    limits = jnp.sum(jnp.where(inside, kept_len[None, :], 0), axis=1)
    places = frame_ids - begins
    return (inside.astype(jnp.float32), owners, places, places < limits)


def key_window(block_index, block_rows, span, frame_count):
    return jnp.clip(block_index * block_rows - (span - block_rows) // 2, 0, frame_count - span)


def block_inputs(queries, keys_all, values, owners, usable, block_index, block_rows, span):
    frame_count, columns = queries.shape
    heads_here = columns // HEAD_DIM
    row_start = block_index * block_rows
    window = key_window(block_index, block_rows, span, frame_count)
    query_rows = lax.dynamic_slice_in_dim(queries, row_start, block_rows, 0).reshape(
        block_rows, heads_here, HEAD_DIM
    )
    keys_win = keys_all.reshape(span, heads_here, HEAD_DIM)
    values_win = values.reshape(span, heads_here, HEAD_DIM)
    query_owner = lax.dynamic_slice_in_dim(owners, row_start, block_rows, 0)
    score_scale = HEAD_DIM ** (-0.5)
    scores = (
        jnp.einsum("qhd,khd->hqk", query_rows, keys_win, preferred_element_type=jnp.float32)
        * score_scale
    )
    allowed = (query_owner[:, None] == owners[None, :]) & usable[None, :]
    masked = jnp.where(allowed[None], scores, masked_score)
    return (row_start, window, query_rows, keys_win, values_win, masked)


def attend_forward(queries, keys_all, values, owners, usable, span):
    frame_count, columns = queries.shape
    block_rows = min(512, frame_count)

    def one_block(block_index):
        row_start, window, query_rows, keys_win, values_win, masked = block_inputs(
            queries, keys_all, values, owners, usable, block_index, block_rows, span
        )
        row_max = jnp.max(masked, axis=-1, keepdims=True)
        row_total = jnp.sum(jnp.exp(masked - row_max), axis=-1, keepdims=True)
        log_total = row_max + jnp.log(row_total)
        probs_low = jnp.exp(masked - log_total).astype(jnp.bfloat16)
        attended = jnp.einsum(
            "hqk,khd->qhd", probs_low, values_win, preferred_element_type=jnp.float32
        )
        return (attended.astype(jnp.bfloat16).reshape(block_rows, columns), log_total)

    outcome, log_totals = lax.map(one_block, jnp.arange(frame_count // block_rows, dtype=jnp.int32))
    return (outcome.reshape(frame_count, columns), log_totals)


def attend_backward(queries, keys_all, values, grad_attended, log_totals, owners, usable, span):
    frame_count, columns = queries.shape
    heads_here = columns // HEAD_DIM
    block_rows = min(512, frame_count)
    score_scale = HEAD_DIM ** (-0.5)

    def one_block(sums, block_data):
        key_sum, value_sum = sums
        block_index, log_total = block_data
        row_start, window, query_rows, keys_win, values_win, masked = block_inputs(
            queries, keys_all, values, owners, usable, block_index, block_rows, span
        )
        grad_rows = lax.dynamic_slice_in_dim(grad_attended, row_start, block_rows, 0).reshape(
            block_rows, heads_here, HEAD_DIM
        )
        probs_full = jnp.exp(masked - log_total)
        probs_low = probs_full.astype(jnp.bfloat16)
        grad_probs = jnp.einsum(
            "qhd,khd->hqk", grad_rows, values_win, preferred_element_type=jnp.float32
        )
        row_delta = jnp.sum(probs_full * grad_probs, axis=-1, keepdims=True)
        grad_scores = (probs_full * (grad_probs - row_delta)).astype(jnp.bfloat16)
        grad_query = (
            jnp.einsum("hqk,khd->qhd", grad_scores, keys_win, preferred_element_type=jnp.float32)
            * score_scale
        )
        grad_key = (
            jnp.einsum("hqk,qhd->khd", grad_scores, query_rows, preferred_element_type=jnp.float32)
            * score_scale
        )
        grad_value = jnp.einsum(
            "hqk,qhd->khd", probs_low, grad_rows, preferred_element_type=jnp.float32
        )
        old_keys = key_sum
        key_sum = old_keys + grad_key.reshape(span, columns)
        old_values = value_sum
        value_sum = old_values + grad_value.reshape(span, columns)
        return ((key_sum, value_sum), grad_query.astype(jnp.bfloat16).reshape(block_rows, columns))

    zeros = jnp.zeros((frame_count, columns), jnp.float32)
    indices = jnp.arange(frame_count // block_rows, dtype=jnp.int32)
    (key_sum, value_sum), grad_queries = lax.scan(one_block, (zeros, zeros), (indices, log_totals))
    return (
        grad_queries.reshape(frame_count, columns),
        key_sum.astype(jnp.bfloat16),
        value_sum.astype(jnp.bfloat16),
    )


def butterfly_sum(values, axes, size):
    step = 1
    while step < size:
        values = values + lax.ppermute(values, axes, [(i, i ^ step) for i in range(size)])
        step *= 2
    return values


def doubling_gather(values, axes, size, index):
    blocks = values[None]
    step = 1
    while step < size:
        other = lax.ppermute(blocks, axes, [(i, i ^ step) for i in range(size)])
        low_side = (index // step) % 2 == 0
        blocks = jnp.concatenate(
            [jnp.where(low_side, blocks, other), jnp.where(low_side, other, blocks)], axis=0
        )
        step *= 2
    return blocks


def gather_rows(shard, row_axis):
    half = shard.shape[row_axis] // 2
    core = lax.axis_index("core")
    piece = lax.dynamic_slice_in_dim(shard, core * half, half, row_axis)
    return lax.all_gather(piece, ("seq", "core"), axis=row_axis, tiled=True)


def reduce_rows(partial, row_axis):
    piece = lax.psum_scatter(partial, ("seq", "core"), scatter_dimension=row_axis, tiled=True)
    piece = lax.psum(piece, "z")
    return lax.all_gather(piece, "core", axis=row_axis, tiled=True)


def adam_direction(weight, moment, second, grad):
    moment_new = beta_one * moment + (1.0 - beta_one) * grad
    second_new = beta_two * second + (1.0 - beta_two) * grad * grad
    corrected = moment_new / (1.0 - beta_one**step_count)
    scaled = second_new / (1.0 - beta_two**step_count)
    direction = corrected / (jnp.sqrt(scaled) + adam_eps) + weight_decay * weight
    return (moment_new, second_new, direction)


def local(
    frames,
    out_grad,
    time_emb,
    clip_len,
    pad_len,
    w_qkv,
    mom_qkv,
    var_qkv,
    w_out,
    mom_out,
    var_out,
    w_up,
    mom_up,
    var_up,
    w_down,
    mom_down,
    var_down,
    w_mod,
    mom_mod,
    var_mod,
    b_mod,
    mom_bias,
    var_bias,
):
    seq_count = lax.axis_size("seq")
    seq_rank = lax.axis_index("seq")
    frame_rows = frames.shape[0]
    group_frames = frame_rows * seq_count
    dp_count = lax.axis_size(("z", "core"))
    dp_rank = lax.axis_index(("z", "core"))
    qkv_full, out_full, up_full, down_full = (
        gather_rows(w_qkv.astype(jnp.bfloat16), 1),
        gather_rows(w_out.astype(jnp.bfloat16), 0),
        gather_rows(w_up.astype(jnp.bfloat16), 0),
        gather_rows(w_down.astype(jnp.bfloat16), 0),
    )
    bias_full = doubling_gather(b_mod.astype(jnp.bfloat16), "seq", seq_count, seq_rank).reshape(-1)
    mod_low = w_mod.astype(jnp.bfloat16)
    mod_rows_here = w_mod.shape[0]
    mod_first = seq_rank * mod_rows_here
    inside_all, owners_all, places_all, usable_all = clip_tables(
        clip_len[0], pad_len[0], jnp.arange(group_frames, dtype=jnp.int32)
    )
    row_first = seq_rank * frame_rows
    inside_own = lax.dynamic_slice_in_dim(inside_all, row_first, frame_rows, 0)
    places_own = lax.dynamic_slice_in_dim(places_all, row_first, frame_rows, 0)
    silu_low = jax.nn.silu(time_emb).astype(jnp.bfloat16)
    silu_part = lax.dynamic_slice_in_dim(silu_low, mod_first, mod_rows_here, 1)
    modulation = butterfly_sum(
        jnp.dot(silu_part, mod_low, preferred_element_type=jnp.float32), "seq", seq_count
    ) + bias_full.astype(jnp.float32)
    mod_rows = jnp.dot(inside_own, modulation, precision=precise)
    shift_attn, scale_attn, gate_attn, shift_ff, scale_ff, gate_ff = jnp.split(mod_rows, 6, axis=1)
    inputs = frames.astype(jnp.float32)
    hidden, attn_norm_back = jax.vjp(modulate, inputs, shift_attn, scale_attn)
    hidden_low = hidden.astype(jnp.bfloat16)
    query_lin = jnp.dot(hidden_low, qkv_full[0], preferred_element_type=jnp.float32)
    key_lin = jnp.dot(hidden_low, qkv_full[1], preferred_element_type=jnp.float32)
    value_lin = jnp.dot(hidden_low, qkv_full[2], preferred_element_type=jnp.float32)
    query_send = rotate(query_lin, places_own, 1.0).astype(jnp.bfloat16)
    key_send = rotate(key_lin, places_own, 1.0).astype(jnp.bfloat16)
    value_send = value_lin.astype(jnp.bfloat16)
    query_heads, key_heads, value_heads = (
        lax.all_to_all(query_send, "seq", split_axis=1, concat_axis=0, tiled=True),
        lax.all_to_all(key_send, "seq", split_axis=1, concat_axis=0, tiled=True),
        lax.all_to_all(value_send, "seq", split_axis=1, concat_axis=0, tiled=True),
    )
    attended_heads, log_totals = attend_forward(
        query_heads, key_heads, value_heads, owners_all, usable_all, group_frames
    )
    attended = lax.all_to_all(attended_heads, "seq", split_axis=0, concat_axis=1, tiled=True)
    attn_proj = jnp.dot(attended, out_full, preferred_element_type=jnp.float32)
    mid = inputs + gate_attn * attn_proj
    hidden_ff, ff_norm_back = jax.vjp(modulate, mid, shift_ff, scale_ff)
    hidden_ff_low = hidden_ff.astype(jnp.bfloat16)
    pre_act = jnp.dot(hidden_ff_low, up_full, preferred_element_type=jnp.float32)
    active, gelu_back = jax.vjp(gelu_tanh, pre_act)
    active_low = active.astype(jnp.bfloat16)
    ff_proj = jnp.dot(active_low, down_full, preferred_element_type=jnp.float32)
    result = mid + gate_ff * ff_proj
    grad_result = out_grad.astype(jnp.float32)
    grad_gate_ff = grad_result * ff_proj
    grad_ff = (grad_result * gate_ff).astype(jnp.bfloat16)
    grad_down_local = jnp.einsum(
        "nf,nd->fd", active_low, grad_ff, preferred_element_type=jnp.float32
    )
    grad_active = jnp.einsum("nd,fd->nf", grad_ff, down_full, preferred_element_type=jnp.float32)
    (grad_pre,) = gelu_back(grad_active)
    grad_pre_low = grad_pre.astype(jnp.bfloat16)
    grad_up_local = jnp.einsum(
        "nd,nf->df", hidden_ff_low, grad_pre_low, preferred_element_type=jnp.float32
    )
    grad_hidden_ff = jnp.einsum(
        "nf,df->nd", grad_pre_low, up_full, preferred_element_type=jnp.float32
    )
    grad_mid_norm, grad_shift_ff, grad_scale_ff = ff_norm_back(grad_hidden_ff)
    grad_mid = grad_result + grad_mid_norm
    grad_gate_attn = grad_mid * attn_proj
    grad_proj = (grad_mid * gate_attn).astype(jnp.bfloat16)
    grad_out_local = jnp.einsum(
        "nd,ne->de", attended, grad_proj, preferred_element_type=jnp.float32
    )
    grad_attended = jnp.einsum(
        "ne,de->nd", grad_proj, out_full, preferred_element_type=jnp.float32
    ).astype(jnp.bfloat16)
    grad_heads = lax.all_to_all(grad_attended, "seq", split_axis=1, concat_axis=0, tiled=True)
    grad_query_heads, grad_key_heads, grad_value_heads = attend_backward(
        query_heads,
        key_heads,
        value_heads,
        grad_heads,
        log_totals,
        owners_all,
        usable_all,
        group_frames,
    )
    grad_query_rows, grad_key_rows, grad_value_rows = (
        lax.all_to_all(grad_query_heads, "seq", split_axis=0, concat_axis=1, tiled=True),
        lax.all_to_all(grad_key_heads, "seq", split_axis=0, concat_axis=1, tiled=True),
        lax.all_to_all(grad_value_heads, "seq", split_axis=0, concat_axis=1, tiled=True),
    )
    grad_query_lin = rotate(grad_query_rows.astype(jnp.float32), places_own, -1.0).astype(
        jnp.bfloat16
    )
    grad_key_lin = rotate(grad_key_rows.astype(jnp.float32), places_own, -1.0).astype(jnp.bfloat16)
    grad_qkv_local = jnp.stack(
        [
            jnp.einsum("nd,ne->de", hidden_low, grad_query_lin, preferred_element_type=jnp.float32),
            jnp.einsum("nd,ne->de", hidden_low, grad_key_lin, preferred_element_type=jnp.float32),
            jnp.einsum(
                "nd,ne->de", hidden_low, grad_value_rows, preferred_element_type=jnp.float32
            ),
        ]
    )
    grad_hidden = jnp.einsum(
        "ne,de->nd", grad_query_lin, qkv_full[0], preferred_element_type=jnp.float32
    )
    grad_hidden = grad_hidden + jnp.einsum(
        "ne,de->nd", grad_key_lin, qkv_full[1], preferred_element_type=jnp.float32
    )
    grad_hidden = grad_hidden + jnp.einsum(
        "ne,de->nd", grad_value_rows, qkv_full[2], preferred_element_type=jnp.float32
    )
    grad_input_norm, grad_shift_attn, grad_scale_attn = attn_norm_back(grad_hidden)
    input_grad = grad_mid + grad_input_norm
    grad_mod_rows = jnp.concatenate(
        [
            grad_shift_attn,
            grad_scale_attn,
            grad_gate_attn,
            grad_shift_ff,
            grad_scale_ff,
            grad_gate_ff,
        ],
        axis=1,
    )
    grad_mod_clip = butterfly_sum(
        jnp.einsum("nc,ne->ce", inside_own, grad_mod_rows, precision=precise), "seq", seq_count
    )
    grad_mod_all = doubling_gather(grad_mod_clip, ("z", "core"), dp_count, dp_rank).reshape(
        -1, grad_mod_clip.shape[1]
    )
    silu_all = doubling_gather(silu_part, ("z", "core"), dp_count, dp_rank).reshape(
        -1, silu_part.shape[1]
    )
    bias_cols = b_mod.shape[0]
    grad_bias_share = jnp.sum(
        lax.dynamic_slice_in_dim(grad_mod_all, seq_rank * bias_cols, bias_cols, 1), axis=0
    )
    grad_mod_share = jnp.einsum(
        "cd,ce->de", silu_all.astype(jnp.float32), grad_mod_all, precision=precise
    )
    grad_silu_part = jnp.einsum(
        "ce,de->cd", grad_mod_clip, mod_low.astype(jnp.float32), precision=precise
    )
    grad_silu = jnp.concatenate(
        list(doubling_gather(grad_silu_part, "seq", seq_count, seq_rank)), axis=1
    )
    time_grad = jax.vjp(jax.nn.silu, time_emb)[1](grad_silu)[0]
    totals = (
        reduce_rows(grad_qkv_local.astype(jnp.bfloat16), 1).astype(jnp.float32),
        reduce_rows(grad_out_local.astype(jnp.bfloat16), 0).astype(jnp.float32),
        reduce_rows(grad_up_local.astype(jnp.bfloat16), 0).astype(jnp.float32),
        reduce_rows(grad_down_local.astype(jnp.bfloat16), 0).astype(jnp.float32),
        grad_mod_share,
        grad_bias_share,
    )
    masters = (w_qkv, w_out, w_up, w_down, w_mod, b_mod)
    moments = (mom_qkv, mom_out, mom_up, mom_down, mom_mod, mom_bias)
    seconds = (var_qkv, var_out, var_up, var_down, var_mod, var_bias)
    new_moments = []
    new_seconds = []
    directions = []
    weight_sums = []
    update_sums = []
    for param in range(6):
        moment_new, second_new, direction = adam_direction(
            masters[param], moments[param], seconds[param], totals[param]
        )
        sum_axes = (1, 2) if param == 0 else None
        new_moments.append(moment_new)
        new_seconds.append(second_new)
        directions.append(direction)
        weight_sums.append(jnp.sum(masters[param] * masters[param], axis=sum_axes, keepdims=True))
        update_sums.append(jnp.sum(direction * direction, axis=sum_axes, keepdims=True))
    packed = jnp.concatenate([jnp.reshape(part, (-1,)) for part in weight_sums + update_sums])
    packed = butterfly_sum(packed, "seq", seq_count)
    norm_sums = []
    offset = 0
    for part in weight_sums + update_sums:
        norm_sums.append(packed[offset : offset + part.size].reshape(part.shape))
        offset += part.size
    new_masters = []
    for param in range(6):
        ratio = jnp.sqrt(norm_sums[param]) * lax.rsqrt(norm_sums[param + 6] + 1e-06)
        new_masters.append(masters[param] - step_rate * ratio * directions[param])
    return (
        result.astype(jnp.bfloat16),
        input_grad,
        time_grad,
        totals[0],
        new_masters[0],
        new_moments[0],
        new_seconds[0],
        totals[1],
        new_masters[1],
        new_moments[1],
        new_seconds[1],
        totals[2],
        new_masters[2],
        new_moments[2],
        new_seconds[2],
        totals[3],
        new_masters[3],
        new_moments[3],
        new_seconds[3],
        totals[4],
        new_masters[4],
        new_moments[4],
        new_seconds[4],
        totals[5],
        new_masters[5],
        new_moments[5],
        new_seconds[5],
    )


def solution(mesh):
    devices = mesh.devices
    chip_mesh = Mesh(
        devices.reshape(devices.shape[0] // 2, 2, devices.shape[1]), ("z", "core", "seq")
    )
    return jax.shard_map(
        local,
        mesh=chip_mesh,
        in_specs=(
            P(("z", "core", "seq"), None),
            P(("z", "core", "seq"), None),
            P(("z", "core"), None),
            P(("z", "core"), None),
            P(("z", "core"), None),
            P(None, "seq", None),
            P(None, "seq", None),
            P(None, "seq", None),
            P("seq", None),
            P("seq", None),
            P("seq", None),
            P("seq", None),
            P("seq", None),
            P("seq", None),
            P("seq", None),
            P("seq", None),
            P("seq", None),
            P("seq", None),
            P("seq", None),
            P("seq", None),
            P("seq"),
            P("seq"),
            P("seq"),
        ),
        out_specs=(
            P(("z", "core", "seq"), None),
            P(("z", "core", "seq"), None),
            P(("z", "core"), None),
            P(None, "seq", None),
            P(None, "seq", None),
            P(None, "seq", None),
            P(None, "seq", None),
            P("seq", None),
            P("seq", None),
            P("seq", None),
            P("seq", None),
            P("seq", None),
            P("seq", None),
            P("seq", None),
            P("seq", None),
            P("seq", None),
            P("seq", None),
            P("seq", None),
            P("seq", None),
            P("seq", None),
            P("seq", None),
            P("seq", None),
            P("seq", None),
            P("seq"),
            P("seq"),
            P("seq"),
            P("seq"),
        ),
        check_vma=False,
    )
```

```python
import jax
import jax.numpy as jnp
from jax import lax
from jax.sharding import Mesh, PartitionSpec as P

HEAD_DIM = 64


precise = lax.Precision.HIGHEST
norm_eps = 1e-06
masked_score = -1e30
beta_one = 0.9
beta_two = 0.999
adam_eps = 1e-08
weight_decay = 0.01
step_rate = 1.0
step_count = 10


def layer_norm(values):
    center = values - jnp.mean(values, axis=-1, keepdims=True)
    spread = jnp.mean(center * center, axis=-1, keepdims=True)
    return center * lax.rsqrt(spread + norm_eps)


def modulate(values, shift, scale):
    return layer_norm(values) * (1.0 + scale) + shift


def gelu_tanh(values):
    return jax.nn.gelu(values, approximate=True)


def rotate(values, places, turn_sign):
    frame_count = values.shape[0]
    half_dim = HEAD_DIM // 2
    exponent = jnp.arange(half_dim, dtype=jnp.float32) * (-2.0 / HEAD_DIM)
    frequency = jnp.power(jnp.float32(10000.0), exponent)
    angles = places.astype(jnp.float32)[:, None] * frequency[None, :]
    cos_table = jnp.cos(angles)[:, None, :]
    sin_table = turn_sign * jnp.sin(angles)[:, None, :]
    paired = values.reshape(frame_count, values.shape[1] // HEAD_DIM, half_dim, 2)
    even_part = paired[..., 0]
    odd_part = paired[..., 1]
    turned = jnp.stack(
        [
            even_part * cos_table - odd_part * sin_table,
            odd_part * cos_table + even_part * sin_table,
        ],
        axis=-1,
    )
    return turned.reshape(frame_count, values.shape[1])


def clip_tables(lengths, padding, frame_ids):
    starts = jnp.cumsum(lengths) - lengths
    finish = starts + lengths
    inside = (frame_ids[:, None] >= starts[None, :]) & (frame_ids[:, None] < finish[None, :])
    clip_ids = jnp.arange(lengths.shape[0], dtype=jnp.int32)
    owners = jnp.sum(jnp.where(inside, clip_ids[None, :], 0), axis=1)
    begins = jnp.sum(jnp.where(inside, starts[None, :], 0), axis=1)
    kept_len = jnp.maximum(lengths - padding, 1)
    limits = jnp.sum(jnp.where(inside, kept_len[None, :], 0), axis=1)
    places = frame_ids - begins
    return (inside.astype(jnp.float32), owners, places, places < limits)


def key_window(block_index, block_rows, span, frame_count):
    return jnp.clip(block_index * block_rows - (span - block_rows) // 2, 0, frame_count - span)


def block_inputs(queries, keys_all, values, owners, usable, block_index, block_rows, span):
    frame_count, columns = queries.shape
    heads_here = columns // HEAD_DIM
    row_start = block_index * block_rows
    window = key_window(block_index, block_rows, span, frame_count)
    query_rows = lax.dynamic_slice_in_dim(queries, row_start, block_rows, 0).reshape(
        block_rows, heads_here, HEAD_DIM
    )
    keys_win = keys_all.reshape(span, heads_here, HEAD_DIM)
    values_win = values.reshape(span, heads_here, HEAD_DIM)
    query_owner = lax.dynamic_slice_in_dim(owners, row_start, block_rows, 0)
    score_scale = HEAD_DIM ** (-0.5)
    scores = (
        jnp.einsum("qhd,khd->hqk", query_rows, keys_win, preferred_element_type=jnp.float32)
        * score_scale
    )
    allowed = (query_owner[:, None] == owners[None, :]) & usable[None, :]
    masked = jnp.where(allowed[None], scores, masked_score)
    return (row_start, window, query_rows, keys_win, values_win, masked)


def attend_forward(queries, keys_all, values, owners, usable, span):
    frame_count, columns = queries.shape
    block_rows = min(512, frame_count)

    def one_block(block_index):
        row_start, window, query_rows, keys_win, values_win, masked = block_inputs(
            queries, keys_all, values, owners, usable, block_index, block_rows, span
        )
        row_max = jnp.max(masked, axis=-1, keepdims=True)
        row_total = jnp.sum(jnp.exp(masked - row_max), axis=-1, keepdims=True)
        log_total = row_max + jnp.log(row_total)
        probs_low = jnp.exp(masked - log_total).astype(jnp.bfloat16)
        attended = jnp.einsum(
            "hqk,khd->qhd", probs_low, values_win, preferred_element_type=jnp.float32
        )
        return (attended.astype(jnp.bfloat16).reshape(block_rows, columns), log_total)

    outcome, log_totals = lax.map(one_block, jnp.arange(frame_count // block_rows, dtype=jnp.int32))
    return (outcome.reshape(frame_count, columns), log_totals)


def attend_backward(queries, keys_all, values, grad_attended, log_totals, owners, usable, span):
    frame_count, columns = queries.shape
    heads_here = columns // HEAD_DIM
    block_rows = min(512, frame_count)
    score_scale = HEAD_DIM ** (-0.5)

    def one_block(sums, block_data):
        key_sum, value_sum = sums
        block_index, log_total = block_data
        row_start, window, query_rows, keys_win, values_win, masked = block_inputs(
            queries, keys_all, values, owners, usable, block_index, block_rows, span
        )
        grad_rows = lax.dynamic_slice_in_dim(grad_attended, row_start, block_rows, 0).reshape(
            block_rows, heads_here, HEAD_DIM
        )
        probs_full = jnp.exp(masked - log_total)
        probs_low = probs_full.astype(jnp.bfloat16)
        grad_probs = jnp.einsum(
            "qhd,khd->hqk", grad_rows, values_win, preferred_element_type=jnp.float32
        )
        row_delta = jnp.sum(probs_full * grad_probs, axis=-1, keepdims=True)
        grad_scores = (probs_full * (grad_probs - row_delta)).astype(jnp.bfloat16)
        grad_query = (
            jnp.einsum("hqk,khd->qhd", grad_scores, keys_win, preferred_element_type=jnp.float32)
            * score_scale
        )
        grad_key = (
            jnp.einsum("hqk,qhd->khd", grad_scores, query_rows, preferred_element_type=jnp.float32)
            * score_scale
        )
        grad_value = jnp.einsum(
            "hqk,qhd->khd", probs_low, grad_rows, preferred_element_type=jnp.float32
        )
        old_keys = key_sum
        key_sum = old_keys + grad_key.reshape(span, columns)
        old_values = value_sum
        value_sum = old_values + grad_value.reshape(span, columns)
        return ((key_sum, value_sum), grad_query.astype(jnp.bfloat16).reshape(block_rows, columns))

    zeros = jnp.zeros((frame_count, columns), jnp.float32)
    indices = jnp.arange(frame_count // block_rows, dtype=jnp.int32)
    (key_sum, value_sum), grad_queries = lax.scan(one_block, (zeros, zeros), (indices, log_totals))
    return (
        grad_queries.reshape(frame_count, columns),
        key_sum.astype(jnp.bfloat16),
        value_sum.astype(jnp.bfloat16),
    )


def butterfly_sum(values, axes, size):
    step = 1
    while step < size:
        values = values + lax.ppermute(values, axes, [(i, i ^ step) for i in range(size)])
        step *= 2
    return values


def doubling_gather(values, axes, size, index):
    blocks = values[None]
    step = 1
    while step < size:
        other = lax.ppermute(blocks, axes, [(i, i ^ step) for i in range(size)])
        low_side = (index // step) % 2 == 0
        blocks = jnp.concatenate(
            [jnp.where(low_side, blocks, other), jnp.where(low_side, other, blocks)], axis=0
        )
        step *= 2
    return blocks


def gather_rows(shard, row_axis):
    half = shard.shape[row_axis] // 2
    core = lax.axis_index("core")
    piece = lax.dynamic_slice_in_dim(shard, core * half, half, row_axis)
    return lax.all_gather(piece, ("seq", "core"), axis=row_axis, tiled=True)


def halving_sum(values, axis_name, size):
    index = lax.axis_index(axis_name)
    total = values.astype(jnp.float32)
    step = 1
    while step < size:
        half = total.shape[-1] // 2
        low_side = (index // step) % 2 == 0
        keep = jnp.where(low_side, total[..., :half], total[..., half:])
        send = jnp.where(low_side, total[..., half:], total[..., :half]).astype(jnp.bfloat16)
        total = keep + lax.ppermute(send, axis_name, [(i, i ^ step) for i in range(size)]).astype(
            jnp.float32
        )
        step *= 2
    blocks = total.astype(jnp.bfloat16)
    step = size // 2
    while step >= 1:
        other = lax.ppermute(blocks, axis_name, [(i, i ^ step) for i in range(size)])
        low_side = (index // step) % 2 == 0
        blocks = jnp.concatenate(
            [jnp.where(low_side, blocks, other), jnp.where(low_side, other, blocks)], axis=-1
        )
        step //= 2
    return blocks


def reduce_rows(partial, row_axis):
    piece = lax.psum_scatter(partial, ("seq", "core"), scatter_dimension=row_axis, tiled=True)
    piece = halving_sum(piece, "z", lax.axis_size("z"))
    other = lax.ppermute(piece, "core", [(0, 1), (1, 0)])
    first = lax.axis_index("core") == 0
    return jnp.concatenate(
        [jnp.where(first, piece, other), jnp.where(first, other, piece)], axis=row_axis
    )


def adam_direction(weight, moment, second, grad):
    moment_new = beta_one * moment + (1.0 - beta_one) * grad
    second_new = beta_two * second + (1.0 - beta_two) * grad * grad
    corrected = moment_new / (1.0 - beta_one**step_count)
    scaled = second_new / (1.0 - beta_two**step_count)
    direction = corrected / (jnp.sqrt(scaled) + adam_eps) + weight_decay * weight
    return (moment_new, second_new, direction)


def local(
    frames,
    out_grad,
    time_emb,
    clip_len,
    pad_len,
    w_qkv,
    mom_qkv,
    var_qkv,
    w_out,
    mom_out,
    var_out,
    w_up,
    mom_up,
    var_up,
    w_down,
    mom_down,
    var_down,
    w_mod,
    mom_mod,
    var_mod,
    b_mod,
    mom_bias,
    var_bias,
):
    seq_count = lax.axis_size("seq")
    seq_rank = lax.axis_index("seq")
    frame_rows = frames.shape[0]
    group_frames = frame_rows * seq_count
    dp_count = lax.axis_size(("z", "core"))
    dp_rank = lax.axis_index(("z", "core"))
    qkv_full, out_full, up_full, down_full = (
        gather_rows(w_qkv.astype(jnp.bfloat16), 1),
        gather_rows(w_out.astype(jnp.bfloat16), 0),
        gather_rows(w_up.astype(jnp.bfloat16), 0),
        gather_rows(w_down.astype(jnp.bfloat16), 0),
    )
    bias_full = doubling_gather(b_mod.astype(jnp.bfloat16), "seq", seq_count, seq_rank).reshape(-1)
    mod_low = w_mod.astype(jnp.bfloat16)
    mod_rows_here = w_mod.shape[0]
    mod_first = seq_rank * mod_rows_here
    inside_all, owners_all, places_all, usable_all = clip_tables(
        clip_len[0], pad_len[0], jnp.arange(group_frames, dtype=jnp.int32)
    )
    row_first = seq_rank * frame_rows
    inside_own = lax.dynamic_slice_in_dim(inside_all, row_first, frame_rows, 0)
    places_own = lax.dynamic_slice_in_dim(places_all, row_first, frame_rows, 0)
    silu_low = jax.nn.silu(time_emb).astype(jnp.bfloat16)
    silu_part = lax.dynamic_slice_in_dim(silu_low, mod_first, mod_rows_here, 1)
    modulation = butterfly_sum(
        jnp.dot(silu_part, mod_low, preferred_element_type=jnp.float32), "seq", seq_count
    ) + bias_full.astype(jnp.float32)
    mod_rows = jnp.dot(inside_own, modulation, precision=precise)
    shift_attn, scale_attn, gate_attn, shift_ff, scale_ff, gate_ff = jnp.split(mod_rows, 6, axis=1)
    inputs = frames.astype(jnp.float32)
    hidden, attn_norm_back = jax.vjp(modulate, inputs, shift_attn, scale_attn)
    hidden_low = hidden.astype(jnp.bfloat16)
    query_lin = jnp.dot(hidden_low, qkv_full[0], preferred_element_type=jnp.float32)
    key_lin = jnp.dot(hidden_low, qkv_full[1], preferred_element_type=jnp.float32)
    value_lin = jnp.dot(hidden_low, qkv_full[2], preferred_element_type=jnp.float32)
    query_send = rotate(query_lin, places_own, 1.0).astype(jnp.bfloat16)
    key_send = rotate(key_lin, places_own, 1.0).astype(jnp.bfloat16)
    value_send = value_lin.astype(jnp.bfloat16)
    query_heads, key_heads, value_heads = (
        lax.all_to_all(query_send, "seq", split_axis=1, concat_axis=0, tiled=True),
        lax.all_to_all(key_send, "seq", split_axis=1, concat_axis=0, tiled=True),
        lax.all_to_all(value_send, "seq", split_axis=1, concat_axis=0, tiled=True),
    )
    attended_heads, log_totals = attend_forward(
        query_heads, key_heads, value_heads, owners_all, usable_all, group_frames
    )
    attended = lax.all_to_all(attended_heads, "seq", split_axis=0, concat_axis=1, tiled=True)
    attn_proj = jnp.dot(attended, out_full, preferred_element_type=jnp.float32)
    mid = inputs + gate_attn * attn_proj
    hidden_ff, ff_norm_back = jax.vjp(modulate, mid, shift_ff, scale_ff)
    hidden_ff_low = hidden_ff.astype(jnp.bfloat16)
    pre_act = jnp.dot(hidden_ff_low, up_full, preferred_element_type=jnp.float32)
    active, gelu_back = jax.vjp(gelu_tanh, pre_act)
    active_low = active.astype(jnp.bfloat16)
    ff_proj = jnp.dot(active_low, down_full, preferred_element_type=jnp.float32)
    result = mid + gate_ff * ff_proj
    grad_result = out_grad.astype(jnp.float32)
    grad_gate_ff = grad_result * ff_proj
    grad_ff = (grad_result * gate_ff).astype(jnp.bfloat16)
    grad_down_local = jnp.einsum(
        "nf,nd->fd", active_low, grad_ff, preferred_element_type=jnp.float32
    )
    grad_active = jnp.einsum("nd,fd->nf", grad_ff, down_full, preferred_element_type=jnp.float32)
    (grad_pre,) = gelu_back(grad_active)
    grad_pre_low = grad_pre.astype(jnp.bfloat16)
    grad_up_local = jnp.einsum(
        "nd,nf->df", hidden_ff_low, grad_pre_low, preferred_element_type=jnp.float32
    )
    grad_hidden_ff = jnp.einsum(
        "nf,df->nd", grad_pre_low, up_full, preferred_element_type=jnp.float32
    )
    grad_mid_norm, grad_shift_ff, grad_scale_ff = ff_norm_back(grad_hidden_ff)
    grad_mid = grad_result + grad_mid_norm
    grad_gate_attn = grad_mid * attn_proj
    grad_proj = (grad_mid * gate_attn).astype(jnp.bfloat16)
    grad_out_local = jnp.einsum(
        "nd,ne->de", attended, grad_proj, preferred_element_type=jnp.float32
    )
    grad_attended = jnp.einsum(
        "ne,de->nd", grad_proj, out_full, preferred_element_type=jnp.float32
    ).astype(jnp.bfloat16)
    grad_heads = lax.all_to_all(grad_attended, "seq", split_axis=1, concat_axis=0, tiled=True)
    grad_query_heads, grad_key_heads, grad_value_heads = attend_backward(
        query_heads,
        key_heads,
        value_heads,
        grad_heads,
        log_totals,
        owners_all,
        usable_all,
        group_frames,
    )
    grad_query_rows, grad_key_rows, grad_value_rows = (
        lax.all_to_all(grad_query_heads, "seq", split_axis=0, concat_axis=1, tiled=True),
        lax.all_to_all(grad_key_heads, "seq", split_axis=0, concat_axis=1, tiled=True),
        lax.all_to_all(grad_value_heads, "seq", split_axis=0, concat_axis=1, tiled=True),
    )
    grad_query_lin = rotate(grad_query_rows.astype(jnp.float32), places_own, -1.0).astype(
        jnp.bfloat16
    )
    grad_key_lin = rotate(grad_key_rows.astype(jnp.float32), places_own, -1.0).astype(jnp.bfloat16)
    grad_qkv_local = jnp.stack(
        [
            jnp.einsum("nd,ne->de", hidden_low, grad_query_lin, preferred_element_type=jnp.float32),
            jnp.einsum("nd,ne->de", hidden_low, grad_key_lin, preferred_element_type=jnp.float32),
            jnp.einsum(
                "nd,ne->de", hidden_low, grad_value_rows, preferred_element_type=jnp.float32
            ),
        ]
    )
    grad_hidden = jnp.einsum(
        "ne,de->nd", grad_query_lin, qkv_full[0], preferred_element_type=jnp.float32
    )
    grad_hidden = grad_hidden + jnp.einsum(
        "ne,de->nd", grad_key_lin, qkv_full[1], preferred_element_type=jnp.float32
    )
    grad_hidden = grad_hidden + jnp.einsum(
        "ne,de->nd", grad_value_rows, qkv_full[2], preferred_element_type=jnp.float32
    )
    grad_input_norm, grad_shift_attn, grad_scale_attn = attn_norm_back(grad_hidden)
    input_grad = grad_mid + grad_input_norm
    grad_mod_rows = jnp.concatenate(
        [
            grad_shift_attn,
            grad_scale_attn,
            grad_gate_attn,
            grad_shift_ff,
            grad_scale_ff,
            grad_gate_ff,
        ],
        axis=1,
    )
    grad_mod_clip = butterfly_sum(
        jnp.einsum("nc,ne->ce", inside_own, grad_mod_rows, precision=precise), "seq", seq_count
    )
    grad_mod_all = doubling_gather(grad_mod_clip, ("z", "core"), dp_count, dp_rank).reshape(
        -1, grad_mod_clip.shape[1]
    )
    silu_all = doubling_gather(silu_part, ("z", "core"), dp_count, dp_rank).reshape(
        -1, silu_part.shape[1]
    )
    bias_cols = b_mod.shape[0]
    grad_bias_share = jnp.sum(
        lax.dynamic_slice_in_dim(grad_mod_all, seq_rank * bias_cols, bias_cols, 1), axis=0
    )
    grad_mod_share = jnp.einsum(
        "cd,ce->de", silu_all.astype(jnp.float32), grad_mod_all, precision=precise
    )
    grad_silu_part = jnp.einsum(
        "ce,de->cd", grad_mod_clip, mod_low.astype(jnp.float32), precision=precise
    )
    grad_silu = jnp.concatenate(
        list(doubling_gather(grad_silu_part, "seq", seq_count, seq_rank)), axis=1
    )
    time_grad = jax.vjp(jax.nn.silu, time_emb)[1](grad_silu)[0]
    totals = (
        reduce_rows(grad_qkv_local.astype(jnp.bfloat16), 1).astype(jnp.float32),
        reduce_rows(grad_out_local.astype(jnp.bfloat16), 0).astype(jnp.float32),
        reduce_rows(grad_up_local.astype(jnp.bfloat16), 0).astype(jnp.float32),
        reduce_rows(grad_down_local.astype(jnp.bfloat16), 0).astype(jnp.float32),
        grad_mod_share,
        grad_bias_share,
    )
    masters = (w_qkv, w_out, w_up, w_down, w_mod, b_mod)
    moments = (mom_qkv, mom_out, mom_up, mom_down, mom_mod, mom_bias)
    seconds = (var_qkv, var_out, var_up, var_down, var_mod, var_bias)
    new_moments = []
    new_seconds = []
    directions = []
    weight_sums = []
    update_sums = []
    for param in range(6):
        moment_new, second_new, direction = adam_direction(
            masters[param], moments[param], seconds[param], totals[param]
        )
        sum_axes = (1, 2) if param == 0 else None
        new_moments.append(moment_new)
        new_seconds.append(second_new)
        directions.append(direction)
        weight_sums.append(jnp.sum(masters[param] * masters[param], axis=sum_axes, keepdims=True))
        update_sums.append(jnp.sum(direction * direction, axis=sum_axes, keepdims=True))
    new_masters = []
    for param in range(6):
        pair = butterfly_sum(
            jnp.concatenate([weight_sums[param], update_sums[param]], axis=-1), "seq", seq_count
        )
        ratio = jnp.sqrt(pair[..., :1]) * lax.rsqrt(pair[..., 1:] + 1e-06)
        new_masters.append(masters[param] - step_rate * ratio * directions[param])
    return (
        result.astype(jnp.bfloat16),
        input_grad,
        time_grad,
        totals[0],
        new_masters[0],
        new_moments[0],
        new_seconds[0],
        totals[1],
        new_masters[1],
        new_moments[1],
        new_seconds[1],
        totals[2],
        new_masters[2],
        new_moments[2],
        new_seconds[2],
        totals[3],
        new_masters[3],
        new_moments[3],
        new_seconds[3],
        totals[4],
        new_masters[4],
        new_moments[4],
        new_seconds[4],
        totals[5],
        new_masters[5],
        new_moments[5],
        new_seconds[5],
    )


def solution(mesh):
    devices = mesh.devices
    chip_mesh = Mesh(
        devices.reshape(devices.shape[0] // 2, 2, devices.shape[1]), ("z", "core", "seq")
    )
    return jax.shard_map(
        local,
        mesh=chip_mesh,
        in_specs=(
            P(("z", "core", "seq"), None),
            P(("z", "core", "seq"), None),
            P(("z", "core"), None),
            P(("z", "core"), None),
            P(("z", "core"), None),
            P(None, "seq", None),
            P(None, "seq", None),
            P(None, "seq", None),
            P("seq", None),
            P("seq", None),
            P("seq", None),
            P("seq", None),
            P("seq", None),
            P("seq", None),
            P("seq", None),
            P("seq", None),
            P("seq", None),
            P("seq", None),
            P("seq", None),
            P("seq", None),
            P("seq"),
            P("seq"),
            P("seq"),
        ),
        out_specs=(
            P(("z", "core", "seq"), None),
            P(("z", "core", "seq"), None),
            P(("z", "core"), None),
            P(None, "seq", None),
            P(None, "seq", None),
            P(None, "seq", None),
            P(None, "seq", None),
            P("seq", None),
            P("seq", None),
            P("seq", None),
            P("seq", None),
            P("seq", None),
            P("seq", None),
            P("seq", None),
            P("seq", None),
            P("seq", None),
            P("seq", None),
            P("seq", None),
            P("seq", None),
            P("seq", None),
            P("seq", None),
            P("seq", None),
            P("seq", None),
            P("seq"),
            P("seq"),
            P("seq"),
            P("seq"),
        ),
        check_vma=False,
    )
```

```python
import jax
import jax.numpy as jnp
from jax import lax
from jax.sharding import Mesh, PartitionSpec as P

HEAD_DIM = 64


precise = lax.Precision.HIGHEST
norm_eps = 1e-06
masked_score = -1e30
beta_one = 0.9
beta_two = 0.999
adam_eps = 1e-08
weight_decay = 0.01
step_rate = 1.0
step_count = 10


def layer_norm(values):
    center = values - jnp.mean(values, axis=-1, keepdims=True)
    spread = jnp.mean(center * center, axis=-1, keepdims=True)
    return center * lax.rsqrt(spread + norm_eps)


def modulate(values, shift, scale):
    return layer_norm(values) * (1.0 + scale) + shift


def gelu_tanh(values):
    return jax.nn.gelu(values, approximate=True)


def rotate(values, places, turn_sign):
    frame_count = values.shape[0]
    half_dim = HEAD_DIM // 2
    exponent = jnp.arange(half_dim, dtype=jnp.float32) * (-2.0 / HEAD_DIM)
    frequency = jnp.power(jnp.float32(10000.0), exponent)
    angles = places.astype(jnp.float32)[:, None] * frequency[None, :]
    cos_table = jnp.cos(angles)[:, None, :]
    sin_table = turn_sign * jnp.sin(angles)[:, None, :]
    paired = values.reshape(frame_count, values.shape[1] // HEAD_DIM, half_dim, 2)
    even_part = paired[..., 0]
    odd_part = paired[..., 1]
    turned = jnp.stack(
        [
            even_part * cos_table - odd_part * sin_table,
            odd_part * cos_table + even_part * sin_table,
        ],
        axis=-1,
    )
    return turned.reshape(frame_count, values.shape[1])


def clip_tables(lengths, padding, frame_ids):
    starts = jnp.cumsum(lengths) - lengths
    finish = starts + lengths
    inside = (frame_ids[:, None] >= starts[None, :]) & (frame_ids[:, None] < finish[None, :])
    clip_ids = jnp.arange(lengths.shape[0], dtype=jnp.int32)
    owners = jnp.sum(jnp.where(inside, clip_ids[None, :], 0), axis=1)
    begins = jnp.sum(jnp.where(inside, starts[None, :], 0), axis=1)
    kept_len = jnp.maximum(lengths - padding, 1)
    limits = jnp.sum(jnp.where(inside, kept_len[None, :], 0), axis=1)
    places = frame_ids - begins
    return (inside.astype(jnp.float32), owners, places, places < limits)


def key_window(block_index, block_rows, span, frame_count):
    return jnp.clip(block_index * block_rows - (span - block_rows) // 2, 0, frame_count - span)


def block_inputs(queries, keys_all, values, owners, usable, block_index, block_rows, span):
    frame_count, columns = queries.shape
    heads_here = columns // HEAD_DIM
    row_start = block_index * block_rows
    window = key_window(block_index, block_rows, span, frame_count)
    query_rows = lax.dynamic_slice_in_dim(queries, row_start, block_rows, 0).reshape(
        block_rows, heads_here, HEAD_DIM
    )
    keys_win = keys_all.reshape(span, heads_here, HEAD_DIM)
    values_win = values.reshape(span, heads_here, HEAD_DIM)
    query_owner = lax.dynamic_slice_in_dim(owners, row_start, block_rows, 0)
    score_scale = HEAD_DIM ** (-0.5)
    scores = (
        jnp.einsum("qhd,khd->hqk", query_rows, keys_win, preferred_element_type=jnp.float32)
        * score_scale
    )
    allowed = (query_owner[:, None] == owners[None, :]) & usable[None, :]
    masked = jnp.where(allowed[None], scores, masked_score)
    return (row_start, window, query_rows, keys_win, values_win, masked)


def attend_forward(queries, keys_all, values, owners, usable, span):
    frame_count, columns = queries.shape
    block_rows = min(512, frame_count)

    def one_block(block_index):
        row_start, window, query_rows, keys_win, values_win, masked = block_inputs(
            queries, keys_all, values, owners, usable, block_index, block_rows, span
        )
        row_max = jnp.max(masked, axis=-1, keepdims=True)
        row_total = jnp.sum(jnp.exp(masked - row_max), axis=-1, keepdims=True)
        log_total = row_max + jnp.log(row_total)
        probs_low = jnp.exp(masked - log_total).astype(jnp.bfloat16)
        attended = jnp.einsum(
            "hqk,khd->qhd", probs_low, values_win, preferred_element_type=jnp.float32
        )
        return (attended.astype(jnp.bfloat16).reshape(block_rows, columns), log_total)

    outcome, log_totals = lax.map(one_block, jnp.arange(frame_count // block_rows, dtype=jnp.int32))
    return (outcome.reshape(frame_count, columns), log_totals)


def attend_backward(queries, keys_all, values, grad_attended, log_totals, owners, usable, span):
    frame_count, columns = queries.shape
    heads_here = columns // HEAD_DIM
    block_rows = min(512, frame_count)
    score_scale = HEAD_DIM ** (-0.5)

    def one_block(sums, block_data):
        key_sum, value_sum = sums
        block_index, log_total = block_data
        row_start, window, query_rows, keys_win, values_win, masked = block_inputs(
            queries, keys_all, values, owners, usable, block_index, block_rows, span
        )
        grad_rows = lax.dynamic_slice_in_dim(grad_attended, row_start, block_rows, 0).reshape(
            block_rows, heads_here, HEAD_DIM
        )
        probs_full = jnp.exp(masked - log_total)
        probs_low = probs_full.astype(jnp.bfloat16)
        grad_probs = jnp.einsum(
            "qhd,khd->hqk", grad_rows, values_win, preferred_element_type=jnp.float32
        )
        row_delta = jnp.sum(probs_full * grad_probs, axis=-1, keepdims=True)
        grad_scores = (probs_full * (grad_probs - row_delta)).astype(jnp.bfloat16)
        grad_query = (
            jnp.einsum("hqk,khd->qhd", grad_scores, keys_win, preferred_element_type=jnp.float32)
            * score_scale
        )
        grad_key = (
            jnp.einsum("hqk,qhd->khd", grad_scores, query_rows, preferred_element_type=jnp.float32)
            * score_scale
        )
        grad_value = jnp.einsum(
            "hqk,qhd->khd", probs_low, grad_rows, preferred_element_type=jnp.float32
        )
        old_keys = key_sum
        key_sum = old_keys + grad_key.reshape(span, columns)
        old_values = value_sum
        value_sum = old_values + grad_value.reshape(span, columns)
        return ((key_sum, value_sum), grad_query.astype(jnp.bfloat16).reshape(block_rows, columns))

    zeros = jnp.zeros((frame_count, columns), jnp.float32)
    indices = jnp.arange(frame_count // block_rows, dtype=jnp.int32)
    (key_sum, value_sum), grad_queries = lax.scan(one_block, (zeros, zeros), (indices, log_totals))
    return (
        grad_queries.reshape(frame_count, columns),
        key_sum.astype(jnp.bfloat16),
        value_sum.astype(jnp.bfloat16),
    )


def butterfly_sum(values, axes, size):
    step = 1
    while step < size:
        values = values + lax.ppermute(values, axes, [(i, i ^ step) for i in range(size)])
        step *= 2
    return values


def doubling_gather(values, axes, size, index):
    blocks = values[None]
    step = 1
    while step < size:
        other = lax.ppermute(blocks, axes, [(i, i ^ step) for i in range(size)])
        low_side = (index // step) % 2 == 0
        blocks = jnp.concatenate(
            [jnp.where(low_side, blocks, other), jnp.where(low_side, other, blocks)], axis=0
        )
        step *= 2
    return blocks


def gather_rows(shard, row_axis):
    half = shard.shape[row_axis] // 2
    core = lax.axis_index("core")
    piece = lax.dynamic_slice_in_dim(shard, core * half, half, row_axis)
    return lax.all_gather(piece, ("seq", "core"), axis=row_axis, tiled=True)


def halving_sum(values, axis_name, size):
    index = lax.axis_index(axis_name)
    total = values.astype(jnp.float32)
    step = 1
    last = total.ndim - 1
    while step < size:
        half = total.shape[-1] // 2
        high_bit = (index // step) % 2
        keep = lax.dynamic_slice_in_dim(total, high_bit * half, half, last)
        send = lax.dynamic_slice_in_dim(total, (1 - high_bit) * half, half, last)
        total = keep + lax.ppermute(
            send.astype(jnp.bfloat16), axis_name, [(i, i ^ step) for i in range(size)]
        ).astype(jnp.float32)
        step *= 2
    blocks = total.astype(jnp.bfloat16)
    step = size // 2
    while step >= 1:
        other = lax.ppermute(blocks, axis_name, [(i, i ^ step) for i in range(size)])
        low_side = (index // step) % 2 == 0
        blocks = jnp.concatenate(
            [jnp.where(low_side, blocks, other), jnp.where(low_side, other, blocks)], axis=-1
        )
        step //= 2
    return blocks


def reduce_rows(partial, row_axis):
    piece = lax.psum_scatter(partial, ("seq", "core"), scatter_dimension=row_axis, tiled=True)
    piece = halving_sum(piece, "z", lax.axis_size("z"))
    other = lax.ppermute(piece, "core", [(0, 1), (1, 0)])
    first = lax.axis_index("core") == 0
    return jnp.concatenate(
        [jnp.where(first, piece, other), jnp.where(first, other, piece)], axis=row_axis
    )


def adam_direction(weight, moment, second, grad):
    moment_new = beta_one * moment + (1.0 - beta_one) * grad
    second_new = beta_two * second + (1.0 - beta_two) * grad * grad
    corrected = moment_new / (1.0 - beta_one**step_count)
    scaled = second_new / (1.0 - beta_two**step_count)
    direction = corrected / (jnp.sqrt(scaled) + adam_eps) + weight_decay * weight
    return (moment_new, second_new, direction)


def local(
    frames,
    out_grad,
    time_emb,
    clip_len,
    pad_len,
    w_qkv,
    mom_qkv,
    var_qkv,
    w_out,
    mom_out,
    var_out,
    w_up,
    mom_up,
    var_up,
    w_down,
    mom_down,
    var_down,
    w_mod,
    mom_mod,
    var_mod,
    b_mod,
    mom_bias,
    var_bias,
):
    seq_count = lax.axis_size("seq")
    seq_rank = lax.axis_index("seq")
    frame_rows = frames.shape[0]
    group_frames = frame_rows * seq_count
    dp_count = lax.axis_size(("z", "core"))
    dp_rank = lax.axis_index(("z", "core"))
    qkv_full, out_full, up_full, down_full = (
        gather_rows(w_qkv.astype(jnp.bfloat16), 1),
        gather_rows(w_out.astype(jnp.bfloat16), 0),
        gather_rows(w_up.astype(jnp.bfloat16), 0),
        gather_rows(w_down.astype(jnp.bfloat16), 0),
    )
    bias_full = doubling_gather(b_mod.astype(jnp.bfloat16), "seq", seq_count, seq_rank).reshape(-1)
    mod_low = w_mod.astype(jnp.bfloat16)
    mod_rows_here = w_mod.shape[0]
    mod_first = seq_rank * mod_rows_here
    inside_all, owners_all, places_all, usable_all = clip_tables(
        clip_len[0], pad_len[0], jnp.arange(group_frames, dtype=jnp.int32)
    )
    row_first = seq_rank * frame_rows
    inside_own = lax.dynamic_slice_in_dim(inside_all, row_first, frame_rows, 0)
    places_own = lax.dynamic_slice_in_dim(places_all, row_first, frame_rows, 0)
    silu_low = jax.nn.silu(time_emb).astype(jnp.bfloat16)
    silu_part = lax.dynamic_slice_in_dim(silu_low, mod_first, mod_rows_here, 1)
    modulation = butterfly_sum(
        jnp.dot(silu_part, mod_low, preferred_element_type=jnp.float32), "seq", seq_count
    ) + bias_full.astype(jnp.float32)
    mod_rows = jnp.dot(inside_own, modulation, precision=precise)
    shift_attn, scale_attn, gate_attn, shift_ff, scale_ff, gate_ff = jnp.split(mod_rows, 6, axis=1)
    inputs = frames.astype(jnp.float32)
    hidden, attn_norm_back = jax.vjp(modulate, inputs, shift_attn, scale_attn)
    hidden_low = hidden.astype(jnp.bfloat16)
    query_lin = jnp.dot(hidden_low, qkv_full[0], preferred_element_type=jnp.float32)
    key_lin = jnp.dot(hidden_low, qkv_full[1], preferred_element_type=jnp.float32)
    value_lin = jnp.dot(hidden_low, qkv_full[2], preferred_element_type=jnp.float32)
    query_send = rotate(query_lin, places_own, 1.0).astype(jnp.bfloat16)
    key_send = rotate(key_lin, places_own, 1.0).astype(jnp.bfloat16)
    value_send = value_lin.astype(jnp.bfloat16)
    query_heads, key_heads, value_heads = (
        lax.all_to_all(query_send, "seq", split_axis=1, concat_axis=0, tiled=True),
        lax.all_to_all(key_send, "seq", split_axis=1, concat_axis=0, tiled=True),
        lax.all_to_all(value_send, "seq", split_axis=1, concat_axis=0, tiled=True),
    )
    attended_heads, log_totals = attend_forward(
        query_heads, key_heads, value_heads, owners_all, usable_all, group_frames
    )
    attended = lax.all_to_all(attended_heads, "seq", split_axis=0, concat_axis=1, tiled=True)
    attn_proj = jnp.dot(attended, out_full, preferred_element_type=jnp.float32)
    mid = inputs + gate_attn * attn_proj
    hidden_ff, ff_norm_back = jax.vjp(modulate, mid, shift_ff, scale_ff)
    hidden_ff_low = hidden_ff.astype(jnp.bfloat16)
    pre_act = jnp.dot(hidden_ff_low, up_full, preferred_element_type=jnp.float32)
    active, gelu_back = jax.vjp(gelu_tanh, pre_act)
    active_low = active.astype(jnp.bfloat16)
    ff_proj = jnp.dot(active_low, down_full, preferred_element_type=jnp.float32)
    result = mid + gate_ff * ff_proj
    grad_result = out_grad.astype(jnp.float32)
    grad_gate_ff = grad_result * ff_proj
    grad_ff = (grad_result * gate_ff).astype(jnp.bfloat16)
    grad_down_local = jnp.einsum(
        "nf,nd->fd", active_low, grad_ff, preferred_element_type=jnp.float32
    )
    grad_active = jnp.einsum("nd,fd->nf", grad_ff, down_full, preferred_element_type=jnp.float32)
    (grad_pre,) = gelu_back(grad_active)
    grad_pre_low = grad_pre.astype(jnp.bfloat16)
    grad_up_local = jnp.einsum(
        "nd,nf->df", hidden_ff_low, grad_pre_low, preferred_element_type=jnp.float32
    )
    grad_hidden_ff = jnp.einsum(
        "nf,df->nd", grad_pre_low, up_full, preferred_element_type=jnp.float32
    )
    grad_mid_norm, grad_shift_ff, grad_scale_ff = ff_norm_back(grad_hidden_ff)
    grad_mid = grad_result + grad_mid_norm
    grad_gate_attn = grad_mid * attn_proj
    grad_proj = (grad_mid * gate_attn).astype(jnp.bfloat16)
    grad_out_local = jnp.einsum(
        "nd,ne->de", attended, grad_proj, preferred_element_type=jnp.float32
    )
    grad_attended = jnp.einsum(
        "ne,de->nd", grad_proj, out_full, preferred_element_type=jnp.float32
    ).astype(jnp.bfloat16)
    grad_heads = lax.all_to_all(grad_attended, "seq", split_axis=1, concat_axis=0, tiled=True)
    grad_query_heads, grad_key_heads, grad_value_heads = attend_backward(
        query_heads,
        key_heads,
        value_heads,
        grad_heads,
        log_totals,
        owners_all,
        usable_all,
        group_frames,
    )
    grad_query_rows, grad_key_rows, grad_value_rows = (
        lax.all_to_all(grad_query_heads, "seq", split_axis=0, concat_axis=1, tiled=True),
        lax.all_to_all(grad_key_heads, "seq", split_axis=0, concat_axis=1, tiled=True),
        lax.all_to_all(grad_value_heads, "seq", split_axis=0, concat_axis=1, tiled=True),
    )
    grad_query_lin = rotate(grad_query_rows.astype(jnp.float32), places_own, -1.0).astype(
        jnp.bfloat16
    )
    grad_key_lin = rotate(grad_key_rows.astype(jnp.float32), places_own, -1.0).astype(jnp.bfloat16)
    grad_qkv_local = jnp.stack(
        [
            jnp.einsum("nd,ne->de", hidden_low, grad_query_lin, preferred_element_type=jnp.float32),
            jnp.einsum("nd,ne->de", hidden_low, grad_key_lin, preferred_element_type=jnp.float32),
            jnp.einsum(
                "nd,ne->de", hidden_low, grad_value_rows, preferred_element_type=jnp.float32
            ),
        ]
    )
    grad_hidden = jnp.einsum(
        "ne,de->nd", grad_query_lin, qkv_full[0], preferred_element_type=jnp.float32
    )
    grad_hidden = grad_hidden + jnp.einsum(
        "ne,de->nd", grad_key_lin, qkv_full[1], preferred_element_type=jnp.float32
    )
    grad_hidden = grad_hidden + jnp.einsum(
        "ne,de->nd", grad_value_rows, qkv_full[2], preferred_element_type=jnp.float32
    )
    grad_input_norm, grad_shift_attn, grad_scale_attn = attn_norm_back(grad_hidden)
    input_grad = grad_mid + grad_input_norm
    grad_mod_rows = jnp.concatenate(
        [
            grad_shift_attn,
            grad_scale_attn,
            grad_gate_attn,
            grad_shift_ff,
            grad_scale_ff,
            grad_gate_ff,
        ],
        axis=1,
    )
    grad_mod_clip = butterfly_sum(
        jnp.einsum("nc,ne->ce", inside_own, grad_mod_rows, precision=precise), "seq", seq_count
    )
    grad_mod_all = doubling_gather(grad_mod_clip, ("z", "core"), dp_count, dp_rank).reshape(
        -1, grad_mod_clip.shape[1]
    )
    silu_all = doubling_gather(silu_part, ("z", "core"), dp_count, dp_rank).reshape(
        -1, silu_part.shape[1]
    )
    bias_cols = b_mod.shape[0]
    grad_bias_share = jnp.sum(
        lax.dynamic_slice_in_dim(grad_mod_all, seq_rank * bias_cols, bias_cols, 1), axis=0
    )
    grad_mod_share = jnp.einsum(
        "cd,ce->de", silu_all.astype(jnp.float32), grad_mod_all, precision=precise
    )
    grad_silu_part = jnp.einsum(
        "ce,de->cd", grad_mod_clip, mod_low.astype(jnp.float32), precision=precise
    )
    grad_silu = jnp.concatenate(
        list(doubling_gather(grad_silu_part, "seq", seq_count, seq_rank)), axis=1
    )
    time_grad = jax.vjp(jax.nn.silu, time_emb)[1](grad_silu)[0]
    totals = (
        jnp.stack(
            [reduce_rows(grad_qkv_local[part].astype(jnp.bfloat16), 0) for part in range(3)]
        ).astype(jnp.float32),
        reduce_rows(grad_out_local.astype(jnp.bfloat16), 0).astype(jnp.float32),
        reduce_rows(grad_up_local.astype(jnp.bfloat16), 0).astype(jnp.float32),
        reduce_rows(grad_down_local.astype(jnp.bfloat16), 0).astype(jnp.float32),
        grad_mod_share,
        grad_bias_share,
    )
    masters = (w_qkv, w_out, w_up, w_down, w_mod, b_mod)
    moments = (mom_qkv, mom_out, mom_up, mom_down, mom_mod, mom_bias)
    seconds = (var_qkv, var_out, var_up, var_down, var_mod, var_bias)
    new_moments = []
    new_seconds = []
    directions = []
    weight_sums = []
    update_sums = []
    for param in range(6):
        moment_new, second_new, direction = adam_direction(
            masters[param], moments[param], seconds[param], totals[param]
        )
        sum_axes = (1, 2) if param == 0 else None
        new_moments.append(moment_new)
        new_seconds.append(second_new)
        directions.append(direction)
        weight_sums.append(jnp.sum(masters[param] * masters[param], axis=sum_axes, keepdims=True))
        update_sums.append(jnp.sum(direction * direction, axis=sum_axes, keepdims=True))
    new_masters = []
    for param in range(6):
        pair = butterfly_sum(
            jnp.concatenate([weight_sums[param], update_sums[param]], axis=-1), "seq", seq_count
        )
        ratio = jnp.sqrt(pair[..., :1]) * lax.rsqrt(pair[..., 1:] + 1e-06)
        new_masters.append(masters[param] - step_rate * ratio * directions[param])
    return (
        result.astype(jnp.bfloat16),
        input_grad,
        time_grad,
        totals[0],
        new_masters[0],
        new_moments[0],
        new_seconds[0],
        totals[1],
        new_masters[1],
        new_moments[1],
        new_seconds[1],
        totals[2],
        new_masters[2],
        new_moments[2],
        new_seconds[2],
        totals[3],
        new_masters[3],
        new_moments[3],
        new_seconds[3],
        totals[4],
        new_masters[4],
        new_moments[4],
        new_seconds[4],
        totals[5],
        new_masters[5],
        new_moments[5],
        new_seconds[5],
    )


def solution(mesh):
    devices = mesh.devices
    chip_mesh = Mesh(
        devices.reshape(devices.shape[0] // 2, 2, devices.shape[1]), ("z", "core", "seq")
    )
    return jax.shard_map(
        local,
        mesh=chip_mesh,
        in_specs=(
            P(("z", "core", "seq"), None),
            P(("z", "core", "seq"), None),
            P(("z", "core"), None),
            P(("z", "core"), None),
            P(("z", "core"), None),
            P(None, "seq", None),
            P(None, "seq", None),
            P(None, "seq", None),
            P("seq", None),
            P("seq", None),
            P("seq", None),
            P("seq", None),
            P("seq", None),
            P("seq", None),
            P("seq", None),
            P("seq", None),
            P("seq", None),
            P("seq", None),
            P("seq", None),
            P("seq", None),
            P("seq"),
            P("seq"),
            P("seq"),
        ),
        out_specs=(
            P(("z", "core", "seq"), None),
            P(("z", "core", "seq"), None),
            P(("z", "core"), None),
            P(None, "seq", None),
            P(None, "seq", None),
            P(None, "seq", None),
            P(None, "seq", None),
            P("seq", None),
            P("seq", None),
            P("seq", None),
            P("seq", None),
            P("seq", None),
            P("seq", None),
            P("seq", None),
            P("seq", None),
            P("seq", None),
            P("seq", None),
            P("seq", None),
            P("seq", None),
            P("seq", None),
            P("seq", None),
            P("seq", None),
            P("seq", None),
            P("seq"),
            P("seq"),
            P("seq"),
            P("seq"),
        ),
        check_vma=False,
    )
```

```python
import jax
import jax.numpy as jnp
from jax import lax
from jax.sharding import Mesh, PartitionSpec as P

HEAD_DIM = 64


precise = lax.Precision.HIGHEST
norm_eps = 1e-06
masked_score = -1e30
beta_one = 0.9
beta_two = 0.999
adam_eps = 1e-08
weight_decay = 0.01
step_rate = 1.0
step_count = 10


def layer_norm(values):
    center = values - jnp.mean(values, axis=-1, keepdims=True)
    spread = jnp.mean(center * center, axis=-1, keepdims=True)
    return center * lax.rsqrt(spread + norm_eps)


def modulate(values, shift, scale):
    return layer_norm(values) * (1.0 + scale) + shift


def gelu_tanh(values):
    return jax.nn.gelu(values, approximate=True)


def rotate(values, places, turn_sign):
    frame_count = values.shape[0]
    half_dim = HEAD_DIM // 2
    exponent = jnp.arange(half_dim, dtype=jnp.float32) * (-2.0 / HEAD_DIM)
    frequency = jnp.power(jnp.float32(10000.0), exponent)
    angles = places.astype(jnp.float32)[:, None] * frequency[None, :]
    cos_table = jnp.cos(angles)[:, None, :]
    sin_table = turn_sign * jnp.sin(angles)[:, None, :]
    paired = values.reshape(frame_count, values.shape[1] // HEAD_DIM, half_dim, 2)
    even_part = paired[..., 0]
    odd_part = paired[..., 1]
    turned = jnp.stack(
        [
            even_part * cos_table - odd_part * sin_table,
            odd_part * cos_table + even_part * sin_table,
        ],
        axis=-1,
    )
    return turned.reshape(frame_count, values.shape[1])


def clip_tables(lengths, padding, frame_ids):
    starts = jnp.cumsum(lengths) - lengths
    finish = starts + lengths
    inside = (frame_ids[:, None] >= starts[None, :]) & (frame_ids[:, None] < finish[None, :])
    clip_ids = jnp.arange(lengths.shape[0], dtype=jnp.int32)
    owners = jnp.sum(jnp.where(inside, clip_ids[None, :], 0), axis=1)
    begins = jnp.sum(jnp.where(inside, starts[None, :], 0), axis=1)
    kept_len = jnp.maximum(lengths - padding, 1)
    limits = jnp.sum(jnp.where(inside, kept_len[None, :], 0), axis=1)
    places = frame_ids - begins
    return (inside.astype(jnp.float32), owners, places, places < limits)


def key_window(block_index, block_rows, span, frame_count):
    return jnp.clip(block_index * block_rows - (span - block_rows) // 2, 0, frame_count - span)


def block_inputs(queries, keys_all, values, owners, usable, block_index, block_rows, span):
    frame_count, columns = queries.shape
    heads_here = columns // HEAD_DIM
    row_start = block_index * block_rows
    window = key_window(block_index, block_rows, span, frame_count)
    query_rows = lax.dynamic_slice_in_dim(queries, row_start, block_rows, 0).reshape(
        block_rows, heads_here, HEAD_DIM
    )
    keys_win = keys_all.reshape(span, heads_here, HEAD_DIM)
    values_win = values.reshape(span, heads_here, HEAD_DIM)
    query_owner = lax.dynamic_slice_in_dim(owners, row_start, block_rows, 0)
    score_scale = HEAD_DIM ** (-0.5)
    scores = (
        jnp.einsum("qhd,khd->hqk", query_rows, keys_win, preferred_element_type=jnp.float32)
        * score_scale
    )
    allowed = (query_owner[:, None] == owners[None, :]) & usable[None, :]
    masked = jnp.where(allowed[None], scores, masked_score)
    return (row_start, window, query_rows, keys_win, values_win, masked)


def attend_forward(queries, keys_all, values, owners, usable, span):
    frame_count, columns = queries.shape
    block_rows = min(512, frame_count)

    def one_block(block_index):
        row_start, window, query_rows, keys_win, values_win, masked = block_inputs(
            queries, keys_all, values, owners, usable, block_index, block_rows, span
        )
        row_max = jnp.max(masked, axis=-1, keepdims=True)
        row_total = jnp.sum(jnp.exp(masked - row_max), axis=-1, keepdims=True)
        log_total = row_max + jnp.log(row_total)
        probs_low = jnp.exp(masked - log_total).astype(jnp.bfloat16)
        attended = jnp.einsum(
            "hqk,khd->qhd", probs_low, values_win, preferred_element_type=jnp.float32
        )
        return (attended.astype(jnp.bfloat16).reshape(block_rows, columns), log_total)

    outcome, log_totals = lax.map(one_block, jnp.arange(frame_count // block_rows, dtype=jnp.int32))
    return (outcome.reshape(frame_count, columns), log_totals)


def attend_backward(queries, keys_all, values, grad_attended, log_totals, owners, usable, span):
    frame_count, columns = queries.shape
    heads_here = columns // HEAD_DIM
    block_rows = min(512, frame_count)
    score_scale = HEAD_DIM ** (-0.5)

    def one_block(sums, block_data):
        key_sum, value_sum = sums
        block_index, log_total = block_data
        row_start, window, query_rows, keys_win, values_win, masked = block_inputs(
            queries, keys_all, values, owners, usable, block_index, block_rows, span
        )
        grad_rows = lax.dynamic_slice_in_dim(grad_attended, row_start, block_rows, 0).reshape(
            block_rows, heads_here, HEAD_DIM
        )
        probs_full = jnp.exp(masked - log_total)
        probs_low = probs_full.astype(jnp.bfloat16)
        grad_probs = jnp.einsum(
            "qhd,khd->hqk", grad_rows, values_win, preferred_element_type=jnp.float32
        )
        row_delta = jnp.sum(probs_full * grad_probs, axis=-1, keepdims=True)
        grad_scores = (probs_full * (grad_probs - row_delta)).astype(jnp.bfloat16)
        grad_query = (
            jnp.einsum("hqk,khd->qhd", grad_scores, keys_win, preferred_element_type=jnp.float32)
            * score_scale
        )
        grad_key = (
            jnp.einsum("hqk,qhd->khd", grad_scores, query_rows, preferred_element_type=jnp.float32)
            * score_scale
        )
        grad_value = jnp.einsum(
            "hqk,qhd->khd", probs_low, grad_rows, preferred_element_type=jnp.float32
        )
        old_keys = key_sum
        key_sum = old_keys + grad_key.reshape(span, columns)
        old_values = value_sum
        value_sum = old_values + grad_value.reshape(span, columns)
        return ((key_sum, value_sum), grad_query.astype(jnp.bfloat16).reshape(block_rows, columns))

    zeros = jnp.zeros((frame_count, columns), jnp.float32)
    indices = jnp.arange(frame_count // block_rows, dtype=jnp.int32)
    (key_sum, value_sum), grad_queries = lax.scan(one_block, (zeros, zeros), (indices, log_totals))
    return (
        grad_queries.reshape(frame_count, columns),
        key_sum.astype(jnp.bfloat16),
        value_sum.astype(jnp.bfloat16),
    )


def butterfly_sum(values, axes, size):
    step = 1
    while step < size:
        values = values + lax.ppermute(values, axes, [(i, i ^ step) for i in range(size)])
        step *= 2
    return values


def doubling_gather(values, axes, size, index):
    blocks = values[None]
    step = 1
    while step < size:
        other = lax.ppermute(blocks, axes, [(i, i ^ step) for i in range(size)])
        low_side = (index // step) % 2 == 0
        blocks = jnp.concatenate(
            [jnp.where(low_side, blocks, other), jnp.where(low_side, other, blocks)], axis=0
        )
        step *= 2
    return blocks


def gather_rows(shard, row_axis):
    half = shard.shape[row_axis] // 2
    core = lax.axis_index("core")
    piece = lax.dynamic_slice_in_dim(shard, core * half, half, row_axis)
    return lax.all_gather(piece, ("seq", "core"), axis=row_axis, tiled=True)


def halving_sum(values, axis_name, size):
    index = lax.axis_index(axis_name)
    total = values.astype(jnp.float32)
    step = 1
    while step < size:
        half = total.shape[-1] // 2
        low_side = (index // step) % 2 == 0
        keep = jnp.where(low_side, total[..., :half], total[..., half:])
        send = jnp.where(low_side, total[..., half:], total[..., :half]).astype(jnp.bfloat16)
        total = keep + lax.ppermute(send, axis_name, [(i, i ^ step) for i in range(size)]).astype(
            jnp.float32
        )
        step *= 2
    blocks = total.astype(jnp.bfloat16)
    step = size // 2
    while step >= 1:
        other = lax.ppermute(blocks, axis_name, [(i, i ^ step) for i in range(size)])
        low_side = (index // step) % 2 == 0
        blocks = jnp.concatenate(
            [jnp.where(low_side, blocks, other), jnp.where(low_side, other, blocks)], axis=-1
        )
        step //= 2
    return blocks


def reduce_rows(partial, row_axis):
    piece = lax.psum_scatter(partial, ("seq", "core"), scatter_dimension=row_axis, tiled=True)
    piece = halving_sum(piece, "z", lax.axis_size("z"))
    other = lax.ppermute(piece, "core", [(0, 1), (1, 0)])
    first = lax.axis_index("core") == 0
    return jnp.concatenate(
        [jnp.where(first, piece, other), jnp.where(first, other, piece)], axis=row_axis
    )


def gather_batch(shards):
    core = lax.axis_index("core")
    flat = []
    for shard in shards:
        half = shard.shape[0] // 2
        flat.append(lax.dynamic_slice_in_dim(shard, core * half, half, 0).reshape(-1))
    blocks = lax.all_gather(jnp.concatenate(flat), ("seq", "core"), axis=0, tiled=False)
    fulls = []
    offset = 0
    for shard, piece in zip(shards, flat):
        fulls.append(
            blocks[:, offset : offset + piece.size].reshape(-1, shard.shape[1])
        )
        offset += piece.size
    return fulls


def reduce_batch(partials):
    groups = lax.axis_size("seq") * 2
    flat = jnp.concatenate([part.reshape(groups, -1) for part in partials], axis=1)
    flat = flat.reshape(groups * 8, -1)
    piece = lax.psum_scatter(flat, ("seq", "core"), scatter_dimension=0, tiled=True).reshape(1, -1)
    piece = halving_sum(piece, "z", lax.axis_size("z"))
    other = lax.ppermute(piece, "core", [(0, 1), (1, 0)])
    first = lax.axis_index("core") == 0
    low = jnp.where(first, piece, other)
    high = jnp.where(first, other, piece)
    shares = []
    offset = 0
    for part in partials:
        size = part.size // groups
        rows = (-1, part.shape[1])
        shares.append(
            jnp.concatenate(
                [
                    low[:, offset : offset + size].reshape(rows),
                    high[:, offset : offset + size].reshape(rows),
                ],
                axis=0,
            )
        )
        offset += size
    return shares


def lamb_update(weight, moment, second, grad, sum_axes, seq_count):
    moment_new, second_new, direction = adam_direction(weight, moment, second, grad)
    sums = jnp.concatenate(
        [
            jnp.sum(weight * weight, axis=sum_axes, keepdims=True),
            jnp.sum(direction * direction, axis=sum_axes, keepdims=True),
        ],
        axis=-1,
    )
    sums = butterfly_sum(sums, "seq", seq_count)
    ratio = jnp.sqrt(sums[..., :1]) * lax.rsqrt(sums[..., 1:] + 1e-06)
    return (weight - step_rate * ratio * direction, moment_new, second_new)


def adam_direction(weight, moment, second, grad):
    moment_new = beta_one * moment + (1.0 - beta_one) * grad
    second_new = beta_two * second + (1.0 - beta_two) * grad * grad
    corrected = moment_new / (1.0 - beta_one**step_count)
    scaled = second_new / (1.0 - beta_two**step_count)
    direction = corrected / (jnp.sqrt(scaled) + adam_eps) + weight_decay * weight
    return (moment_new, second_new, direction)


def local(
    frames,
    out_grad,
    time_emb,
    clip_len,
    pad_len,
    w_qkv,
    mom_qkv,
    var_qkv,
    w_out,
    mom_out,
    var_out,
    w_up,
    mom_up,
    var_up,
    w_down,
    mom_down,
    var_down,
    w_mod,
    mom_mod,
    var_mod,
    b_mod,
    mom_bias,
    var_bias,
):
    seq_count = lax.axis_size("seq")
    seq_rank = lax.axis_index("seq")
    frame_rows = frames.shape[0]
    group_frames = frame_rows * seq_count
    dp_count = lax.axis_size(("z", "core"))
    dp_rank = lax.axis_index(("z", "core"))
    qkv_full = gather_rows(w_qkv.astype(jnp.bfloat16), 1)
    out_full, up_full, down_full = gather_batch(
        [w_out.astype(jnp.bfloat16), w_up.astype(jnp.bfloat16), w_down.astype(jnp.bfloat16)]
    )
    bias_full = doubling_gather(b_mod.astype(jnp.bfloat16), "seq", seq_count, seq_rank).reshape(-1)
    mod_low = w_mod.astype(jnp.bfloat16)
    mod_rows_here = w_mod.shape[0]
    mod_first = seq_rank * mod_rows_here
    inside_all, owners_all, places_all, usable_all = clip_tables(
        clip_len[0], pad_len[0], jnp.arange(group_frames, dtype=jnp.int32)
    )
    row_first = seq_rank * frame_rows
    inside_own = lax.dynamic_slice_in_dim(inside_all, row_first, frame_rows, 0)
    places_own = lax.dynamic_slice_in_dim(places_all, row_first, frame_rows, 0)
    silu_low = jax.nn.silu(time_emb).astype(jnp.bfloat16)
    silu_part = lax.dynamic_slice_in_dim(silu_low, mod_first, mod_rows_here, 1)
    modulation = butterfly_sum(
        jnp.dot(silu_part, mod_low, preferred_element_type=jnp.float32), "seq", seq_count
    ) + bias_full.astype(jnp.float32)
    mod_rows = jnp.dot(inside_own, modulation, precision=precise)
    shift_attn, scale_attn, gate_attn, shift_ff, scale_ff, gate_ff = jnp.split(mod_rows, 6, axis=1)
    inputs = frames.astype(jnp.float32)
    hidden, attn_norm_back = jax.vjp(modulate, inputs, shift_attn, scale_attn)
    hidden_low = hidden.astype(jnp.bfloat16)
    query_lin = jnp.dot(hidden_low, qkv_full[0], preferred_element_type=jnp.float32)
    key_lin = jnp.dot(hidden_low, qkv_full[1], preferred_element_type=jnp.float32)
    value_lin = jnp.dot(hidden_low, qkv_full[2], preferred_element_type=jnp.float32)
    query_send = rotate(query_lin, places_own, 1.0).astype(jnp.bfloat16)
    key_send = rotate(key_lin, places_own, 1.0).astype(jnp.bfloat16)
    value_send = value_lin.astype(jnp.bfloat16)
    query_heads, key_heads, value_heads = (
        lax.all_to_all(query_send, "seq", split_axis=1, concat_axis=0, tiled=True),
        lax.all_to_all(key_send, "seq", split_axis=1, concat_axis=0, tiled=True),
        lax.all_to_all(value_send, "seq", split_axis=1, concat_axis=0, tiled=True),
    )
    attended_heads, log_totals = attend_forward(
        query_heads, key_heads, value_heads, owners_all, usable_all, group_frames
    )
    attended = lax.all_to_all(attended_heads, "seq", split_axis=0, concat_axis=1, tiled=True)
    attn_proj = jnp.dot(attended, out_full, preferred_element_type=jnp.float32)
    mid = inputs + gate_attn * attn_proj
    hidden_ff, ff_norm_back = jax.vjp(modulate, mid, shift_ff, scale_ff)
    hidden_ff_low = hidden_ff.astype(jnp.bfloat16)
    pre_act = jnp.dot(hidden_ff_low, up_full, preferred_element_type=jnp.float32)
    active, gelu_back = jax.vjp(gelu_tanh, pre_act)
    active_low = active.astype(jnp.bfloat16)
    ff_proj = jnp.dot(active_low, down_full, preferred_element_type=jnp.float32)
    result = mid + gate_ff * ff_proj
    grad_result = out_grad.astype(jnp.float32)
    grad_gate_ff = grad_result * ff_proj
    grad_ff = (grad_result * gate_ff).astype(jnp.bfloat16)
    grad_down_local = jnp.einsum(
        "nf,nd->fd", active_low, grad_ff, preferred_element_type=jnp.float32
    )
    grad_active = jnp.einsum("nd,fd->nf", grad_ff, down_full, preferred_element_type=jnp.float32)
    (grad_pre,) = gelu_back(grad_active)
    grad_pre_low = grad_pre.astype(jnp.bfloat16)
    grad_up_local = jnp.einsum(
        "nd,nf->df", hidden_ff_low, grad_pre_low, preferred_element_type=jnp.float32
    )
    grad_hidden_ff = jnp.einsum(
        "nf,df->nd", grad_pre_low, up_full, preferred_element_type=jnp.float32
    )
    grad_mid_norm, grad_shift_ff, grad_scale_ff = ff_norm_back(grad_hidden_ff)
    grad_mid = grad_result + grad_mid_norm
    grad_gate_attn = grad_mid * attn_proj
    grad_proj = (grad_mid * gate_attn).astype(jnp.bfloat16)
    grad_out_local = jnp.einsum(
        "nd,ne->de", attended, grad_proj, preferred_element_type=jnp.float32
    )
    grad_attended = jnp.einsum(
        "ne,de->nd", grad_proj, out_full, preferred_element_type=jnp.float32
    ).astype(jnp.bfloat16)
    grad_heads = lax.all_to_all(grad_attended, "seq", split_axis=1, concat_axis=0, tiled=True)
    grad_query_heads, grad_key_heads, grad_value_heads = attend_backward(
        query_heads,
        key_heads,
        value_heads,
        grad_heads,
        log_totals,
        owners_all,
        usable_all,
        group_frames,
    )
    grad_query_rows, grad_key_rows, grad_value_rows = (
        lax.all_to_all(grad_query_heads, "seq", split_axis=0, concat_axis=1, tiled=True),
        lax.all_to_all(grad_key_heads, "seq", split_axis=0, concat_axis=1, tiled=True),
        lax.all_to_all(grad_value_heads, "seq", split_axis=0, concat_axis=1, tiled=True),
    )
    grad_query_lin = rotate(grad_query_rows.astype(jnp.float32), places_own, -1.0).astype(
        jnp.bfloat16
    )
    grad_key_lin = rotate(grad_key_rows.astype(jnp.float32), places_own, -1.0).astype(jnp.bfloat16)
    grad_qkv_local = jnp.stack(
        [
            jnp.einsum("nd,ne->de", hidden_low, grad_query_lin, preferred_element_type=jnp.float32),
            jnp.einsum("nd,ne->de", hidden_low, grad_key_lin, preferred_element_type=jnp.float32),
            jnp.einsum(
                "nd,ne->de", hidden_low, grad_value_rows, preferred_element_type=jnp.float32
            ),
        ]
    )
    grad_hidden = jnp.einsum(
        "ne,de->nd", grad_query_lin, qkv_full[0], preferred_element_type=jnp.float32
    )
    grad_hidden = grad_hidden + jnp.einsum(
        "ne,de->nd", grad_key_lin, qkv_full[1], preferred_element_type=jnp.float32
    )
    grad_hidden = grad_hidden + jnp.einsum(
        "ne,de->nd", grad_value_rows, qkv_full[2], preferred_element_type=jnp.float32
    )
    grad_input_norm, grad_shift_attn, grad_scale_attn = attn_norm_back(grad_hidden)
    input_grad = grad_mid + grad_input_norm
    grad_mod_rows = jnp.concatenate(
        [
            grad_shift_attn,
            grad_scale_attn,
            grad_gate_attn,
            grad_shift_ff,
            grad_scale_ff,
            grad_gate_ff,
        ],
        axis=1,
    )
    grad_mod_clip = butterfly_sum(
        jnp.einsum("nc,ne->ce", inside_own, grad_mod_rows, precision=precise), "seq", seq_count
    )
    grad_mod_all = doubling_gather(grad_mod_clip, ("z", "core"), dp_count, dp_rank).reshape(
        -1, grad_mod_clip.shape[1]
    )
    silu_all = doubling_gather(silu_part, ("z", "core"), dp_count, dp_rank).reshape(
        -1, silu_part.shape[1]
    )
    bias_cols = b_mod.shape[0]
    grad_bias_share = jnp.sum(
        lax.dynamic_slice_in_dim(grad_mod_all, seq_rank * bias_cols, bias_cols, 1), axis=0
    )
    grad_mod_share = jnp.einsum(
        "cd,ce->de", silu_all.astype(jnp.float32), grad_mod_all, precision=precise
    )
    grad_silu_part = jnp.einsum(
        "ce,de->cd", grad_mod_clip, mod_low.astype(jnp.float32), precision=precise
    )
    grad_silu = jnp.concatenate(
        list(doubling_gather(grad_silu_part, "seq", seq_count, seq_rank)), axis=1
    )
    time_grad = jax.vjp(jax.nn.silu, time_emb)[1](grad_silu)[0]
    grad_out, grad_up, grad_down = [
        share.astype(jnp.float32)
        for share in reduce_batch(
            [
                grad_out_local.astype(jnp.bfloat16),
                grad_up_local.astype(jnp.bfloat16),
                grad_down_local.astype(jnp.bfloat16),
            ]
        )
    ]
    qkv_piece = lax.psum_scatter(
        grad_qkv_local.astype(jnp.bfloat16), ("seq", "core"), scatter_dimension=1, tiled=True
    )
    updated = [
        lamb_update(w_out, mom_out, var_out, grad_out, None, seq_count),
        lamb_update(w_up, mom_up, var_up, grad_up, None, seq_count),
        lamb_update(w_down, mom_down, var_down, grad_down, None, seq_count),
        lamb_update(w_mod, mom_mod, var_mod, grad_mod_share, None, seq_count),
        lamb_update(b_mod, mom_bias, var_bias, grad_bias_share, None, seq_count),
    ]
    qkv_piece, updated = lax.optimization_barrier((qkv_piece, updated))
    qkv_piece = halving_sum(qkv_piece, "z", lax.axis_size("z"))
    qkv_other = lax.ppermute(qkv_piece, "core", [(0, 1), (1, 0)])
    qkv_first = lax.axis_index("core") == 0
    grad_qkv = jnp.concatenate(
        [jnp.where(qkv_first, qkv_piece, qkv_other), jnp.where(qkv_first, qkv_other, qkv_piece)],
        axis=1,
    ).astype(jnp.float32)
    updated = [lamb_update(w_qkv, mom_qkv, var_qkv, grad_qkv, (1, 2), seq_count)] + updated
    totals = (grad_qkv, grad_out, grad_up, grad_down, grad_mod_share, grad_bias_share)
    new_masters = [entry[0] for entry in updated]
    new_moments = [entry[1] for entry in updated]
    new_seconds = [entry[2] for entry in updated]
    return (
        result.astype(jnp.bfloat16),
        input_grad,
        time_grad,
        totals[0],
        new_masters[0],
        new_moments[0],
        new_seconds[0],
        totals[1],
        new_masters[1],
        new_moments[1],
        new_seconds[1],
        totals[2],
        new_masters[2],
        new_moments[2],
        new_seconds[2],
        totals[3],
        new_masters[3],
        new_moments[3],
        new_seconds[3],
        totals[4],
        new_masters[4],
        new_moments[4],
        new_seconds[4],
        totals[5],
        new_masters[5],
        new_moments[5],
        new_seconds[5],
    )


def solution(mesh):
    devices = mesh.devices
    chip_mesh = Mesh(
        devices.reshape(devices.shape[0] // 2, 2, devices.shape[1]), ("z", "core", "seq")
    )
    return jax.shard_map(
        local,
        mesh=chip_mesh,
        in_specs=(
            P(("z", "core", "seq"), None),
            P(("z", "core", "seq"), None),
            P(("z", "core"), None),
            P(("z", "core"), None),
            P(("z", "core"), None),
            P(None, "seq", None),
            P(None, "seq", None),
            P(None, "seq", None),
            P("seq", None),
            P("seq", None),
            P("seq", None),
            P("seq", None),
            P("seq", None),
            P("seq", None),
            P("seq", None),
            P("seq", None),
            P("seq", None),
            P("seq", None),
            P("seq", None),
            P("seq", None),
            P("seq"),
            P("seq"),
            P("seq"),
        ),
        out_specs=(
            P(("z", "core", "seq"), None),
            P(("z", "core", "seq"), None),
            P(("z", "core"), None),
            P(None, "seq", None),
            P(None, "seq", None),
            P(None, "seq", None),
            P(None, "seq", None),
            P("seq", None),
            P("seq", None),
            P("seq", None),
            P("seq", None),
            P("seq", None),
            P("seq", None),
            P("seq", None),
            P("seq", None),
            P("seq", None),
            P("seq", None),
            P("seq", None),
            P("seq", None),
            P("seq", None),
            P("seq", None),
            P("seq", None),
            P("seq", None),
            P("seq"),
            P("seq"),
            P("seq"),
            P("seq"),
        ),
        check_vma=False,
    )
```

```python
import jax
import jax.numpy as jnp
from jax import lax
from jax.sharding import Mesh, PartitionSpec as P

HEAD_DIM = 64


precise = lax.Precision.HIGHEST
norm_eps = 1e-06
masked_score = -1e30
beta_one = 0.9
beta_two = 0.999
adam_eps = 1e-08
weight_decay = 0.01
step_rate = 1.0
step_count = 10


def layer_norm(values):
    center = values - jnp.mean(values, axis=-1, keepdims=True)
    spread = jnp.mean(center * center, axis=-1, keepdims=True)
    return center * lax.rsqrt(spread + norm_eps)


def modulate(values, shift, scale):
    return layer_norm(values) * (1.0 + scale) + shift


def gelu_tanh(values):
    return jax.nn.gelu(values, approximate=True)


def rotate(values, places, turn_sign):
    frame_count = values.shape[0]
    half_dim = HEAD_DIM // 2
    exponent = jnp.arange(half_dim, dtype=jnp.float32) * (-2.0 / HEAD_DIM)
    frequency = jnp.power(jnp.float32(10000.0), exponent)
    angles = places.astype(jnp.float32)[:, None] * frequency[None, :]
    cos_table = jnp.cos(angles)[:, None, :]
    sin_table = turn_sign * jnp.sin(angles)[:, None, :]
    paired = values.reshape(frame_count, values.shape[1] // HEAD_DIM, half_dim, 2)
    even_part = paired[..., 0]
    odd_part = paired[..., 1]
    turned = jnp.stack(
        [
            even_part * cos_table - odd_part * sin_table,
            odd_part * cos_table + even_part * sin_table,
        ],
        axis=-1,
    )
    return turned.reshape(frame_count, values.shape[1])


def clip_tables(lengths, padding, frame_ids):
    starts = jnp.cumsum(lengths) - lengths
    finish = starts + lengths
    inside = (frame_ids[:, None] >= starts[None, :]) & (frame_ids[:, None] < finish[None, :])
    clip_ids = jnp.arange(lengths.shape[0], dtype=jnp.int32)
    owners = jnp.sum(jnp.where(inside, clip_ids[None, :], 0), axis=1)
    begins = jnp.sum(jnp.where(inside, starts[None, :], 0), axis=1)
    kept_len = jnp.maximum(lengths - padding, 1)
    limits = jnp.sum(jnp.where(inside, kept_len[None, :], 0), axis=1)
    places = frame_ids - begins
    return (inside.astype(jnp.float32), owners, places, places < limits)


def key_window(block_index, block_rows, span, frame_count):
    return jnp.clip(block_index * block_rows - (span - block_rows) // 2, 0, frame_count - span)


def block_inputs(queries, keys_all, values, owners, usable, block_index, block_rows, span):
    frame_count, columns = queries.shape
    heads_here = columns // HEAD_DIM
    row_start = block_index * block_rows
    window = key_window(block_index, block_rows, span, frame_count)
    query_rows = lax.dynamic_slice_in_dim(queries, row_start, block_rows, 0).reshape(
        block_rows, heads_here, HEAD_DIM
    )
    keys_win = keys_all.reshape(span, heads_here, HEAD_DIM)
    values_win = values.reshape(span, heads_here, HEAD_DIM)
    query_owner = lax.dynamic_slice_in_dim(owners, row_start, block_rows, 0)
    score_scale = HEAD_DIM ** (-0.5)
    scores = (
        jnp.einsum("qhd,khd->hqk", query_rows, keys_win, preferred_element_type=jnp.float32)
        * score_scale
    )
    allowed = (query_owner[:, None] == owners[None, :]) & usable[None, :]
    masked = jnp.where(allowed[None], scores, masked_score)
    return (row_start, window, query_rows, keys_win, values_win, masked)


def attend_forward(queries, keys_all, values, owners, usable, span):
    frame_count, columns = queries.shape
    block_rows = min(512, frame_count)

    def one_block(block_index):
        row_start, window, query_rows, keys_win, values_win, masked = block_inputs(
            queries, keys_all, values, owners, usable, block_index, block_rows, span
        )
        row_max = jnp.max(masked, axis=-1, keepdims=True)
        row_total = jnp.sum(jnp.exp(masked - row_max), axis=-1, keepdims=True)
        log_total = row_max + jnp.log(row_total)
        probs_low = jnp.exp(masked - log_total).astype(jnp.bfloat16)
        attended = jnp.einsum(
            "hqk,khd->qhd", probs_low, values_win, preferred_element_type=jnp.float32
        )
        return (attended.astype(jnp.bfloat16).reshape(block_rows, columns), log_total)

    outcome, log_totals = lax.map(one_block, jnp.arange(frame_count // block_rows, dtype=jnp.int32))
    return (outcome.reshape(frame_count, columns), log_totals)


def attend_backward(queries, keys_all, values, grad_attended, log_totals, owners, usable, span):
    frame_count, columns = queries.shape
    heads_here = columns // HEAD_DIM
    block_rows = min(512, frame_count)
    score_scale = HEAD_DIM ** (-0.5)

    def one_block(sums, block_data):
        key_sum, value_sum = sums
        block_index, log_total = block_data
        row_start, window, query_rows, keys_win, values_win, masked = block_inputs(
            queries, keys_all, values, owners, usable, block_index, block_rows, span
        )
        grad_rows = lax.dynamic_slice_in_dim(grad_attended, row_start, block_rows, 0).reshape(
            block_rows, heads_here, HEAD_DIM
        )
        probs_full = jnp.exp(masked - log_total)
        probs_low = probs_full.astype(jnp.bfloat16)
        grad_probs = jnp.einsum(
            "qhd,khd->hqk", grad_rows, values_win, preferred_element_type=jnp.float32
        )
        row_delta = jnp.sum(probs_full * grad_probs, axis=-1, keepdims=True)
        grad_scores = (probs_full * (grad_probs - row_delta)).astype(jnp.bfloat16)
        grad_query = (
            jnp.einsum("hqk,khd->qhd", grad_scores, keys_win, preferred_element_type=jnp.float32)
            * score_scale
        )
        grad_key = (
            jnp.einsum("hqk,qhd->khd", grad_scores, query_rows, preferred_element_type=jnp.float32)
            * score_scale
        )
        grad_value = jnp.einsum(
            "hqk,qhd->khd", probs_low, grad_rows, preferred_element_type=jnp.float32
        )
        old_keys = key_sum
        key_sum = old_keys + grad_key.reshape(span, columns)
        old_values = value_sum
        value_sum = old_values + grad_value.reshape(span, columns)
        return ((key_sum, value_sum), grad_query.astype(jnp.bfloat16).reshape(block_rows, columns))

    zeros = jnp.zeros((frame_count, columns), jnp.float32)
    indices = jnp.arange(frame_count // block_rows, dtype=jnp.int32)
    (key_sum, value_sum), grad_queries = lax.scan(one_block, (zeros, zeros), (indices, log_totals))
    return (
        grad_queries.reshape(frame_count, columns),
        key_sum.astype(jnp.bfloat16),
        value_sum.astype(jnp.bfloat16),
    )


def butterfly_sum(values, axes, size):
    step = 1
    while step < size:
        values = values + lax.ppermute(values, axes, [(i, i ^ step) for i in range(size)])
        step *= 2
    return values


def doubling_gather(values, axes, size, index):
    blocks = values[None]
    step = 1
    while step < size:
        other = lax.ppermute(blocks, axes, [(i, i ^ step) for i in range(size)])
        low_side = (index // step) % 2 == 0
        blocks = jnp.concatenate(
            [jnp.where(low_side, blocks, other), jnp.where(low_side, other, blocks)], axis=0
        )
        step *= 2
    return blocks


def gather_rows(shard, row_axis):
    half = shard.shape[row_axis] // 2
    core = lax.axis_index("core")
    piece = lax.dynamic_slice_in_dim(shard, core * half, half, row_axis)
    return lax.all_gather(piece, ("seq", "core"), axis=row_axis, tiled=True)


def halving_sum(values, axis_name, size):
    index = lax.axis_index(axis_name)
    total = values.astype(jnp.float32)
    step = 1
    while step < size:
        half = total.shape[-1] // 2
        low_side = (index // step) % 2 == 0
        keep = jnp.where(low_side, total[..., :half], total[..., half:])
        send = jnp.where(low_side, total[..., half:], total[..., :half]).astype(jnp.bfloat16)
        total = keep + lax.ppermute(send, axis_name, [(i, i ^ step) for i in range(size)]).astype(
            jnp.float32
        )
        step *= 2
    blocks = total.astype(jnp.bfloat16)
    step = size // 2
    while step >= 1:
        other = lax.ppermute(blocks, axis_name, [(i, i ^ step) for i in range(size)])
        low_side = (index // step) % 2 == 0
        blocks = jnp.concatenate(
            [jnp.where(low_side, blocks, other), jnp.where(low_side, other, blocks)], axis=-1
        )
        step //= 2
    return blocks


def reduce_rows(partial, row_axis):
    piece = lax.psum_scatter(partial, ("seq", "core"), scatter_dimension=row_axis, tiled=True)
    piece = halving_sum(piece, "z", lax.axis_size("z"))
    other = lax.ppermute(piece, "core", [(0, 1), (1, 0)])
    first = lax.axis_index("core") == 0
    return jnp.concatenate(
        [jnp.where(first, piece, other), jnp.where(first, other, piece)], axis=row_axis
    )


def gather_batch(shards):
    core = lax.axis_index("core")
    base = min(shard.shape[1] for shard in shards)
    pieces = []
    for shard in shards:
        half = shard.shape[0] // 2
        piece = lax.dynamic_slice_in_dim(shard, core * half, half, 0)
        pieces.append(piece.reshape(-1, base))
    blocks = lax.all_gather(jnp.concatenate(pieces, axis=0), ("seq", "core"), axis=0, tiled=False)
    fulls = []
    offset = 0
    for shard, piece in zip(shards, pieces):
        rows = piece.shape[0]
        fulls.append(blocks[:, offset : offset + rows].reshape(-1, shard.shape[1]))
        offset += rows
    return fulls


def reduce_batch(partials):
    groups = lax.axis_size("seq") * 2
    base = min(part.shape[1] for part in partials)
    views = [part.reshape(groups, -1, base) for part in partials]
    flat = jnp.concatenate(views, axis=1)
    piece = lax.psum_scatter(flat, ("seq", "core"), scatter_dimension=0, tiled=True)[0]
    piece = halving_sum(piece, "z", lax.axis_size("z"))
    other = lax.ppermute(piece, "core", [(0, 1), (1, 0)])
    first = lax.axis_index("core") == 0
    low = jnp.where(first, piece, other)
    high = jnp.where(first, other, piece)
    shares = []
    offset = 0
    for part, view in zip(partials, views):
        rows = view.shape[1]
        shape = (-1, part.shape[1])
        shares.append(
            jnp.concatenate(
                [
                    low[offset : offset + rows].reshape(shape),
                    high[offset : offset + rows].reshape(shape),
                ],
                axis=0,
            )
        )
        offset += rows
    return shares


def lamb_update(weight, moment, second, grad, sum_axes, seq_count):
    moment_new, second_new, direction = adam_direction(weight, moment, second, grad)
    sums = jnp.concatenate(
        [
            jnp.sum(weight * weight, axis=sum_axes, keepdims=True),
            jnp.sum(direction * direction, axis=sum_axes, keepdims=True),
        ],
        axis=-1,
    )
    sums = butterfly_sum(sums, "seq", seq_count)
    ratio = jnp.sqrt(sums[..., :1]) * lax.rsqrt(sums[..., 1:] + 1e-06)
    return (weight - step_rate * ratio * direction, moment_new, second_new)


def adam_direction(weight, moment, second, grad):
    moment_new = beta_one * moment + (1.0 - beta_one) * grad
    second_new = beta_two * second + (1.0 - beta_two) * grad * grad
    corrected = moment_new / (1.0 - beta_one**step_count)
    scaled = second_new / (1.0 - beta_two**step_count)
    direction = corrected / (jnp.sqrt(scaled) + adam_eps) + weight_decay * weight
    return (moment_new, second_new, direction)


def local(
    frames,
    out_grad,
    time_emb,
    clip_len,
    pad_len,
    w_qkv,
    mom_qkv,
    var_qkv,
    w_out,
    mom_out,
    var_out,
    w_up,
    mom_up,
    var_up,
    w_down,
    mom_down,
    var_down,
    w_mod,
    mom_mod,
    var_mod,
    b_mod,
    mom_bias,
    var_bias,
):
    seq_count = lax.axis_size("seq")
    seq_rank = lax.axis_index("seq")
    frame_rows = frames.shape[0]
    group_frames = frame_rows * seq_count
    dp_count = lax.axis_size(("z", "core"))
    dp_rank = lax.axis_index(("z", "core"))
    qkv_full = gather_rows(w_qkv.astype(jnp.bfloat16), 1)
    out_full, up_full, down_full = gather_batch(
        [w_out.astype(jnp.bfloat16), w_up.astype(jnp.bfloat16), w_down.astype(jnp.bfloat16)]
    )
    bias_full = doubling_gather(b_mod.astype(jnp.bfloat16), "seq", seq_count, seq_rank).reshape(-1)
    mod_low = w_mod.astype(jnp.bfloat16)
    mod_rows_here = w_mod.shape[0]
    mod_first = seq_rank * mod_rows_here
    inside_all, owners_all, places_all, usable_all = clip_tables(
        clip_len[0], pad_len[0], jnp.arange(group_frames, dtype=jnp.int32)
    )
    row_first = seq_rank * frame_rows
    inside_own = lax.dynamic_slice_in_dim(inside_all, row_first, frame_rows, 0)
    places_own = lax.dynamic_slice_in_dim(places_all, row_first, frame_rows, 0)
    silu_low = jax.nn.silu(time_emb).astype(jnp.bfloat16)
    silu_part = lax.dynamic_slice_in_dim(silu_low, mod_first, mod_rows_here, 1)
    modulation = butterfly_sum(
        jnp.dot(silu_part, mod_low, preferred_element_type=jnp.float32), "seq", seq_count
    ) + bias_full.astype(jnp.float32)
    mod_rows = jnp.dot(inside_own, modulation, precision=precise)
    shift_attn, scale_attn, gate_attn, shift_ff, scale_ff, gate_ff = jnp.split(mod_rows, 6, axis=1)
    inputs = frames.astype(jnp.float32)
    hidden, attn_norm_back = jax.vjp(modulate, inputs, shift_attn, scale_attn)
    hidden_low = hidden.astype(jnp.bfloat16)
    query_lin = jnp.dot(hidden_low, qkv_full[0], preferred_element_type=jnp.float32)
    key_lin = jnp.dot(hidden_low, qkv_full[1], preferred_element_type=jnp.float32)
    value_lin = jnp.dot(hidden_low, qkv_full[2], preferred_element_type=jnp.float32)
    query_send = rotate(query_lin, places_own, 1.0).astype(jnp.bfloat16)
    key_send = rotate(key_lin, places_own, 1.0).astype(jnp.bfloat16)
    value_send = value_lin.astype(jnp.bfloat16)
    query_heads, key_heads, value_heads = (
        lax.all_to_all(query_send, "seq", split_axis=1, concat_axis=0, tiled=True),
        lax.all_to_all(key_send, "seq", split_axis=1, concat_axis=0, tiled=True),
        lax.all_to_all(value_send, "seq", split_axis=1, concat_axis=0, tiled=True),
    )
    attended_heads, log_totals = attend_forward(
        query_heads, key_heads, value_heads, owners_all, usable_all, group_frames
    )
    attended = lax.all_to_all(attended_heads, "seq", split_axis=0, concat_axis=1, tiled=True)
    attn_proj = jnp.dot(attended, out_full, preferred_element_type=jnp.float32)
    mid = inputs + gate_attn * attn_proj
    hidden_ff, ff_norm_back = jax.vjp(modulate, mid, shift_ff, scale_ff)
    hidden_ff_low = hidden_ff.astype(jnp.bfloat16)
    pre_act = jnp.dot(hidden_ff_low, up_full, preferred_element_type=jnp.float32)
    active, gelu_back = jax.vjp(gelu_tanh, pre_act)
    active_low = active.astype(jnp.bfloat16)
    ff_proj = jnp.dot(active_low, down_full, preferred_element_type=jnp.float32)
    result = mid + gate_ff * ff_proj
    grad_result = out_grad.astype(jnp.float32)
    grad_gate_ff = grad_result * ff_proj
    grad_ff = (grad_result * gate_ff).astype(jnp.bfloat16)
    grad_down_local = jnp.einsum(
        "nf,nd->fd", active_low, grad_ff, preferred_element_type=jnp.float32
    )
    grad_active = jnp.einsum("nd,fd->nf", grad_ff, down_full, preferred_element_type=jnp.float32)
    (grad_pre,) = gelu_back(grad_active)
    grad_pre_low = grad_pre.astype(jnp.bfloat16)
    grad_up_local = jnp.einsum(
        "nd,nf->df", hidden_ff_low, grad_pre_low, preferred_element_type=jnp.float32
    )
    grad_hidden_ff = jnp.einsum(
        "nf,df->nd", grad_pre_low, up_full, preferred_element_type=jnp.float32
    )
    grad_mid_norm, grad_shift_ff, grad_scale_ff = ff_norm_back(grad_hidden_ff)
    grad_mid = grad_result + grad_mid_norm
    grad_gate_attn = grad_mid * attn_proj
    grad_proj = (grad_mid * gate_attn).astype(jnp.bfloat16)
    grad_out_local = jnp.einsum(
        "nd,ne->de", attended, grad_proj, preferred_element_type=jnp.float32
    )
    grad_attended = jnp.einsum(
        "ne,de->nd", grad_proj, out_full, preferred_element_type=jnp.float32
    ).astype(jnp.bfloat16)
    grad_heads = lax.all_to_all(grad_attended, "seq", split_axis=1, concat_axis=0, tiled=True)
    grad_query_heads, grad_key_heads, grad_value_heads = attend_backward(
        query_heads,
        key_heads,
        value_heads,
        grad_heads,
        log_totals,
        owners_all,
        usable_all,
        group_frames,
    )
    grad_query_rows, grad_key_rows, grad_value_rows = (
        lax.all_to_all(grad_query_heads, "seq", split_axis=0, concat_axis=1, tiled=True),
        lax.all_to_all(grad_key_heads, "seq", split_axis=0, concat_axis=1, tiled=True),
        lax.all_to_all(grad_value_heads, "seq", split_axis=0, concat_axis=1, tiled=True),
    )
    grad_query_lin = rotate(grad_query_rows.astype(jnp.float32), places_own, -1.0).astype(
        jnp.bfloat16
    )
    grad_key_lin = rotate(grad_key_rows.astype(jnp.float32), places_own, -1.0).astype(jnp.bfloat16)
    grad_qkv_local = jnp.stack(
        [
            jnp.einsum("nd,ne->de", hidden_low, grad_query_lin, preferred_element_type=jnp.float32),
            jnp.einsum("nd,ne->de", hidden_low, grad_key_lin, preferred_element_type=jnp.float32),
            jnp.einsum(
                "nd,ne->de", hidden_low, grad_value_rows, preferred_element_type=jnp.float32
            ),
        ]
    )
    grad_hidden = jnp.einsum(
        "ne,de->nd", grad_query_lin, qkv_full[0], preferred_element_type=jnp.float32
    )
    grad_hidden = grad_hidden + jnp.einsum(
        "ne,de->nd", grad_key_lin, qkv_full[1], preferred_element_type=jnp.float32
    )
    grad_hidden = grad_hidden + jnp.einsum(
        "ne,de->nd", grad_value_rows, qkv_full[2], preferred_element_type=jnp.float32
    )
    grad_input_norm, grad_shift_attn, grad_scale_attn = attn_norm_back(grad_hidden)
    input_grad = grad_mid + grad_input_norm
    grad_mod_rows = jnp.concatenate(
        [
            grad_shift_attn,
            grad_scale_attn,
            grad_gate_attn,
            grad_shift_ff,
            grad_scale_ff,
            grad_gate_ff,
        ],
        axis=1,
    )
    grad_mod_clip = butterfly_sum(
        jnp.einsum("nc,ne->ce", inside_own, grad_mod_rows, precision=precise), "seq", seq_count
    )
    grad_mod_all = doubling_gather(grad_mod_clip, ("z", "core"), dp_count, dp_rank).reshape(
        -1, grad_mod_clip.shape[1]
    )
    silu_all = doubling_gather(silu_part, ("z", "core"), dp_count, dp_rank).reshape(
        -1, silu_part.shape[1]
    )
    bias_cols = b_mod.shape[0]
    grad_bias_share = jnp.sum(
        lax.dynamic_slice_in_dim(grad_mod_all, seq_rank * bias_cols, bias_cols, 1), axis=0
    )
    grad_mod_share = jnp.einsum(
        "cd,ce->de", silu_all.astype(jnp.float32), grad_mod_all, precision=precise
    )
    grad_silu_part = jnp.einsum(
        "ce,de->cd", grad_mod_clip, mod_low.astype(jnp.float32), precision=precise
    )
    grad_silu = jnp.concatenate(
        list(doubling_gather(grad_silu_part, "seq", seq_count, seq_rank)), axis=1
    )
    time_grad = jax.vjp(jax.nn.silu, time_emb)[1](grad_silu)[0]
    grad_out, grad_up, grad_down = [
        share.astype(jnp.float32)
        for share in reduce_batch(
            [
                grad_out_local.astype(jnp.bfloat16),
                grad_up_local.astype(jnp.bfloat16),
                grad_down_local.astype(jnp.bfloat16),
            ]
        )
    ]
    qkv_piece = lax.psum_scatter(
        grad_qkv_local.astype(jnp.bfloat16), ("seq", "core"), scatter_dimension=1, tiled=True
    )
    updated = [
        lamb_update(w_out, mom_out, var_out, grad_out, None, seq_count),
        lamb_update(w_up, mom_up, var_up, grad_up, None, seq_count),
        lamb_update(w_down, mom_down, var_down, grad_down, None, seq_count),
        lamb_update(w_mod, mom_mod, var_mod, grad_mod_share, None, seq_count),
        lamb_update(b_mod, mom_bias, var_bias, grad_bias_share, None, seq_count),
    ]
    qkv_piece, updated = lax.optimization_barrier((qkv_piece, updated))
    qkv_piece = halving_sum(qkv_piece, "z", lax.axis_size("z"))
    qkv_other = lax.ppermute(qkv_piece, "core", [(0, 1), (1, 0)])
    qkv_first = lax.axis_index("core") == 0
    grad_qkv = jnp.concatenate(
        [jnp.where(qkv_first, qkv_piece, qkv_other), jnp.where(qkv_first, qkv_other, qkv_piece)],
        axis=1,
    ).astype(jnp.float32)
    updated = [lamb_update(w_qkv, mom_qkv, var_qkv, grad_qkv, (1, 2), seq_count)] + updated
    totals = (grad_qkv, grad_out, grad_up, grad_down, grad_mod_share, grad_bias_share)
    new_masters = [entry[0] for entry in updated]
    new_moments = [entry[1] for entry in updated]
    new_seconds = [entry[2] for entry in updated]
    return (
        result.astype(jnp.bfloat16),
        input_grad,
        time_grad,
        totals[0],
        new_masters[0],
        new_moments[0],
        new_seconds[0],
        totals[1],
        new_masters[1],
        new_moments[1],
        new_seconds[1],
        totals[2],
        new_masters[2],
        new_moments[2],
        new_seconds[2],
        totals[3],
        new_masters[3],
        new_moments[3],
        new_seconds[3],
        totals[4],
        new_masters[4],
        new_moments[4],
        new_seconds[4],
        totals[5],
        new_masters[5],
        new_moments[5],
        new_seconds[5],
    )


def solution(mesh):
    devices = mesh.devices
    chip_mesh = Mesh(
        devices.reshape(devices.shape[0] // 2, 2, devices.shape[1]), ("z", "core", "seq")
    )
    return jax.shard_map(
        local,
        mesh=chip_mesh,
        in_specs=(
            P(("z", "core", "seq"), None),
            P(("z", "core", "seq"), None),
            P(("z", "core"), None),
            P(("z", "core"), None),
            P(("z", "core"), None),
            P(None, "seq", None),
            P(None, "seq", None),
            P(None, "seq", None),
            P("seq", None),
            P("seq", None),
            P("seq", None),
            P("seq", None),
            P("seq", None),
            P("seq", None),
            P("seq", None),
            P("seq", None),
            P("seq", None),
            P("seq", None),
            P("seq", None),
            P("seq", None),
            P("seq"),
            P("seq"),
            P("seq"),
        ),
        out_specs=(
            P(("z", "core", "seq"), None),
            P(("z", "core", "seq"), None),
            P(("z", "core"), None),
            P(None, "seq", None),
            P(None, "seq", None),
            P(None, "seq", None),
            P(None, "seq", None),
            P("seq", None),
            P("seq", None),
            P("seq", None),
            P("seq", None),
            P("seq", None),
            P("seq", None),
            P("seq", None),
            P("seq", None),
            P("seq", None),
            P("seq", None),
            P("seq", None),
            P("seq", None),
            P("seq", None),
            P("seq", None),
            P("seq", None),
            P("seq", None),
            P("seq"),
            P("seq"),
            P("seq"),
            P("seq"),
        ),
        check_vma=False,
    )
```

```python
import jax
import jax.numpy as jnp
from jax import lax
from jax.sharding import Mesh, PartitionSpec as P

HEAD_DIM = 64


precise = lax.Precision.HIGHEST
norm_eps = 1e-06
masked_score = -1e30
beta_one = 0.9
beta_two = 0.999
adam_eps = 1e-08
weight_decay = 0.01
step_rate = 1.0
step_count = 10


def layer_norm(values):
    center = values - jnp.mean(values, axis=-1, keepdims=True)
    spread = jnp.mean(center * center, axis=-1, keepdims=True)
    return center * lax.rsqrt(spread + norm_eps)


def modulate(values, shift, scale):
    return layer_norm(values) * (1.0 + scale) + shift


def gelu_tanh(values):
    return jax.nn.gelu(values, approximate=True)


def rotate(values, places, turn_sign):
    frame_count = values.shape[0]
    half_dim = HEAD_DIM // 2
    exponent = jnp.arange(half_dim, dtype=jnp.float32) * (-2.0 / HEAD_DIM)
    frequency = jnp.power(jnp.float32(10000.0), exponent)
    angles = places.astype(jnp.float32)[:, None] * frequency[None, :]
    cos_table = jnp.cos(angles)[:, None, :]
    sin_table = turn_sign * jnp.sin(angles)[:, None, :]
    paired = values.reshape(frame_count, values.shape[1] // HEAD_DIM, half_dim, 2)
    even_part = paired[..., 0]
    odd_part = paired[..., 1]
    turned = jnp.stack(
        [
            even_part * cos_table - odd_part * sin_table,
            odd_part * cos_table + even_part * sin_table,
        ],
        axis=-1,
    )
    return turned.reshape(frame_count, values.shape[1])


def clip_tables(lengths, padding, frame_ids):
    starts = jnp.cumsum(lengths) - lengths
    finish = starts + lengths
    inside = (frame_ids[:, None] >= starts[None, :]) & (frame_ids[:, None] < finish[None, :])
    clip_ids = jnp.arange(lengths.shape[0], dtype=jnp.int32)
    owners = jnp.sum(jnp.where(inside, clip_ids[None, :], 0), axis=1)
    begins = jnp.sum(jnp.where(inside, starts[None, :], 0), axis=1)
    kept_len = jnp.maximum(lengths - padding, 1)
    limits = jnp.sum(jnp.where(inside, kept_len[None, :], 0), axis=1)
    places = frame_ids - begins
    return (inside.astype(jnp.float32), owners, places, places < limits)


def key_window(block_index, block_rows, span, frame_count):
    return jnp.clip(block_index * block_rows - (span - block_rows) // 2, 0, frame_count - span)


def block_inputs(queries, keys_all, values, owners, usable, block_index, block_rows, span):
    frame_count, columns = queries.shape
    heads_here = columns // HEAD_DIM
    row_start = block_index * block_rows
    window = key_window(block_index, block_rows, span, frame_count)
    query_rows = lax.dynamic_slice_in_dim(queries, row_start, block_rows, 0).reshape(
        block_rows, heads_here, HEAD_DIM
    )
    keys_win = keys_all.reshape(span, heads_here, HEAD_DIM)
    values_win = values.reshape(span, heads_here, HEAD_DIM)
    query_owner = lax.dynamic_slice_in_dim(owners, row_start, block_rows, 0)
    score_scale = HEAD_DIM ** (-0.5)
    scores = (
        jnp.einsum("qhd,khd->hqk", query_rows, keys_win, preferred_element_type=jnp.float32)
        * score_scale
    )
    allowed = (query_owner[:, None] == owners[None, :]) & usable[None, :]
    masked = jnp.where(allowed[None], scores, masked_score)
    return (row_start, window, query_rows, keys_win, values_win, masked)


def attend_forward(queries, keys_all, values, owners, usable, span):
    frame_count, columns = queries.shape
    block_rows = min(512, frame_count)

    def one_block(block_index):
        row_start, window, query_rows, keys_win, values_win, masked = block_inputs(
            queries, keys_all, values, owners, usable, block_index, block_rows, span
        )
        row_max = jnp.max(masked, axis=-1, keepdims=True)
        row_total = jnp.sum(jnp.exp(masked - row_max), axis=-1, keepdims=True)
        log_total = row_max + jnp.log(row_total)
        probs_low = jnp.exp(masked - log_total).astype(jnp.bfloat16)
        attended = jnp.einsum(
            "hqk,khd->qhd", probs_low, values_win, preferred_element_type=jnp.float32
        )
        return (attended.astype(jnp.bfloat16).reshape(block_rows, columns), log_total)

    outcome, log_totals = lax.map(one_block, jnp.arange(frame_count // block_rows, dtype=jnp.int32))
    return (outcome.reshape(frame_count, columns), log_totals)


def attend_backward(queries, keys_all, values, grad_attended, log_totals, owners, usable, span):
    frame_count, columns = queries.shape
    heads_here = columns // HEAD_DIM
    block_rows = min(512, frame_count)
    score_scale = HEAD_DIM ** (-0.5)

    def one_block(sums, block_data):
        key_sum, value_sum = sums
        block_index, log_total = block_data
        row_start, window, query_rows, keys_win, values_win, masked = block_inputs(
            queries, keys_all, values, owners, usable, block_index, block_rows, span
        )
        grad_rows = lax.dynamic_slice_in_dim(grad_attended, row_start, block_rows, 0).reshape(
            block_rows, heads_here, HEAD_DIM
        )
        probs_full = jnp.exp(masked - log_total)
        probs_low = probs_full.astype(jnp.bfloat16)
        grad_probs = jnp.einsum(
            "qhd,khd->hqk", grad_rows, values_win, preferred_element_type=jnp.float32
        )
        row_delta = jnp.sum(probs_full * grad_probs, axis=-1, keepdims=True)
        grad_scores = (probs_full * (grad_probs - row_delta)).astype(jnp.bfloat16)
        grad_query = (
            jnp.einsum("hqk,khd->qhd", grad_scores, keys_win, preferred_element_type=jnp.float32)
            * score_scale
        )
        grad_key = (
            jnp.einsum("hqk,qhd->khd", grad_scores, query_rows, preferred_element_type=jnp.float32)
            * score_scale
        )
        grad_value = jnp.einsum(
            "hqk,qhd->khd", probs_low, grad_rows, preferred_element_type=jnp.float32
        )
        old_keys = key_sum
        key_sum = old_keys + grad_key.reshape(span, columns)
        old_values = value_sum
        value_sum = old_values + grad_value.reshape(span, columns)
        return ((key_sum, value_sum), grad_query.astype(jnp.bfloat16).reshape(block_rows, columns))

    zeros = jnp.zeros((frame_count, columns), jnp.float32)
    indices = jnp.arange(frame_count // block_rows, dtype=jnp.int32)
    (key_sum, value_sum), grad_queries = lax.scan(one_block, (zeros, zeros), (indices, log_totals))
    return (
        grad_queries.reshape(frame_count, columns),
        key_sum.astype(jnp.bfloat16),
        value_sum.astype(jnp.bfloat16),
    )


def butterfly_sum(values, axes, size):
    step = 1
    while step < size:
        values = values + lax.ppermute(values, axes, [(i, i ^ step) for i in range(size)])
        step *= 2
    return values


def doubling_gather(values, axes, size, index):
    blocks = values[None]
    step = 1
    while step < size:
        other = lax.ppermute(blocks, axes, [(i, i ^ step) for i in range(size)])
        low_side = (index // step) % 2 == 0
        blocks = jnp.concatenate(
            [jnp.where(low_side, blocks, other), jnp.where(low_side, other, blocks)], axis=0
        )
        step *= 2
    return blocks


def gather_rows(shard, row_axis):
    half = shard.shape[row_axis] // 2
    core = lax.axis_index("core")
    piece = lax.dynamic_slice_in_dim(shard, core * half, half, row_axis)
    return lax.all_gather(piece, ("seq", "core"), axis=row_axis, tiled=True)


def halving_sum(values, axis_name, size):
    index = lax.axis_index(axis_name)
    total = values.astype(jnp.float32)
    step = 1
    while step < size:
        half = total.shape[-1] // 2
        low_side = (index // step) % 2 == 0
        keep = jnp.where(low_side, total[..., :half], total[..., half:])
        send = jnp.where(low_side, total[..., half:], total[..., :half]).astype(jnp.bfloat16)
        total = keep + lax.ppermute(send, axis_name, [(i, i ^ step) for i in range(size)]).astype(
            jnp.float32
        )
        step *= 2
    blocks = total.astype(jnp.bfloat16)
    step = size // 2
    while step >= 1:
        other = lax.ppermute(blocks, axis_name, [(i, i ^ step) for i in range(size)])
        low_side = (index // step) % 2 == 0
        blocks = jnp.concatenate(
            [jnp.where(low_side, blocks, other), jnp.where(low_side, other, blocks)], axis=-1
        )
        step //= 2
    return blocks


def reduce_rows(partial, row_axis):
    piece = lax.psum_scatter(partial, ("seq", "core"), scatter_dimension=row_axis, tiled=True)
    piece = halving_sum(piece, "z", lax.axis_size("z"))
    other = lax.ppermute(piece, "core", [(0, 1), (1, 0)])
    first = lax.axis_index("core") == 0
    return jnp.concatenate(
        [jnp.where(first, piece, other), jnp.where(first, other, piece)], axis=row_axis
    )


def gather_batch(shards):
    core = lax.axis_index("core")
    base = min(shard.shape[1] for shard in shards)
    pieces = []
    for shard in shards:
        half = shard.shape[0] // 2
        piece = lax.dynamic_slice_in_dim(shard, core * half, half, 0)
        pieces.append(piece.reshape(-1, base))
    blocks = lax.all_gather(jnp.concatenate(pieces, axis=0), ("seq", "core"), axis=0, tiled=False)
    fulls = []
    offset = 0
    for shard, piece in zip(shards, pieces):
        rows = piece.shape[0]
        fulls.append(blocks[:, offset : offset + rows].reshape(-1, shard.shape[1]))
        offset += rows
    return fulls


def reduce_batch(partials):
    groups = lax.axis_size("seq") * 2
    base = min(part.shape[1] for part in partials)
    views = [part.reshape(groups, -1, base) for part in partials]
    flat = jnp.concatenate(views, axis=1)
    piece = lax.psum_scatter(flat, ("seq", "core"), scatter_dimension=0, tiled=True)[0]
    piece = halving_sum(piece, "z", lax.axis_size("z"))
    other = lax.ppermute(piece, "core", [(0, 1), (1, 0)])
    first = lax.axis_index("core") == 0
    low = jnp.where(first, piece, other)
    high = jnp.where(first, other, piece)
    shares = []
    offset = 0
    for part, view in zip(partials, views):
        rows = view.shape[1]
        shape = (-1, part.shape[1])
        shares.append(
            jnp.concatenate(
                [
                    low[offset : offset + rows].reshape(shape),
                    high[offset : offset + rows].reshape(shape),
                ],
                axis=0,
            )
        )
        offset += rows
    return shares


def lamb_update(weight, moment, second, grad, sum_axes, seq_count):
    moment_new, second_new, direction = adam_direction(weight, moment, second, grad)
    sums = jnp.concatenate(
        [
            jnp.sum(weight * weight, axis=sum_axes, keepdims=True),
            jnp.sum(direction * direction, axis=sum_axes, keepdims=True),
        ],
        axis=-1,
    )
    sums = butterfly_sum(sums, "seq", seq_count)
    ratio = jnp.sqrt(sums[..., :1]) * lax.rsqrt(sums[..., 1:] + 1e-06)
    return (weight - step_rate * ratio * direction, moment_new, second_new)


def adam_direction(weight, moment, second, grad):
    moment_new = beta_one * moment + (1.0 - beta_one) * grad
    second_new = beta_two * second + (1.0 - beta_two) * grad * grad
    corrected = moment_new / (1.0 - beta_one**step_count)
    scaled = second_new / (1.0 - beta_two**step_count)
    direction = corrected / (jnp.sqrt(scaled) + adam_eps) + weight_decay * weight
    return (moment_new, second_new, direction)


def local(
    frames,
    out_grad,
    time_emb,
    clip_len,
    pad_len,
    w_qkv,
    mom_qkv,
    var_qkv,
    w_out,
    mom_out,
    var_out,
    w_up,
    mom_up,
    var_up,
    w_down,
    mom_down,
    var_down,
    w_mod,
    mom_mod,
    var_mod,
    b_mod,
    mom_bias,
    var_bias,
):
    seq_count = lax.axis_size("seq")
    seq_rank = lax.axis_index("seq")
    frame_rows = frames.shape[0]
    group_frames = frame_rows * seq_count
    dp_count = lax.axis_size(("z", "core"))
    dp_rank = lax.axis_index(("z", "core"))
    qkv_full = gather_rows(w_qkv.astype(jnp.bfloat16), 1)
    out_full, up_full, down_full = gather_batch(
        [w_out.astype(jnp.bfloat16), w_up.astype(jnp.bfloat16), w_down.astype(jnp.bfloat16)]
    )
    bias_full = doubling_gather(b_mod.astype(jnp.bfloat16), "seq", seq_count, seq_rank).reshape(-1)
    mod_low = w_mod.astype(jnp.bfloat16)
    mod_rows_here = w_mod.shape[0]
    mod_first = seq_rank * mod_rows_here
    inside_all, owners_all, places_all, usable_all = clip_tables(
        clip_len[0], pad_len[0], jnp.arange(group_frames, dtype=jnp.int32)
    )
    row_first = seq_rank * frame_rows
    inside_own = lax.dynamic_slice_in_dim(inside_all, row_first, frame_rows, 0)
    places_own = lax.dynamic_slice_in_dim(places_all, row_first, frame_rows, 0)
    silu_low = jax.nn.silu(time_emb).astype(jnp.bfloat16)
    silu_part = lax.dynamic_slice_in_dim(silu_low, mod_first, mod_rows_here, 1)
    modulation = butterfly_sum(
        jnp.dot(silu_part, mod_low, preferred_element_type=jnp.float32), "seq", seq_count
    ) + bias_full.astype(jnp.float32)
    mod_rows = jnp.dot(inside_own, modulation, precision=precise)
    shift_attn, scale_attn, gate_attn, shift_ff, scale_ff, gate_ff = jnp.split(mod_rows, 6, axis=1)
    inputs = frames.astype(jnp.float32)
    hidden, attn_norm_back = jax.vjp(modulate, inputs, shift_attn, scale_attn)
    hidden_low = hidden.astype(jnp.bfloat16)
    query_lin = jnp.dot(hidden_low, qkv_full[0], preferred_element_type=jnp.float32)
    key_lin = jnp.dot(hidden_low, qkv_full[1], preferred_element_type=jnp.float32)
    value_lin = jnp.dot(hidden_low, qkv_full[2], preferred_element_type=jnp.float32)
    query_send = rotate(query_lin, places_own, 1.0).astype(jnp.bfloat16)
    key_send = rotate(key_lin, places_own, 1.0).astype(jnp.bfloat16)
    value_send = value_lin.astype(jnp.bfloat16)
    query_heads, key_heads, value_heads = lax.all_to_all(
        jnp.stack([query_send, key_send, value_send]), "seq", split_axis=2, concat_axis=1, tiled=True
    )
    attended_heads, log_totals = attend_forward(
        query_heads, key_heads, value_heads, owners_all, usable_all, group_frames
    )
    attended = lax.all_to_all(attended_heads, "seq", split_axis=0, concat_axis=1, tiled=True)
    attn_proj = jnp.dot(attended, out_full, preferred_element_type=jnp.float32)
    mid = inputs + gate_attn * attn_proj
    hidden_ff, ff_norm_back = jax.vjp(modulate, mid, shift_ff, scale_ff)
    hidden_ff_low = hidden_ff.astype(jnp.bfloat16)
    pre_act = jnp.dot(hidden_ff_low, up_full, preferred_element_type=jnp.float32)
    active, gelu_back = jax.vjp(gelu_tanh, pre_act)
    active_low = active.astype(jnp.bfloat16)
    ff_proj = jnp.dot(active_low, down_full, preferred_element_type=jnp.float32)
    result = mid + gate_ff * ff_proj
    grad_result = out_grad.astype(jnp.float32)
    grad_gate_ff = grad_result * ff_proj
    grad_ff = (grad_result * gate_ff).astype(jnp.bfloat16)
    grad_down_local = jnp.einsum(
        "nf,nd->fd", active_low, grad_ff, preferred_element_type=jnp.float32
    )
    grad_active = jnp.einsum("nd,fd->nf", grad_ff, down_full, preferred_element_type=jnp.float32)
    (grad_pre,) = gelu_back(grad_active)
    grad_pre_low = grad_pre.astype(jnp.bfloat16)
    grad_up_local = jnp.einsum(
        "nd,nf->df", hidden_ff_low, grad_pre_low, preferred_element_type=jnp.float32
    )
    grad_hidden_ff = jnp.einsum(
        "nf,df->nd", grad_pre_low, up_full, preferred_element_type=jnp.float32
    )
    grad_mid_norm, grad_shift_ff, grad_scale_ff = ff_norm_back(grad_hidden_ff)
    grad_mid = grad_result + grad_mid_norm
    grad_gate_attn = grad_mid * attn_proj
    grad_proj = (grad_mid * gate_attn).astype(jnp.bfloat16)
    grad_out_local = jnp.einsum(
        "nd,ne->de", attended, grad_proj, preferred_element_type=jnp.float32
    )
    grad_attended = jnp.einsum(
        "ne,de->nd", grad_proj, out_full, preferred_element_type=jnp.float32
    ).astype(jnp.bfloat16)
    grad_heads = lax.all_to_all(grad_attended, "seq", split_axis=1, concat_axis=0, tiled=True)
    grad_query_heads, grad_key_heads, grad_value_heads = attend_backward(
        query_heads,
        key_heads,
        value_heads,
        grad_heads,
        log_totals,
        owners_all,
        usable_all,
        group_frames,
    )
    grad_query_rows, grad_key_rows, grad_value_rows = lax.all_to_all(
        jnp.stack([grad_query_heads, grad_key_heads, grad_value_heads]),
        "seq",
        split_axis=1,
        concat_axis=2,
        tiled=True,
    )
    grad_query_lin = rotate(grad_query_rows.astype(jnp.float32), places_own, -1.0).astype(
        jnp.bfloat16
    )
    grad_key_lin = rotate(grad_key_rows.astype(jnp.float32), places_own, -1.0).astype(jnp.bfloat16)
    grad_qkv_local = jnp.stack(
        [
            jnp.einsum("nd,ne->de", hidden_low, grad_query_lin, preferred_element_type=jnp.float32),
            jnp.einsum("nd,ne->de", hidden_low, grad_key_lin, preferred_element_type=jnp.float32),
            jnp.einsum(
                "nd,ne->de", hidden_low, grad_value_rows, preferred_element_type=jnp.float32
            ),
        ]
    )
    grad_hidden = jnp.einsum(
        "ne,de->nd", grad_query_lin, qkv_full[0], preferred_element_type=jnp.float32
    )
    grad_hidden = grad_hidden + jnp.einsum(
        "ne,de->nd", grad_key_lin, qkv_full[1], preferred_element_type=jnp.float32
    )
    grad_hidden = grad_hidden + jnp.einsum(
        "ne,de->nd", grad_value_rows, qkv_full[2], preferred_element_type=jnp.float32
    )
    grad_input_norm, grad_shift_attn, grad_scale_attn = attn_norm_back(grad_hidden)
    input_grad = grad_mid + grad_input_norm
    grad_mod_rows = jnp.concatenate(
        [
            grad_shift_attn,
            grad_scale_attn,
            grad_gate_attn,
            grad_shift_ff,
            grad_scale_ff,
            grad_gate_ff,
        ],
        axis=1,
    )
    grad_mod_clip = butterfly_sum(
        jnp.einsum("nc,ne->ce", inside_own, grad_mod_rows, precision=precise), "seq", seq_count
    )
    grad_mod_all = doubling_gather(grad_mod_clip, ("z", "core"), dp_count, dp_rank).reshape(
        -1, grad_mod_clip.shape[1]
    )
    silu_all = doubling_gather(silu_part, ("z", "core"), dp_count, dp_rank).reshape(
        -1, silu_part.shape[1]
    )
    bias_cols = b_mod.shape[0]
    grad_bias_share = jnp.sum(
        lax.dynamic_slice_in_dim(grad_mod_all, seq_rank * bias_cols, bias_cols, 1), axis=0
    )
    grad_mod_share = jnp.einsum(
        "cd,ce->de", silu_all.astype(jnp.float32), grad_mod_all, precision=precise
    )
    grad_silu_part = jnp.einsum(
        "ce,de->cd", grad_mod_clip, mod_low.astype(jnp.float32), precision=precise
    )
    grad_silu = jnp.concatenate(
        list(doubling_gather(grad_silu_part, "seq", seq_count, seq_rank)), axis=1
    )
    time_grad = jax.vjp(jax.nn.silu, time_emb)[1](grad_silu)[0]
    batch_shares = reduce_batch(
        [
            grad_out_local.astype(jnp.bfloat16),
            grad_up_local.astype(jnp.bfloat16),
            grad_down_local.astype(jnp.bfloat16),
        ]
    )
    batch_shares, grad_mod_share, grad_bias_share = lax.optimization_barrier(
        (batch_shares, grad_mod_share, grad_bias_share)
    )
    grad_out, grad_up, grad_down = [share.astype(jnp.float32) for share in batch_shares]
    qkv_piece = lax.psum_scatter(
        grad_qkv_local.astype(jnp.bfloat16), ("seq", "core"), scatter_dimension=1, tiled=True
    )
    qkv_piece, batch_shares = lax.optimization_barrier((qkv_piece, batch_shares))
    updated = [
        lamb_update(w_out, mom_out, var_out, grad_out, None, seq_count),
        lamb_update(w_up, mom_up, var_up, grad_up, None, seq_count),
        lamb_update(w_down, mom_down, var_down, grad_down, None, seq_count),
        lamb_update(w_mod, mom_mod, var_mod, grad_mod_share, None, seq_count),
        lamb_update(b_mod, mom_bias, var_bias, grad_bias_share, None, seq_count),
    ]
    qkv_piece = halving_sum(qkv_piece, "z", lax.axis_size("z"))
    qkv_other = lax.ppermute(qkv_piece, "core", [(0, 1), (1, 0)])
    qkv_first = lax.axis_index("core") == 0
    grad_qkv = jnp.concatenate(
        [jnp.where(qkv_first, qkv_piece, qkv_other), jnp.where(qkv_first, qkv_other, qkv_piece)],
        axis=1,
    ).astype(jnp.float32)
    updated = [lamb_update(w_qkv, mom_qkv, var_qkv, grad_qkv, (1, 2), seq_count)] + updated
    totals = (grad_qkv, grad_out, grad_up, grad_down, grad_mod_share, grad_bias_share)
    new_masters = [entry[0] for entry in updated]
    new_moments = [entry[1] for entry in updated]
    new_seconds = [entry[2] for entry in updated]
    return (
        result.astype(jnp.bfloat16),
        input_grad,
        time_grad,
        totals[0],
        new_masters[0],
        new_moments[0],
        new_seconds[0],
        totals[1],
        new_masters[1],
        new_moments[1],
        new_seconds[1],
        totals[2],
        new_masters[2],
        new_moments[2],
        new_seconds[2],
        totals[3],
        new_masters[3],
        new_moments[3],
        new_seconds[3],
        totals[4],
        new_masters[4],
        new_moments[4],
        new_seconds[4],
        totals[5],
        new_masters[5],
        new_moments[5],
        new_seconds[5],
    )


def solution(mesh):
    devices = mesh.devices
    chip_mesh = Mesh(
        devices.reshape(devices.shape[0] // 2, 2, devices.shape[1]), ("z", "core", "seq")
    )
    return jax.shard_map(
        local,
        mesh=chip_mesh,
        in_specs=(
            P(("z", "core", "seq"), None),
            P(("z", "core", "seq"), None),
            P(("z", "core"), None),
            P(("z", "core"), None),
            P(("z", "core"), None),
            P(None, "seq", None),
            P(None, "seq", None),
            P(None, "seq", None),
            P("seq", None),
            P("seq", None),
            P("seq", None),
            P("seq", None),
            P("seq", None),
            P("seq", None),
            P("seq", None),
            P("seq", None),
            P("seq", None),
            P("seq", None),
            P("seq", None),
            P("seq", None),
            P("seq"),
            P("seq"),
            P("seq"),
        ),
        out_specs=(
            P(("z", "core", "seq"), None),
            P(("z", "core", "seq"), None),
            P(("z", "core"), None),
            P(None, "seq", None),
            P(None, "seq", None),
            P(None, "seq", None),
            P(None, "seq", None),
            P("seq", None),
            P("seq", None),
            P("seq", None),
            P("seq", None),
            P("seq", None),
            P("seq", None),
            P("seq", None),
            P("seq", None),
            P("seq", None),
            P("seq", None),
            P("seq", None),
            P("seq", None),
            P("seq", None),
            P("seq", None),
            P("seq", None),
            P("seq", None),
            P("seq"),
            P("seq"),
            P("seq"),
            P("seq"),
        ),
        check_vma=False,
    )
```

```python
import jax
import jax.numpy as jnp
from jax import lax
from jax.sharding import Mesh, PartitionSpec as P

HEAD_DIM = 64


precise = lax.Precision.HIGHEST
norm_eps = 1e-06
masked_score = -1e30
beta_one = 0.9
beta_two = 0.999
adam_eps = 1e-08
weight_decay = 0.01
step_rate = 1.0
step_count = 10


def layer_norm(values):
    center = values - jnp.mean(values, axis=-1, keepdims=True)
    spread = jnp.mean(center * center, axis=-1, keepdims=True)
    return center * lax.rsqrt(spread + norm_eps)


def modulate(values, shift, scale):
    return layer_norm(values) * (1.0 + scale) + shift


def gelu_tanh(values):
    return jax.nn.gelu(values, approximate=True)


def rotate(values, places, turn_sign):
    frame_count = values.shape[0]
    half_dim = HEAD_DIM // 2
    exponent = jnp.arange(half_dim, dtype=jnp.float32) * (-2.0 / HEAD_DIM)
    frequency = jnp.power(jnp.float32(10000.0), exponent)
    angles = places.astype(jnp.float32)[:, None] * frequency[None, :]
    cos_table = jnp.cos(angles)[:, None, :]
    sin_table = turn_sign * jnp.sin(angles)[:, None, :]
    paired = values.reshape(frame_count, values.shape[1] // HEAD_DIM, half_dim, 2)
    even_part = paired[..., 0]
    odd_part = paired[..., 1]
    turned = jnp.stack(
        [
            even_part * cos_table - odd_part * sin_table,
            odd_part * cos_table + even_part * sin_table,
        ],
        axis=-1,
    )
    return turned.reshape(frame_count, values.shape[1])


def clip_tables(lengths, padding, frame_ids):
    starts = jnp.cumsum(lengths) - lengths
    finish = starts + lengths
    inside = (frame_ids[:, None] >= starts[None, :]) & (frame_ids[:, None] < finish[None, :])
    clip_ids = jnp.arange(lengths.shape[0], dtype=jnp.int32)
    owners = jnp.sum(jnp.where(inside, clip_ids[None, :], 0), axis=1)
    begins = jnp.sum(jnp.where(inside, starts[None, :], 0), axis=1)
    kept_len = jnp.maximum(lengths - padding, 1)
    limits = jnp.sum(jnp.where(inside, kept_len[None, :], 0), axis=1)
    places = frame_ids - begins
    return (inside.astype(jnp.float32), owners, places, places < limits)


def key_window(block_index, block_rows, span, frame_count):
    return jnp.clip(block_index * block_rows - (span - block_rows) // 2, 0, frame_count - span)


def block_inputs(queries, keys_all, values, owners, usable, block_index, block_rows, span):
    frame_count, columns = queries.shape
    heads_here = columns // HEAD_DIM
    row_start = block_index * block_rows
    window = key_window(block_index, block_rows, span, frame_count)
    query_rows = lax.dynamic_slice_in_dim(queries, row_start, block_rows, 0).reshape(
        block_rows, heads_here, HEAD_DIM
    )
    keys_win = keys_all.reshape(span, heads_here, HEAD_DIM)
    values_win = values.reshape(span, heads_here, HEAD_DIM)
    query_owner = lax.dynamic_slice_in_dim(owners, row_start, block_rows, 0)
    score_scale = HEAD_DIM ** (-0.5)
    scores = (
        jnp.einsum("qhd,khd->hqk", query_rows, keys_win, preferred_element_type=jnp.float32)
        * score_scale
    )
    allowed = (query_owner[:, None] == owners[None, :]) & usable[None, :]
    masked = jnp.where(allowed[None], scores, masked_score)
    return (row_start, window, query_rows, keys_win, values_win, masked)


def attend_forward(queries, keys_all, values, owners, usable, span):
    frame_count, columns = queries.shape
    block_rows = min(512, frame_count)

    def one_block(block_index):
        row_start, window, query_rows, keys_win, values_win, masked = block_inputs(
            queries, keys_all, values, owners, usable, block_index, block_rows, span
        )
        row_max = jnp.max(masked, axis=-1, keepdims=True)
        row_total = jnp.sum(jnp.exp(masked - row_max), axis=-1, keepdims=True)
        log_total = row_max + jnp.log(row_total)
        probs_low = jnp.exp(masked - log_total).astype(jnp.bfloat16)
        attended = jnp.einsum(
            "hqk,khd->qhd", probs_low, values_win, preferred_element_type=jnp.float32
        )
        return (attended.astype(jnp.bfloat16).reshape(block_rows, columns), log_total)

    outcome, log_totals = lax.map(one_block, jnp.arange(frame_count // block_rows, dtype=jnp.int32))
    return (outcome.reshape(frame_count, columns), log_totals)


def attend_backward(queries, keys_all, values, grad_attended, log_totals, owners, usable, span):
    frame_count, columns = queries.shape
    heads_here = columns // HEAD_DIM
    block_rows = min(512, frame_count)
    score_scale = HEAD_DIM ** (-0.5)

    def one_block(sums, block_data):
        key_sum, value_sum = sums
        block_index, log_total = block_data
        row_start, window, query_rows, keys_win, values_win, masked = block_inputs(
            queries, keys_all, values, owners, usable, block_index, block_rows, span
        )
        grad_rows = lax.dynamic_slice_in_dim(grad_attended, row_start, block_rows, 0).reshape(
            block_rows, heads_here, HEAD_DIM
        )
        probs_full = jnp.exp(masked - log_total)
        probs_low = probs_full.astype(jnp.bfloat16)
        grad_probs = jnp.einsum(
            "qhd,khd->hqk", grad_rows, values_win, preferred_element_type=jnp.float32
        )
        row_delta = jnp.sum(probs_full * grad_probs, axis=-1, keepdims=True)
        grad_scores = (probs_full * (grad_probs - row_delta)).astype(jnp.bfloat16)
        grad_query = (
            jnp.einsum("hqk,khd->qhd", grad_scores, keys_win, preferred_element_type=jnp.float32)
            * score_scale
        )
        grad_key = (
            jnp.einsum("hqk,qhd->khd", grad_scores, query_rows, preferred_element_type=jnp.float32)
            * score_scale
        )
        grad_value = jnp.einsum(
            "hqk,qhd->khd", probs_low, grad_rows, preferred_element_type=jnp.float32
        )
        old_keys = key_sum
        key_sum = old_keys + grad_key.reshape(span, columns)
        old_values = value_sum
        value_sum = old_values + grad_value.reshape(span, columns)
        return ((key_sum, value_sum), grad_query.astype(jnp.bfloat16).reshape(block_rows, columns))

    zeros = jnp.zeros((frame_count, columns), jnp.float32)
    indices = jnp.arange(frame_count // block_rows, dtype=jnp.int32)
    (key_sum, value_sum), grad_queries = lax.scan(one_block, (zeros, zeros), (indices, log_totals))
    return (
        grad_queries.reshape(frame_count, columns),
        key_sum.astype(jnp.bfloat16),
        value_sum.astype(jnp.bfloat16),
    )


def butterfly_sum(values, axes, size):
    step = 1
    while step < size:
        values = values + lax.ppermute(values, axes, [(i, i ^ step) for i in range(size)])
        step *= 2
    return values


def doubling_gather(values, axes, size, index):
    blocks = values[None]
    step = 1
    while step < size:
        other = lax.ppermute(blocks, axes, [(i, i ^ step) for i in range(size)])
        low_side = (index // step) % 2 == 0
        blocks = jnp.concatenate(
            [jnp.where(low_side, blocks, other), jnp.where(low_side, other, blocks)], axis=0
        )
        step *= 2
    return blocks


def gather_rows(shard, row_axis):
    half = shard.shape[row_axis] // 2
    core = lax.axis_index("core")
    piece = lax.dynamic_slice_in_dim(shard, core * half, half, row_axis)
    return lax.all_gather(piece, ("seq", "core"), axis=row_axis, tiled=True)


def halving_sum(values, axis_name, size):
    index = lax.axis_index(axis_name)
    total = values.astype(jnp.float32)
    step = 1
    while step < size:
        half = total.shape[-1] // 2
        low_side = (index // step) % 2 == 0
        keep = jnp.where(low_side, total[..., :half], total[..., half:])
        send = jnp.where(low_side, total[..., half:], total[..., :half]).astype(jnp.bfloat16)
        total = keep + lax.ppermute(send, axis_name, [(i, i ^ step) for i in range(size)]).astype(
            jnp.float32
        )
        step *= 2
    blocks = total.astype(jnp.bfloat16)
    step = size // 2
    while step >= 1:
        other = lax.ppermute(blocks, axis_name, [(i, i ^ step) for i in range(size)])
        low_side = (index // step) % 2 == 0
        blocks = jnp.concatenate(
            [jnp.where(low_side, blocks, other), jnp.where(low_side, other, blocks)], axis=-1
        )
        step //= 2
    return blocks


def reduce_rows(partial, row_axis):
    piece = lax.psum_scatter(partial, ("seq", "core"), scatter_dimension=row_axis, tiled=True)
    piece = halving_sum(piece, "z", lax.axis_size("z"))
    other = lax.ppermute(piece, "core", [(0, 1), (1, 0)])
    first = lax.axis_index("core") == 0
    return jnp.concatenate(
        [jnp.where(first, piece, other), jnp.where(first, other, piece)], axis=row_axis
    )


def gather_batch(shards):
    core = lax.axis_index("core")
    base = min(shard.shape[1] for shard in shards)
    pieces = []
    for shard in shards:
        half = shard.shape[0] // 2
        piece = lax.dynamic_slice_in_dim(shard, core * half, half, 0)
        pieces.append(piece.reshape(-1, base))
    blocks = lax.all_gather(jnp.concatenate(pieces, axis=0), ("seq", "core"), axis=0, tiled=False)
    fulls = []
    offset = 0
    for shard, piece in zip(shards, pieces):
        rows = piece.shape[0]
        fulls.append(blocks[:, offset : offset + rows].reshape(-1, shard.shape[1]))
        offset += rows
    return fulls


def reduce_batch(partials):
    groups = lax.axis_size("seq") * 2
    base = min(part.shape[1] for part in partials)
    views = [part.reshape(groups, -1, base) for part in partials]
    flat = jnp.concatenate(views, axis=1)
    piece = lax.psum_scatter(flat, ("seq", "core"), scatter_dimension=0, tiled=True)[0]
    piece = halving_sum(piece, "z", lax.axis_size("z"))
    other = lax.ppermute(piece, "core", [(0, 1), (1, 0)])
    first = lax.axis_index("core") == 0
    low = jnp.where(first, piece, other)
    high = jnp.where(first, other, piece)
    shares = []
    offset = 0
    for part, view in zip(partials, views):
        rows = view.shape[1]
        shape = (-1, part.shape[1])
        shares.append(
            jnp.concatenate(
                [
                    low[offset : offset + rows].reshape(shape),
                    high[offset : offset + rows].reshape(shape),
                ],
                axis=0,
            )
        )
        offset += rows
    return shares


def lamb_update(weight, moment, second, grad, sum_axes, seq_count):
    moment_new, second_new, direction = adam_direction(weight, moment, second, grad)
    sums = jnp.concatenate(
        [
            jnp.sum(weight * weight, axis=sum_axes, keepdims=True),
            jnp.sum(direction * direction, axis=sum_axes, keepdims=True),
        ],
        axis=-1,
    )
    sums = butterfly_sum(sums, "seq", seq_count)
    ratio = jnp.sqrt(sums[..., :1]) * lax.rsqrt(sums[..., 1:] + 1e-06)
    return (weight - step_rate * ratio * direction, moment_new, second_new)


def adam_direction(weight, moment, second, grad):
    moment_new = beta_one * moment + (1.0 - beta_one) * grad
    second_new = beta_two * second + (1.0 - beta_two) * grad * grad
    corrected = moment_new / (1.0 - beta_one**step_count)
    scaled = second_new / (1.0 - beta_two**step_count)
    direction = corrected / (jnp.sqrt(scaled) + adam_eps) + weight_decay * weight
    return (moment_new, second_new, direction)


def local(
    frames,
    out_grad,
    time_emb,
    clip_len,
    pad_len,
    w_qkv,
    mom_qkv,
    var_qkv,
    w_out,
    mom_out,
    var_out,
    w_up,
    mom_up,
    var_up,
    w_down,
    mom_down,
    var_down,
    w_mod,
    mom_mod,
    var_mod,
    b_mod,
    mom_bias,
    var_bias,
):
    seq_count = lax.axis_size("seq")
    seq_rank = lax.axis_index("seq")
    frame_rows = frames.shape[0]
    group_frames = frame_rows * seq_count
    dp_count = lax.axis_size(("z", "core"))
    dp_rank = lax.axis_index(("z", "core"))
    qkv_full = gather_rows(w_qkv.astype(jnp.bfloat16), 1)
    out_full, up_full, down_full = gather_batch(
        [w_out.astype(jnp.bfloat16), w_up.astype(jnp.bfloat16), w_down.astype(jnp.bfloat16)]
    )
    bias_full = doubling_gather(b_mod.astype(jnp.bfloat16), "seq", seq_count, seq_rank).reshape(-1)
    mod_low = w_mod.astype(jnp.bfloat16)
    mod_rows_here = w_mod.shape[0]
    mod_first = seq_rank * mod_rows_here
    inside_all, owners_all, places_all, usable_all = clip_tables(
        clip_len[0], pad_len[0], jnp.arange(group_frames, dtype=jnp.int32)
    )
    row_first = seq_rank * frame_rows
    inside_own = lax.dynamic_slice_in_dim(inside_all, row_first, frame_rows, 0)
    places_own = lax.dynamic_slice_in_dim(places_all, row_first, frame_rows, 0)
    silu_low = jax.nn.silu(time_emb).astype(jnp.bfloat16)
    silu_part = lax.dynamic_slice_in_dim(silu_low, mod_first, mod_rows_here, 1)
    modulation = butterfly_sum(
        jnp.dot(silu_part, mod_low, preferred_element_type=jnp.float32), "seq", seq_count
    ) + bias_full.astype(jnp.float32)
    mod_rows = jnp.dot(inside_own, modulation, precision=precise)
    shift_attn, scale_attn, gate_attn, shift_ff, scale_ff, gate_ff = jnp.split(mod_rows, 6, axis=1)
    inputs = frames.astype(jnp.float32)
    hidden, attn_norm_back = jax.vjp(modulate, inputs, shift_attn, scale_attn)
    hidden_low = hidden.astype(jnp.bfloat16)
    query_lin = jnp.dot(hidden_low, qkv_full[0], preferred_element_type=jnp.float32)
    key_lin = jnp.dot(hidden_low, qkv_full[1], preferred_element_type=jnp.float32)
    value_lin = jnp.dot(hidden_low, qkv_full[2], preferred_element_type=jnp.float32)
    query_send = rotate(query_lin, places_own, 1.0).astype(jnp.bfloat16)
    key_send = rotate(key_lin, places_own, 1.0).astype(jnp.bfloat16)
    value_send = value_lin.astype(jnp.bfloat16)
    query_heads, key_heads, value_heads = (
        lax.all_to_all(query_send, "seq", split_axis=1, concat_axis=0, tiled=True),
        lax.all_to_all(key_send, "seq", split_axis=1, concat_axis=0, tiled=True),
        lax.all_to_all(value_send, "seq", split_axis=1, concat_axis=0, tiled=True),
    )
    attended_heads, log_totals = attend_forward(
        query_heads, key_heads, value_heads, owners_all, usable_all, group_frames
    )
    attended = lax.all_to_all(attended_heads, "seq", split_axis=0, concat_axis=1, tiled=True)
    attn_proj = jnp.dot(attended, out_full, preferred_element_type=jnp.float32)
    mid = inputs + gate_attn * attn_proj
    hidden_ff, ff_norm_back = jax.vjp(modulate, mid, shift_ff, scale_ff)
    hidden_ff_low = hidden_ff.astype(jnp.bfloat16)
    pre_act = jnp.dot(hidden_ff_low, up_full, preferred_element_type=jnp.float32)
    active, gelu_back = jax.vjp(gelu_tanh, pre_act)
    active_low = active.astype(jnp.bfloat16)
    ff_proj = jnp.dot(active_low, down_full, preferred_element_type=jnp.float32)
    result = mid + gate_ff * ff_proj
    grad_result = out_grad.astype(jnp.float32)
    grad_gate_ff = grad_result * ff_proj
    grad_ff = (grad_result * gate_ff).astype(jnp.bfloat16)
    grad_down_local = jnp.einsum(
        "nf,nd->fd", active_low, grad_ff, preferred_element_type=jnp.float32
    )
    grad_active = jnp.einsum("nd,fd->nf", grad_ff, down_full, preferred_element_type=jnp.float32)
    (grad_pre,) = gelu_back(grad_active)
    grad_pre_low = grad_pre.astype(jnp.bfloat16)
    grad_up_local = jnp.einsum(
        "nd,nf->df", hidden_ff_low, grad_pre_low, preferred_element_type=jnp.float32
    )
    grad_hidden_ff = jnp.einsum(
        "nf,df->nd", grad_pre_low, up_full, preferred_element_type=jnp.float32
    )
    grad_mid_norm, grad_shift_ff, grad_scale_ff = ff_norm_back(grad_hidden_ff)
    grad_mid = grad_result + grad_mid_norm
    grad_gate_attn = grad_mid * attn_proj
    grad_proj = (grad_mid * gate_attn).astype(jnp.bfloat16)
    grad_out_local = jnp.einsum(
        "nd,ne->de", attended, grad_proj, preferred_element_type=jnp.float32
    )
    grad_attended = jnp.einsum(
        "ne,de->nd", grad_proj, out_full, preferred_element_type=jnp.float32
    ).astype(jnp.bfloat16)
    grad_heads = lax.all_to_all(grad_attended, "seq", split_axis=1, concat_axis=0, tiled=True)
    grad_query_heads, grad_key_heads, grad_value_heads = attend_backward(
        query_heads,
        key_heads,
        value_heads,
        grad_heads,
        log_totals,
        owners_all,
        usable_all,
        group_frames,
    )
    grad_query_rows, grad_key_rows, grad_value_rows = (
        lax.all_to_all(grad_query_heads, "seq", split_axis=0, concat_axis=1, tiled=True),
        lax.all_to_all(grad_key_heads, "seq", split_axis=0, concat_axis=1, tiled=True),
        lax.all_to_all(grad_value_heads, "seq", split_axis=0, concat_axis=1, tiled=True),
    )
    grad_query_lin = rotate(grad_query_rows.astype(jnp.float32), places_own, -1.0).astype(
        jnp.bfloat16
    )
    grad_key_lin = rotate(grad_key_rows.astype(jnp.float32), places_own, -1.0).astype(jnp.bfloat16)
    grad_qkv_local = jnp.stack(
        [
            jnp.einsum("nd,ne->de", hidden_low, grad_query_lin, preferred_element_type=jnp.float32),
            jnp.einsum("nd,ne->de", hidden_low, grad_key_lin, preferred_element_type=jnp.float32),
            jnp.einsum(
                "nd,ne->de", hidden_low, grad_value_rows, preferred_element_type=jnp.float32
            ),
        ]
    )
    grad_hidden = jnp.einsum(
        "ne,de->nd", grad_query_lin, qkv_full[0], preferred_element_type=jnp.float32
    )
    grad_hidden = grad_hidden + jnp.einsum(
        "ne,de->nd", grad_key_lin, qkv_full[1], preferred_element_type=jnp.float32
    )
    grad_hidden = grad_hidden + jnp.einsum(
        "ne,de->nd", grad_value_rows, qkv_full[2], preferred_element_type=jnp.float32
    )
    grad_input_norm, grad_shift_attn, grad_scale_attn = attn_norm_back(grad_hidden)
    input_grad = grad_mid + grad_input_norm
    grad_mod_rows = jnp.concatenate(
        [
            grad_shift_attn,
            grad_scale_attn,
            grad_gate_attn,
            grad_shift_ff,
            grad_scale_ff,
            grad_gate_ff,
        ],
        axis=1,
    )
    grad_mod_clip = butterfly_sum(
        jnp.einsum("nc,ne->ce", inside_own, grad_mod_rows, precision=precise), "seq", seq_count
    )
    grad_mod_all = doubling_gather(grad_mod_clip, ("z", "core"), dp_count, dp_rank).reshape(
        -1, grad_mod_clip.shape[1]
    )
    silu_all = doubling_gather(silu_part, ("z", "core"), dp_count, dp_rank).reshape(
        -1, silu_part.shape[1]
    )
    bias_cols = b_mod.shape[0]
    grad_bias_share = jnp.sum(
        lax.dynamic_slice_in_dim(grad_mod_all, seq_rank * bias_cols, bias_cols, 1), axis=0
    )
    grad_mod_share = jnp.einsum(
        "cd,ce->de", silu_all.astype(jnp.float32), grad_mod_all, precision=precise
    )
    grad_silu_part = jnp.einsum(
        "ce,de->cd", grad_mod_clip, mod_low.astype(jnp.float32), precision=precise
    )
    grad_silu = jnp.concatenate(
        list(doubling_gather(grad_silu_part, "seq", seq_count, seq_rank)), axis=1
    )
    time_grad = jax.vjp(jax.nn.silu, time_emb)[1](grad_silu)[0]
    batch_shares = reduce_batch(
        [
            grad_out_local.astype(jnp.bfloat16),
            grad_up_local.astype(jnp.bfloat16),
            grad_down_local.astype(jnp.bfloat16),
        ]
    )
    qkv_partial, batch_shares, grad_mod_share, grad_bias_share = lax.optimization_barrier(
        (grad_qkv_local.astype(jnp.bfloat16), batch_shares, grad_mod_share, grad_bias_share)
    )
    grad_out, grad_up, grad_down = [share.astype(jnp.float32) for share in batch_shares]
    qkv_piece = lax.psum_scatter(qkv_partial, ("seq", "core"), scatter_dimension=1, tiled=True)
    updated = [
        lamb_update(w_out, mom_out, var_out, grad_out, None, seq_count),
        lamb_update(w_up, mom_up, var_up, grad_up, None, seq_count),
        lamb_update(w_down, mom_down, var_down, grad_down, None, seq_count),
        lamb_update(w_mod, mom_mod, var_mod, grad_mod_share, None, seq_count),
        lamb_update(b_mod, mom_bias, var_bias, grad_bias_share, None, seq_count),
    ]
    qkv_piece = halving_sum(qkv_piece, "z", lax.axis_size("z"))
    qkv_other = lax.ppermute(qkv_piece, "core", [(0, 1), (1, 0)])
    qkv_first = lax.axis_index("core") == 0
    grad_qkv = jnp.concatenate(
        [jnp.where(qkv_first, qkv_piece, qkv_other), jnp.where(qkv_first, qkv_other, qkv_piece)],
        axis=1,
    ).astype(jnp.float32)
    updated = [lamb_update(w_qkv, mom_qkv, var_qkv, grad_qkv, (1, 2), seq_count)] + updated
    totals = (grad_qkv, grad_out, grad_up, grad_down, grad_mod_share, grad_bias_share)
    new_masters = [entry[0] for entry in updated]
    new_moments = [entry[1] for entry in updated]
    new_seconds = [entry[2] for entry in updated]
    return (
        result.astype(jnp.bfloat16),
        input_grad,
        time_grad,
        totals[0],
        new_masters[0],
        new_moments[0],
        new_seconds[0],
        totals[1],
        new_masters[1],
        new_moments[1],
        new_seconds[1],
        totals[2],
        new_masters[2],
        new_moments[2],
        new_seconds[2],
        totals[3],
        new_masters[3],
        new_moments[3],
        new_seconds[3],
        totals[4],
        new_masters[4],
        new_moments[4],
        new_seconds[4],
        totals[5],
        new_masters[5],
        new_moments[5],
        new_seconds[5],
    )


def solution(mesh):
    devices = mesh.devices
    chip_mesh = Mesh(
        devices.reshape(devices.shape[0] // 2, 2, devices.shape[1]), ("z", "core", "seq")
    )
    return jax.shard_map(
        local,
        mesh=chip_mesh,
        in_specs=(
            P(("z", "core", "seq"), None),
            P(("z", "core", "seq"), None),
            P(("z", "core"), None),
            P(("z", "core"), None),
            P(("z", "core"), None),
            P(None, "seq", None),
            P(None, "seq", None),
            P(None, "seq", None),
            P("seq", None),
            P("seq", None),
            P("seq", None),
            P("seq", None),
            P("seq", None),
            P("seq", None),
            P("seq", None),
            P("seq", None),
            P("seq", None),
            P("seq", None),
            P("seq", None),
            P("seq", None),
            P("seq"),
            P("seq"),
            P("seq"),
        ),
        out_specs=(
            P(("z", "core", "seq"), None),
            P(("z", "core", "seq"), None),
            P(("z", "core"), None),
            P(None, "seq", None),
            P(None, "seq", None),
            P(None, "seq", None),
            P(None, "seq", None),
            P("seq", None),
            P("seq", None),
            P("seq", None),
            P("seq", None),
            P("seq", None),
            P("seq", None),
            P("seq", None),
            P("seq", None),
            P("seq", None),
            P("seq", None),
            P("seq", None),
            P("seq", None),
            P("seq", None),
            P("seq", None),
            P("seq", None),
            P("seq", None),
            P("seq"),
            P("seq"),
            P("seq"),
            P("seq"),
        ),
        check_vma=False,
    )
```

```python
import jax
import jax.numpy as jnp
from jax import lax
from jax.sharding import Mesh, PartitionSpec as P

HEAD_DIM = 64


precise = lax.Precision.HIGHEST
norm_eps = 1e-06
masked_score = -1e30
beta_one = 0.9
beta_two = 0.999
adam_eps = 1e-08
weight_decay = 0.01
step_rate = 1.0
step_count = 10


def layer_norm(values):
    center = values - jnp.mean(values, axis=-1, keepdims=True)
    spread = jnp.mean(center * center, axis=-1, keepdims=True)
    return center * lax.rsqrt(spread + norm_eps)


def modulate(values, shift, scale):
    return layer_norm(values) * (1.0 + scale) + shift


def gelu_tanh(values):
    return jax.nn.gelu(values, approximate=True)


def rotate(values, places, turn_sign):
    frame_count = values.shape[0]
    half_dim = HEAD_DIM // 2
    exponent = jnp.arange(half_dim, dtype=jnp.float32) * (-2.0 / HEAD_DIM)
    frequency = jnp.power(jnp.float32(10000.0), exponent)
    angles = places.astype(jnp.float32)[:, None] * frequency[None, :]
    cos_table = jnp.cos(angles)[:, None, :]
    sin_table = turn_sign * jnp.sin(angles)[:, None, :]
    paired = values.reshape(frame_count, values.shape[1] // HEAD_DIM, half_dim, 2)
    even_part = paired[..., 0]
    odd_part = paired[..., 1]
    turned = jnp.stack(
        [
            even_part * cos_table - odd_part * sin_table,
            odd_part * cos_table + even_part * sin_table,
        ],
        axis=-1,
    )
    return turned.reshape(frame_count, values.shape[1])


def clip_tables(lengths, padding, frame_ids):
    starts = jnp.cumsum(lengths) - lengths
    finish = starts + lengths
    inside = (frame_ids[:, None] >= starts[None, :]) & (frame_ids[:, None] < finish[None, :])
    clip_ids = jnp.arange(lengths.shape[0], dtype=jnp.int32)
    owners = jnp.sum(jnp.where(inside, clip_ids[None, :], 0), axis=1)
    begins = jnp.sum(jnp.where(inside, starts[None, :], 0), axis=1)
    kept_len = jnp.maximum(lengths - padding, 1)
    limits = jnp.sum(jnp.where(inside, kept_len[None, :], 0), axis=1)
    places = frame_ids - begins
    return (inside.astype(jnp.float32), owners, places, places < limits)


def key_window(block_index, block_rows, span, frame_count):
    return jnp.clip(block_index * block_rows - (span - block_rows) // 2, 0, frame_count - span)


def block_inputs(queries, keys_all, values, owners, usable, block_index, block_rows, span):
    frame_count, columns = queries.shape
    heads_here = columns // HEAD_DIM
    row_start = block_index * block_rows
    window = key_window(block_index, block_rows, span, frame_count)
    query_rows = lax.dynamic_slice_in_dim(queries, row_start, block_rows, 0).reshape(
        block_rows, heads_here, HEAD_DIM
    )
    keys_win = keys_all.reshape(span, heads_here, HEAD_DIM)
    values_win = values.reshape(span, heads_here, HEAD_DIM)
    query_owner = lax.dynamic_slice_in_dim(owners, row_start, block_rows, 0)
    score_scale = HEAD_DIM ** (-0.5)
    scores = (
        jnp.einsum("qhd,khd->hqk", query_rows, keys_win, preferred_element_type=jnp.float32)
        * score_scale
    )
    allowed = (query_owner[:, None] == owners[None, :]) & usable[None, :]
    masked = jnp.where(allowed[None], scores, masked_score)
    return (row_start, window, query_rows, keys_win, values_win, masked)


def attend_forward(queries, keys_all, values, owners, usable, span):
    frame_count, columns = queries.shape
    block_rows = min(512, frame_count)

    def one_block(block_index):
        row_start, window, query_rows, keys_win, values_win, masked = block_inputs(
            queries, keys_all, values, owners, usable, block_index, block_rows, span
        )
        row_max = jnp.max(masked, axis=-1, keepdims=True)
        row_total = jnp.sum(jnp.exp(masked - row_max), axis=-1, keepdims=True)
        log_total = row_max + jnp.log(row_total)
        probs_low = jnp.exp(masked - log_total).astype(jnp.bfloat16)
        attended = jnp.einsum(
            "hqk,khd->qhd", probs_low, values_win, preferred_element_type=jnp.float32
        )
        return (attended.astype(jnp.bfloat16).reshape(block_rows, columns), log_total)

    outcome, log_totals = lax.map(one_block, jnp.arange(frame_count // block_rows, dtype=jnp.int32))
    return (outcome.reshape(frame_count, columns), log_totals)


def attend_backward(queries, keys_all, values, grad_attended, log_totals, owners, usable, span):
    frame_count, columns = queries.shape
    heads_here = columns // HEAD_DIM
    block_rows = min(512, frame_count)
    score_scale = HEAD_DIM ** (-0.5)

    def one_block(sums, block_data):
        key_sum, value_sum = sums
        block_index, log_total = block_data
        row_start, window, query_rows, keys_win, values_win, masked = block_inputs(
            queries, keys_all, values, owners, usable, block_index, block_rows, span
        )
        grad_rows = lax.dynamic_slice_in_dim(grad_attended, row_start, block_rows, 0).reshape(
            block_rows, heads_here, HEAD_DIM
        )
        probs_full = jnp.exp(masked - log_total)
        probs_low = probs_full.astype(jnp.bfloat16)
        grad_probs = jnp.einsum(
            "qhd,khd->hqk", grad_rows, values_win, preferred_element_type=jnp.float32
        )
        row_delta = jnp.sum(probs_full * grad_probs, axis=-1, keepdims=True)
        grad_scores = (probs_full * (grad_probs - row_delta)).astype(jnp.bfloat16)
        grad_query = (
            jnp.einsum("hqk,khd->qhd", grad_scores, keys_win, preferred_element_type=jnp.float32)
            * score_scale
        )
        grad_key = (
            jnp.einsum("hqk,qhd->khd", grad_scores, query_rows, preferred_element_type=jnp.float32)
            * score_scale
        )
        grad_value = jnp.einsum(
            "hqk,qhd->khd", probs_low, grad_rows, preferred_element_type=jnp.float32
        )
        old_keys = key_sum
        key_sum = old_keys + grad_key.reshape(span, columns)
        old_values = value_sum
        value_sum = old_values + grad_value.reshape(span, columns)
        return ((key_sum, value_sum), grad_query.astype(jnp.bfloat16).reshape(block_rows, columns))

    zeros = jnp.zeros((frame_count, columns), jnp.float32)
    indices = jnp.arange(frame_count // block_rows, dtype=jnp.int32)
    (key_sum, value_sum), grad_queries = lax.scan(one_block, (zeros, zeros), (indices, log_totals))
    return (
        grad_queries.reshape(frame_count, columns),
        key_sum.astype(jnp.bfloat16),
        value_sum.astype(jnp.bfloat16),
    )


def butterfly_sum(values, axes, size):
    step = 1
    while step < size:
        values = values + lax.ppermute(values, axes, [(i, i ^ step) for i in range(size)])
        step *= 2
    return values


def doubling_gather(values, axes, size, index):
    blocks = values[None]
    step = 1
    while step < size:
        other = lax.ppermute(blocks, axes, [(i, i ^ step) for i in range(size)])
        low_side = (index // step) % 2 == 0
        blocks = jnp.concatenate(
            [jnp.where(low_side, blocks, other), jnp.where(low_side, other, blocks)], axis=0
        )
        step *= 2
    return blocks


def gather_rows(shard, row_axis):
    half = shard.shape[row_axis] // 2
    core = lax.axis_index("core")
    piece = lax.dynamic_slice_in_dim(shard, core * half, half, row_axis)
    return lax.all_gather(piece, ("seq", "core"), axis=row_axis, tiled=True)


def halving_sum(values, axis_name, size):
    index = lax.axis_index(axis_name)
    total = values.astype(jnp.float32)
    step = 1
    while step < size:
        half = total.shape[-1] // 2
        low_side = (index // step) % 2 == 0
        keep = jnp.where(low_side, total[..., :half], total[..., half:])
        send = jnp.where(low_side, total[..., half:], total[..., :half]).astype(jnp.bfloat16)
        total = keep + lax.ppermute(send, axis_name, [(i, i ^ step) for i in range(size)]).astype(
            jnp.float32
        )
        step *= 2
    blocks = total.astype(jnp.bfloat16)
    step = size // 2
    while step >= 1:
        other = lax.ppermute(blocks, axis_name, [(i, i ^ step) for i in range(size)])
        low_side = (index // step) % 2 == 0
        blocks = jnp.concatenate(
            [jnp.where(low_side, blocks, other), jnp.where(low_side, other, blocks)], axis=-1
        )
        step //= 2
    return blocks


def reduce_rows(partial, row_axis):
    piece = lax.psum_scatter(partial, ("seq", "core"), scatter_dimension=row_axis, tiled=True)
    piece = halving_sum(piece, "z", lax.axis_size("z"))
    other = lax.ppermute(piece, "core", [(0, 1), (1, 0)])
    first = lax.axis_index("core") == 0
    return jnp.concatenate(
        [jnp.where(first, piece, other), jnp.where(first, other, piece)], axis=row_axis
    )


def gather_batch(shards):
    core = lax.axis_index("core")
    base = min(shard.shape[1] for shard in shards)
    pieces = []
    for shard in shards:
        half = shard.shape[0] // 2
        piece = lax.dynamic_slice_in_dim(shard, core * half, half, 0)
        pieces.append(piece.reshape(-1, base))
    blocks = lax.all_gather(jnp.concatenate(pieces, axis=0), ("seq", "core"), axis=0, tiled=False)
    fulls = []
    offset = 0
    for shard, piece in zip(shards, pieces):
        rows = piece.shape[0]
        fulls.append(blocks[:, offset : offset + rows].reshape(-1, shard.shape[1]))
        offset += rows
    return fulls


def reduce_batch(partials):
    groups = lax.axis_size("seq") * 2
    base = min(part.shape[1] for part in partials)
    views = [part.reshape(groups, -1, base) for part in partials]
    flat = jnp.concatenate(views, axis=1)
    piece = lax.psum_scatter(flat, ("seq", "core"), scatter_dimension=0, tiled=True)[0]
    piece = lax.psum(piece, "z")
    other = lax.ppermute(piece, "core", [(0, 1), (1, 0)])
    first = lax.axis_index("core") == 0
    low = jnp.where(first, piece, other)
    high = jnp.where(first, other, piece)
    shares = []
    offset = 0
    for part, view in zip(partials, views):
        rows = view.shape[1]
        shape = (-1, part.shape[1])
        shares.append(
            jnp.concatenate(
                [
                    low[offset : offset + rows].reshape(shape),
                    high[offset : offset + rows].reshape(shape),
                ],
                axis=0,
            )
        )
        offset += rows
    return shares


def lamb_update(weight, moment, second, grad, sum_axes, seq_count):
    moment_new, second_new, direction = adam_direction(weight, moment, second, grad)
    sums = jnp.concatenate(
        [
            jnp.sum(weight * weight, axis=sum_axes, keepdims=True),
            jnp.sum(direction * direction, axis=sum_axes, keepdims=True),
        ],
        axis=-1,
    )
    sums = butterfly_sum(sums, "seq", seq_count)
    ratio = jnp.sqrt(sums[..., :1]) * lax.rsqrt(sums[..., 1:] + 1e-06)
    return (weight - step_rate * ratio * direction, moment_new, second_new)


def adam_direction(weight, moment, second, grad):
    moment_new = beta_one * moment + (1.0 - beta_one) * grad
    second_new = beta_two * second + (1.0 - beta_two) * grad * grad
    corrected = moment_new / (1.0 - beta_one**step_count)
    scaled = second_new / (1.0 - beta_two**step_count)
    direction = corrected / (jnp.sqrt(scaled) + adam_eps) + weight_decay * weight
    return (moment_new, second_new, direction)


def local(
    frames,
    out_grad,
    time_emb,
    clip_len,
    pad_len,
    w_qkv,
    mom_qkv,
    var_qkv,
    w_out,
    mom_out,
    var_out,
    w_up,
    mom_up,
    var_up,
    w_down,
    mom_down,
    var_down,
    w_mod,
    mom_mod,
    var_mod,
    b_mod,
    mom_bias,
    var_bias,
):
    seq_count = lax.axis_size("seq")
    seq_rank = lax.axis_index("seq")
    frame_rows = frames.shape[0]
    group_frames = frame_rows * seq_count
    dp_count = lax.axis_size(("z", "core"))
    dp_rank = lax.axis_index(("z", "core"))
    qkv_full = gather_rows(w_qkv.astype(jnp.bfloat16), 1)
    out_full, up_full, down_full = gather_batch(
        [w_out.astype(jnp.bfloat16), w_up.astype(jnp.bfloat16), w_down.astype(jnp.bfloat16)]
    )
    bias_full = doubling_gather(b_mod.astype(jnp.bfloat16), "seq", seq_count, seq_rank).reshape(-1)
    mod_low = w_mod.astype(jnp.bfloat16)
    mod_rows_here = w_mod.shape[0]
    mod_first = seq_rank * mod_rows_here
    inside_all, owners_all, places_all, usable_all = clip_tables(
        clip_len[0], pad_len[0], jnp.arange(group_frames, dtype=jnp.int32)
    )
    row_first = seq_rank * frame_rows
    inside_own = lax.dynamic_slice_in_dim(inside_all, row_first, frame_rows, 0)
    places_own = lax.dynamic_slice_in_dim(places_all, row_first, frame_rows, 0)
    silu_low = jax.nn.silu(time_emb).astype(jnp.bfloat16)
    silu_part = lax.dynamic_slice_in_dim(silu_low, mod_first, mod_rows_here, 1)
    modulation = butterfly_sum(
        jnp.dot(silu_part, mod_low, preferred_element_type=jnp.float32), "seq", seq_count
    ) + bias_full.astype(jnp.float32)
    mod_rows = jnp.dot(inside_own, modulation, precision=precise)
    shift_attn, scale_attn, gate_attn, shift_ff, scale_ff, gate_ff = jnp.split(mod_rows, 6, axis=1)
    inputs = frames.astype(jnp.float32)
    hidden, attn_norm_back = jax.vjp(modulate, inputs, shift_attn, scale_attn)
    hidden_low = hidden.astype(jnp.bfloat16)
    query_lin = jnp.dot(hidden_low, qkv_full[0], preferred_element_type=jnp.float32)
    key_lin = jnp.dot(hidden_low, qkv_full[1], preferred_element_type=jnp.float32)
    value_lin = jnp.dot(hidden_low, qkv_full[2], preferred_element_type=jnp.float32)
    query_send = rotate(query_lin, places_own, 1.0).astype(jnp.bfloat16)
    key_send = rotate(key_lin, places_own, 1.0).astype(jnp.bfloat16)
    value_send = value_lin.astype(jnp.bfloat16)
    query_heads, key_heads, value_heads = (
        lax.all_to_all(query_send, "seq", split_axis=1, concat_axis=0, tiled=True),
        lax.all_to_all(key_send, "seq", split_axis=1, concat_axis=0, tiled=True),
        lax.all_to_all(value_send, "seq", split_axis=1, concat_axis=0, tiled=True),
    )
    attended_heads, log_totals = attend_forward(
        query_heads, key_heads, value_heads, owners_all, usable_all, group_frames
    )
    attended = lax.all_to_all(attended_heads, "seq", split_axis=0, concat_axis=1, tiled=True)
    attn_proj = jnp.dot(attended, out_full, preferred_element_type=jnp.float32)
    mid = inputs + gate_attn * attn_proj
    hidden_ff, ff_norm_back = jax.vjp(modulate, mid, shift_ff, scale_ff)
    hidden_ff_low = hidden_ff.astype(jnp.bfloat16)
    pre_act = jnp.dot(hidden_ff_low, up_full, preferred_element_type=jnp.float32)
    active, gelu_back = jax.vjp(gelu_tanh, pre_act)
    active_low = active.astype(jnp.bfloat16)
    ff_proj = jnp.dot(active_low, down_full, preferred_element_type=jnp.float32)
    result = mid + gate_ff * ff_proj
    grad_result = out_grad.astype(jnp.float32)
    grad_gate_ff = grad_result * ff_proj
    grad_ff = (grad_result * gate_ff).astype(jnp.bfloat16)
    grad_down_local = jnp.einsum(
        "nf,nd->fd", active_low, grad_ff, preferred_element_type=jnp.float32
    )
    grad_active = jnp.einsum("nd,fd->nf", grad_ff, down_full, preferred_element_type=jnp.float32)
    (grad_pre,) = gelu_back(grad_active)
    grad_pre_low = grad_pre.astype(jnp.bfloat16)
    grad_up_local = jnp.einsum(
        "nd,nf->df", hidden_ff_low, grad_pre_low, preferred_element_type=jnp.float32
    )
    grad_hidden_ff = jnp.einsum(
        "nf,df->nd", grad_pre_low, up_full, preferred_element_type=jnp.float32
    )
    grad_mid_norm, grad_shift_ff, grad_scale_ff = ff_norm_back(grad_hidden_ff)
    grad_mid = grad_result + grad_mid_norm
    grad_gate_attn = grad_mid * attn_proj
    grad_proj = (grad_mid * gate_attn).astype(jnp.bfloat16)
    grad_out_local = jnp.einsum(
        "nd,ne->de", attended, grad_proj, preferred_element_type=jnp.float32
    )
    grad_attended = jnp.einsum(
        "ne,de->nd", grad_proj, out_full, preferred_element_type=jnp.float32
    ).astype(jnp.bfloat16)
    grad_heads = lax.all_to_all(grad_attended, "seq", split_axis=1, concat_axis=0, tiled=True)
    grad_query_heads, grad_key_heads, grad_value_heads = attend_backward(
        query_heads,
        key_heads,
        value_heads,
        grad_heads,
        log_totals,
        owners_all,
        usable_all,
        group_frames,
    )
    grad_query_rows, grad_key_rows, grad_value_rows = (
        lax.all_to_all(grad_query_heads, "seq", split_axis=0, concat_axis=1, tiled=True),
        lax.all_to_all(grad_key_heads, "seq", split_axis=0, concat_axis=1, tiled=True),
        lax.all_to_all(grad_value_heads, "seq", split_axis=0, concat_axis=1, tiled=True),
    )
    grad_query_lin = rotate(grad_query_rows.astype(jnp.float32), places_own, -1.0).astype(
        jnp.bfloat16
    )
    grad_key_lin = rotate(grad_key_rows.astype(jnp.float32), places_own, -1.0).astype(jnp.bfloat16)
    grad_qkv_local = jnp.stack(
        [
            jnp.einsum("nd,ne->de", hidden_low, grad_query_lin, preferred_element_type=jnp.float32),
            jnp.einsum("nd,ne->de", hidden_low, grad_key_lin, preferred_element_type=jnp.float32),
            jnp.einsum(
                "nd,ne->de", hidden_low, grad_value_rows, preferred_element_type=jnp.float32
            ),
        ]
    )
    grad_hidden = jnp.einsum(
        "ne,de->nd", grad_query_lin, qkv_full[0], preferred_element_type=jnp.float32
    )
    grad_hidden = grad_hidden + jnp.einsum(
        "ne,de->nd", grad_key_lin, qkv_full[1], preferred_element_type=jnp.float32
    )
    grad_hidden = grad_hidden + jnp.einsum(
        "ne,de->nd", grad_value_rows, qkv_full[2], preferred_element_type=jnp.float32
    )
    grad_input_norm, grad_shift_attn, grad_scale_attn = attn_norm_back(grad_hidden)
    input_grad = grad_mid + grad_input_norm
    grad_mod_rows = jnp.concatenate(
        [
            grad_shift_attn,
            grad_scale_attn,
            grad_gate_attn,
            grad_shift_ff,
            grad_scale_ff,
            grad_gate_ff,
        ],
        axis=1,
    )
    grad_mod_clip = butterfly_sum(
        jnp.einsum("nc,ne->ce", inside_own, grad_mod_rows, precision=precise), "seq", seq_count
    )
    grad_mod_all = doubling_gather(grad_mod_clip, ("z", "core"), dp_count, dp_rank).reshape(
        -1, grad_mod_clip.shape[1]
    )
    silu_all = doubling_gather(silu_part, ("z", "core"), dp_count, dp_rank).reshape(
        -1, silu_part.shape[1]
    )
    bias_cols = b_mod.shape[0]
    grad_bias_share = jnp.sum(
        lax.dynamic_slice_in_dim(grad_mod_all, seq_rank * bias_cols, bias_cols, 1), axis=0
    )
    grad_mod_share = jnp.einsum(
        "cd,ce->de", silu_all.astype(jnp.float32), grad_mod_all, precision=precise
    )
    grad_silu_part = jnp.einsum(
        "ce,de->cd", grad_mod_clip, mod_low.astype(jnp.float32), precision=precise
    )
    grad_silu = jnp.concatenate(
        list(doubling_gather(grad_silu_part, "seq", seq_count, seq_rank)), axis=1
    )
    time_grad = jax.vjp(jax.nn.silu, time_emb)[1](grad_silu)[0]
    batch_shares = reduce_batch(
        [
            grad_out_local.astype(jnp.bfloat16),
            grad_up_local.astype(jnp.bfloat16),
            grad_down_local.astype(jnp.bfloat16),
        ]
    )
    qkv_partial, batch_shares, grad_mod_share, grad_bias_share = lax.optimization_barrier(
        (grad_qkv_local.astype(jnp.bfloat16), batch_shares, grad_mod_share, grad_bias_share)
    )
    grad_out, grad_up, grad_down = [share.astype(jnp.float32) for share in batch_shares]
    qkv_piece = lax.psum_scatter(qkv_partial, ("seq", "core"), scatter_dimension=1, tiled=True)
    updated = [
        lamb_update(w_out, mom_out, var_out, grad_out, None, seq_count),
        lamb_update(w_up, mom_up, var_up, grad_up, None, seq_count),
        lamb_update(w_down, mom_down, var_down, grad_down, None, seq_count),
        lamb_update(w_mod, mom_mod, var_mod, grad_mod_share, None, seq_count),
        lamb_update(b_mod, mom_bias, var_bias, grad_bias_share, None, seq_count),
    ]
    qkv_piece = halving_sum(qkv_piece, "z", lax.axis_size("z"))
    qkv_other = lax.ppermute(qkv_piece, "core", [(0, 1), (1, 0)])
    qkv_first = lax.axis_index("core") == 0
    grad_qkv = jnp.concatenate(
        [jnp.where(qkv_first, qkv_piece, qkv_other), jnp.where(qkv_first, qkv_other, qkv_piece)],
        axis=1,
    ).astype(jnp.float32)
    updated = [lamb_update(w_qkv, mom_qkv, var_qkv, grad_qkv, (1, 2), seq_count)] + updated
    totals = (grad_qkv, grad_out, grad_up, grad_down, grad_mod_share, grad_bias_share)
    new_masters = [entry[0] for entry in updated]
    new_moments = [entry[1] for entry in updated]
    new_seconds = [entry[2] for entry in updated]
    return (
        result.astype(jnp.bfloat16),
        input_grad,
        time_grad,
        totals[0],
        new_masters[0],
        new_moments[0],
        new_seconds[0],
        totals[1],
        new_masters[1],
        new_moments[1],
        new_seconds[1],
        totals[2],
        new_masters[2],
        new_moments[2],
        new_seconds[2],
        totals[3],
        new_masters[3],
        new_moments[3],
        new_seconds[3],
        totals[4],
        new_masters[4],
        new_moments[4],
        new_seconds[4],
        totals[5],
        new_masters[5],
        new_moments[5],
        new_seconds[5],
    )


def solution(mesh):
    devices = mesh.devices
    chip_mesh = Mesh(
        devices.reshape(devices.shape[0] // 2, 2, devices.shape[1]), ("z", "core", "seq")
    )
    return jax.shard_map(
        local,
        mesh=chip_mesh,
        in_specs=(
            P(("z", "core", "seq"), None),
            P(("z", "core", "seq"), None),
            P(("z", "core"), None),
            P(("z", "core"), None),
            P(("z", "core"), None),
            P(None, "seq", None),
            P(None, "seq", None),
            P(None, "seq", None),
            P("seq", None),
            P("seq", None),
            P("seq", None),
            P("seq", None),
            P("seq", None),
            P("seq", None),
            P("seq", None),
            P("seq", None),
            P("seq", None),
            P("seq", None),
            P("seq", None),
            P("seq", None),
            P("seq"),
            P("seq"),
            P("seq"),
        ),
        out_specs=(
            P(("z", "core", "seq"), None),
            P(("z", "core", "seq"), None),
            P(("z", "core"), None),
            P(None, "seq", None),
            P(None, "seq", None),
            P(None, "seq", None),
            P(None, "seq", None),
            P("seq", None),
            P("seq", None),
            P("seq", None),
            P("seq", None),
            P("seq", None),
            P("seq", None),
            P("seq", None),
            P("seq", None),
            P("seq", None),
            P("seq", None),
            P("seq", None),
            P("seq", None),
            P("seq", None),
            P("seq", None),
            P("seq", None),
            P("seq", None),
            P("seq"),
            P("seq"),
            P("seq"),
            P("seq"),
        ),
        check_vma=False,
    )
```

```python
import jax
import jax.numpy as jnp
from jax import lax
from jax.sharding import Mesh, PartitionSpec as P

HEAD_DIM = 64


precise = lax.Precision.HIGHEST
norm_eps = 1e-06
masked_score = -1e30
beta_one = 0.9
beta_two = 0.999
adam_eps = 1e-08
weight_decay = 0.01
step_rate = 1.0
step_count = 10


def layer_norm(values):
    center = values - jnp.mean(values, axis=-1, keepdims=True)
    spread = jnp.mean(center * center, axis=-1, keepdims=True)
    return center * lax.rsqrt(spread + norm_eps)


def modulate(values, shift, scale):
    return layer_norm(values) * (1.0 + scale) + shift


def gelu_tanh(values):
    return jax.nn.gelu(values, approximate=True)


def rotate(values, places, turn_sign):
    frame_count = values.shape[0]
    half_dim = HEAD_DIM // 2
    exponent = jnp.arange(half_dim, dtype=jnp.float32) * (-2.0 / HEAD_DIM)
    frequency = jnp.power(jnp.float32(10000.0), exponent)
    angles = places.astype(jnp.float32)[:, None] * frequency[None, :]
    cos_table = jnp.cos(angles)[:, None, :]
    sin_table = turn_sign * jnp.sin(angles)[:, None, :]
    paired = values.reshape(frame_count, values.shape[1] // HEAD_DIM, half_dim, 2)
    even_part = paired[..., 0]
    odd_part = paired[..., 1]
    turned = jnp.stack(
        [
            even_part * cos_table - odd_part * sin_table,
            odd_part * cos_table + even_part * sin_table,
        ],
        axis=-1,
    )
    return turned.reshape(frame_count, values.shape[1])


def clip_tables(lengths, padding, frame_ids):
    starts = jnp.cumsum(lengths) - lengths
    finish = starts + lengths
    inside = (frame_ids[:, None] >= starts[None, :]) & (frame_ids[:, None] < finish[None, :])
    clip_ids = jnp.arange(lengths.shape[0], dtype=jnp.int32)
    owners = jnp.sum(jnp.where(inside, clip_ids[None, :], 0), axis=1)
    begins = jnp.sum(jnp.where(inside, starts[None, :], 0), axis=1)
    kept_len = jnp.maximum(lengths - padding, 1)
    limits = jnp.sum(jnp.where(inside, kept_len[None, :], 0), axis=1)
    places = frame_ids - begins
    return (inside.astype(jnp.float32), owners, places, places < limits)


def key_window(block_index, block_rows, span, frame_count):
    return jnp.clip(block_index * block_rows - (span - block_rows) // 2, 0, frame_count - span)


def block_inputs(queries, keys_all, values, owners, usable, block_index, block_rows, span):
    frame_count, columns = queries.shape
    heads_here = columns // HEAD_DIM
    row_start = block_index * block_rows
    window = key_window(block_index, block_rows, span, frame_count)
    query_rows = lax.dynamic_slice_in_dim(queries, row_start, block_rows, 0).reshape(
        block_rows, heads_here, HEAD_DIM
    )
    keys_win = keys_all.reshape(span, heads_here, HEAD_DIM)
    values_win = values.reshape(span, heads_here, HEAD_DIM)
    query_owner = lax.dynamic_slice_in_dim(owners, row_start, block_rows, 0)
    score_scale = HEAD_DIM ** (-0.5)
    scores = (
        jnp.einsum("qhd,khd->hqk", query_rows, keys_win, preferred_element_type=jnp.float32)
        * score_scale
    )
    allowed = (query_owner[:, None] == owners[None, :]) & usable[None, :]
    masked = jnp.where(allowed[None], scores, masked_score)
    return (row_start, window, query_rows, keys_win, values_win, masked)


def attend_forward(queries, keys_all, values, owners, usable, span):
    frame_count, columns = queries.shape
    block_rows = min(512, frame_count)

    def one_block(block_index):
        row_start, window, query_rows, keys_win, values_win, masked = block_inputs(
            queries, keys_all, values, owners, usable, block_index, block_rows, span
        )
        row_max = jnp.max(masked, axis=-1, keepdims=True)
        row_total = jnp.sum(jnp.exp(masked - row_max), axis=-1, keepdims=True)
        log_total = row_max + jnp.log(row_total)
        probs_low = jnp.exp(masked - log_total).astype(jnp.bfloat16)
        attended = jnp.einsum(
            "hqk,khd->qhd", probs_low, values_win, preferred_element_type=jnp.float32
        )
        return (attended.astype(jnp.bfloat16).reshape(block_rows, columns), log_total)

    outcome, log_totals = lax.map(one_block, jnp.arange(frame_count // block_rows, dtype=jnp.int32))
    return (outcome.reshape(frame_count, columns), log_totals)


def attend_backward(queries, keys_all, values, grad_attended, log_totals, owners, usable, span):
    frame_count, columns = queries.shape
    heads_here = columns // HEAD_DIM
    block_rows = min(512, frame_count)
    score_scale = HEAD_DIM ** (-0.5)

    def one_block(sums, block_data):
        key_sum, value_sum = sums
        block_index, log_total = block_data
        row_start, window, query_rows, keys_win, values_win, masked = block_inputs(
            queries, keys_all, values, owners, usable, block_index, block_rows, span
        )
        grad_rows = lax.dynamic_slice_in_dim(grad_attended, row_start, block_rows, 0).reshape(
            block_rows, heads_here, HEAD_DIM
        )
        probs_full = jnp.exp(masked - log_total)
        probs_low = probs_full.astype(jnp.bfloat16)
        grad_probs = jnp.einsum(
            "qhd,khd->hqk", grad_rows, values_win, preferred_element_type=jnp.float32
        )
        row_delta = jnp.sum(probs_full * grad_probs, axis=-1, keepdims=True)
        grad_scores = (probs_full * (grad_probs - row_delta)).astype(jnp.bfloat16)
        grad_query = (
            jnp.einsum("hqk,khd->qhd", grad_scores, keys_win, preferred_element_type=jnp.float32)
            * score_scale
        )
        grad_key = (
            jnp.einsum("hqk,qhd->khd", grad_scores, query_rows, preferred_element_type=jnp.float32)
            * score_scale
        )
        grad_value = jnp.einsum(
            "hqk,qhd->khd", probs_low, grad_rows, preferred_element_type=jnp.float32
        )
        old_keys = key_sum
        key_sum = old_keys + grad_key.reshape(span, columns)
        old_values = value_sum
        value_sum = old_values + grad_value.reshape(span, columns)
        return ((key_sum, value_sum), grad_query.astype(jnp.bfloat16).reshape(block_rows, columns))

    zeros = jnp.zeros((frame_count, columns), jnp.float32)
    indices = jnp.arange(frame_count // block_rows, dtype=jnp.int32)
    (key_sum, value_sum), grad_queries = lax.scan(one_block, (zeros, zeros), (indices, log_totals))
    return (
        grad_queries.reshape(frame_count, columns),
        key_sum.astype(jnp.bfloat16),
        value_sum.astype(jnp.bfloat16),
    )


def butterfly_sum(values, axes, size):
    step = 1
    while step < size:
        values = values + lax.ppermute(values, axes, [(i, i ^ step) for i in range(size)])
        step *= 2
    return values


def doubling_gather(values, axes, size, index):
    blocks = values[None]
    step = 1
    while step < size:
        other = lax.ppermute(blocks, axes, [(i, i ^ step) for i in range(size)])
        low_side = (index // step) % 2 == 0
        blocks = jnp.concatenate(
            [jnp.where(low_side, blocks, other), jnp.where(low_side, other, blocks)], axis=0
        )
        step *= 2
    return blocks


def gather_rows(shard, row_axis):
    half = shard.shape[row_axis] // 2
    core = lax.axis_index("core")
    piece = lax.dynamic_slice_in_dim(shard, core * half, half, row_axis)
    return lax.all_gather(piece, ("seq", "core"), axis=row_axis, tiled=True)


def halving_sum(values, axis_name, size):
    index = lax.axis_index(axis_name)
    total = values.astype(jnp.float32)
    step = 1
    while step < size:
        half = total.shape[-1] // 2
        low_side = (index // step) % 2 == 0
        keep = jnp.where(low_side, total[..., :half], total[..., half:])
        send = jnp.where(low_side, total[..., half:], total[..., :half]).astype(jnp.bfloat16)
        total = keep + lax.ppermute(send, axis_name, [(i, i ^ step) for i in range(size)]).astype(
            jnp.float32
        )
        step *= 2
    blocks = total.astype(jnp.bfloat16)
    step = size // 2
    while step >= 1:
        other = lax.ppermute(blocks, axis_name, [(i, i ^ step) for i in range(size)])
        low_side = (index // step) % 2 == 0
        blocks = jnp.concatenate(
            [jnp.where(low_side, blocks, other), jnp.where(low_side, other, blocks)], axis=-1
        )
        step //= 2
    return blocks


def reduce_rows(partial, row_axis):
    piece = lax.psum_scatter(partial, ("seq", "core"), scatter_dimension=row_axis, tiled=True)
    piece = halving_sum(piece, "z", lax.axis_size("z"))
    other = lax.ppermute(piece, "core", [(0, 1), (1, 0)])
    first = lax.axis_index("core") == 0
    return jnp.concatenate(
        [jnp.where(first, piece, other), jnp.where(first, other, piece)], axis=row_axis
    )


def gather_batch(shards):
    core = lax.axis_index("core")
    base = min(shard.shape[1] for shard in shards)
    pieces = []
    for shard in shards:
        half = shard.shape[0] // 2
        piece = lax.dynamic_slice_in_dim(shard, core * half, half, 0)
        pieces.append(piece.reshape(-1, base))
    blocks = lax.all_gather(jnp.concatenate(pieces, axis=0), ("seq", "core"), axis=0, tiled=False)
    fulls = []
    offset = 0
    for shard, piece in zip(shards, pieces):
        rows = piece.shape[0]
        fulls.append(blocks[:, offset : offset + rows].reshape(-1, shard.shape[1]))
        offset += rows
    return fulls


def reduce_batch(partials, after=None):
    groups = lax.axis_size("seq") * 2
    base = min(part.shape[1] for part in partials)
    views = [part.reshape(groups, -1, base) for part in partials]
    flat = jnp.concatenate(views, axis=1)
    piece = lax.psum_scatter(flat, ("seq", "core"), scatter_dimension=0, tiled=True)[0]
    if after is not None:
        piece, after = lax.optimization_barrier((piece, after))
    piece = lax.psum(piece, "z")
    other = lax.ppermute(piece, "core", [(0, 1), (1, 0)])
    first = lax.axis_index("core") == 0
    low = jnp.where(first, piece, other)
    high = jnp.where(first, other, piece)
    shares = []
    offset = 0
    for part, view in zip(partials, views):
        rows = view.shape[1]
        shape = (-1, part.shape[1])
        shares.append(
            jnp.concatenate(
                [
                    low[offset : offset + rows].reshape(shape),
                    high[offset : offset + rows].reshape(shape),
                ],
                axis=0,
            )
        )
        offset += rows
    return shares


def lamb_update(weight, moment, second, grad, sum_axes, seq_count):
    moment_new, second_new, direction = adam_direction(weight, moment, second, grad)
    sums = jnp.concatenate(
        [
            jnp.sum(weight * weight, axis=sum_axes, keepdims=True),
            jnp.sum(direction * direction, axis=sum_axes, keepdims=True),
        ],
        axis=-1,
    )
    sums = butterfly_sum(sums, "seq", seq_count)
    ratio = jnp.sqrt(sums[..., :1]) * lax.rsqrt(sums[..., 1:] + 1e-06)
    return (weight - step_rate * ratio * direction, moment_new, second_new)


def adam_direction(weight, moment, second, grad):
    moment_new = beta_one * moment + (1.0 - beta_one) * grad
    second_new = beta_two * second + (1.0 - beta_two) * grad * grad
    corrected = moment_new / (1.0 - beta_one**step_count)
    scaled = second_new / (1.0 - beta_two**step_count)
    direction = corrected / (jnp.sqrt(scaled) + adam_eps) + weight_decay * weight
    return (moment_new, second_new, direction)


def local(
    frames,
    out_grad,
    time_emb,
    clip_len,
    pad_len,
    w_qkv,
    mom_qkv,
    var_qkv,
    w_out,
    mom_out,
    var_out,
    w_up,
    mom_up,
    var_up,
    w_down,
    mom_down,
    var_down,
    w_mod,
    mom_mod,
    var_mod,
    b_mod,
    mom_bias,
    var_bias,
):
    seq_count = lax.axis_size("seq")
    seq_rank = lax.axis_index("seq")
    frame_rows = frames.shape[0]
    group_frames = frame_rows * seq_count
    dp_count = lax.axis_size(("z", "core"))
    dp_rank = lax.axis_index(("z", "core"))
    qkv_full = gather_rows(w_qkv.astype(jnp.bfloat16), 1)
    out_full, up_full, down_full = gather_batch(
        [w_out.astype(jnp.bfloat16), w_up.astype(jnp.bfloat16), w_down.astype(jnp.bfloat16)]
    )
    bias_full = doubling_gather(b_mod.astype(jnp.bfloat16), "seq", seq_count, seq_rank).reshape(-1)
    mod_low = w_mod.astype(jnp.bfloat16)
    mod_rows_here = w_mod.shape[0]
    mod_first = seq_rank * mod_rows_here
    inside_all, owners_all, places_all, usable_all = clip_tables(
        clip_len[0], pad_len[0], jnp.arange(group_frames, dtype=jnp.int32)
    )
    row_first = seq_rank * frame_rows
    inside_own = lax.dynamic_slice_in_dim(inside_all, row_first, frame_rows, 0)
    places_own = lax.dynamic_slice_in_dim(places_all, row_first, frame_rows, 0)
    silu_low = jax.nn.silu(time_emb).astype(jnp.bfloat16)
    silu_part = lax.dynamic_slice_in_dim(silu_low, mod_first, mod_rows_here, 1)
    modulation = butterfly_sum(
        jnp.dot(silu_part, mod_low, preferred_element_type=jnp.float32), "seq", seq_count
    ) + bias_full.astype(jnp.float32)
    mod_rows = jnp.dot(inside_own, modulation, precision=precise)
    shift_attn, scale_attn, gate_attn, shift_ff, scale_ff, gate_ff = jnp.split(mod_rows, 6, axis=1)
    inputs = frames.astype(jnp.float32)
    hidden, attn_norm_back = jax.vjp(modulate, inputs, shift_attn, scale_attn)
    hidden_low = hidden.astype(jnp.bfloat16)
    query_lin = jnp.dot(hidden_low, qkv_full[0], preferred_element_type=jnp.float32)
    key_lin = jnp.dot(hidden_low, qkv_full[1], preferred_element_type=jnp.float32)
    value_lin = jnp.dot(hidden_low, qkv_full[2], preferred_element_type=jnp.float32)
    query_send = rotate(query_lin, places_own, 1.0).astype(jnp.bfloat16)
    key_send = rotate(key_lin, places_own, 1.0).astype(jnp.bfloat16)
    value_send = value_lin.astype(jnp.bfloat16)
    query_heads, key_heads, value_heads = (
        lax.all_to_all(query_send, "seq", split_axis=1, concat_axis=0, tiled=True),
        lax.all_to_all(key_send, "seq", split_axis=1, concat_axis=0, tiled=True),
        lax.all_to_all(value_send, "seq", split_axis=1, concat_axis=0, tiled=True),
    )
    attended_heads, log_totals = attend_forward(
        query_heads, key_heads, value_heads, owners_all, usable_all, group_frames
    )
    attended = lax.all_to_all(attended_heads, "seq", split_axis=0, concat_axis=1, tiled=True)
    attn_proj = jnp.dot(attended, out_full, preferred_element_type=jnp.float32)
    mid = inputs + gate_attn * attn_proj
    hidden_ff, ff_norm_back = jax.vjp(modulate, mid, shift_ff, scale_ff)
    hidden_ff_low = hidden_ff.astype(jnp.bfloat16)
    pre_act = jnp.dot(hidden_ff_low, up_full, preferred_element_type=jnp.float32)
    active, gelu_back = jax.vjp(gelu_tanh, pre_act)
    active_low = active.astype(jnp.bfloat16)
    ff_proj = jnp.dot(active_low, down_full, preferred_element_type=jnp.float32)
    result = mid + gate_ff * ff_proj
    grad_result = out_grad.astype(jnp.float32)
    grad_gate_ff = grad_result * ff_proj
    grad_ff = (grad_result * gate_ff).astype(jnp.bfloat16)
    grad_down_local = jnp.einsum(
        "nf,nd->fd", active_low, grad_ff, preferred_element_type=jnp.float32
    )
    grad_active = jnp.einsum("nd,fd->nf", grad_ff, down_full, preferred_element_type=jnp.float32)
    (grad_pre,) = gelu_back(grad_active)
    grad_pre_low = grad_pre.astype(jnp.bfloat16)
    grad_up_local = jnp.einsum(
        "nd,nf->df", hidden_ff_low, grad_pre_low, preferred_element_type=jnp.float32
    )
    grad_hidden_ff = jnp.einsum(
        "nf,df->nd", grad_pre_low, up_full, preferred_element_type=jnp.float32
    )
    grad_mid_norm, grad_shift_ff, grad_scale_ff = ff_norm_back(grad_hidden_ff)
    grad_mid = grad_result + grad_mid_norm
    grad_gate_attn = grad_mid * attn_proj
    grad_proj = (grad_mid * gate_attn).astype(jnp.bfloat16)
    grad_out_local = jnp.einsum(
        "nd,ne->de", attended, grad_proj, preferred_element_type=jnp.float32
    )
    grad_attended = jnp.einsum(
        "ne,de->nd", grad_proj, out_full, preferred_element_type=jnp.float32
    ).astype(jnp.bfloat16)
    grad_heads = lax.all_to_all(grad_attended, "seq", split_axis=1, concat_axis=0, tiled=True)
    grad_query_heads, grad_key_heads, grad_value_heads = attend_backward(
        query_heads,
        key_heads,
        value_heads,
        grad_heads,
        log_totals,
        owners_all,
        usable_all,
        group_frames,
    )
    grad_query_rows, grad_key_rows, grad_value_rows = (
        lax.all_to_all(grad_query_heads, "seq", split_axis=0, concat_axis=1, tiled=True),
        lax.all_to_all(grad_key_heads, "seq", split_axis=0, concat_axis=1, tiled=True),
        lax.all_to_all(grad_value_heads, "seq", split_axis=0, concat_axis=1, tiled=True),
    )
    grad_query_lin = rotate(grad_query_rows.astype(jnp.float32), places_own, -1.0).astype(
        jnp.bfloat16
    )
    grad_key_lin = rotate(grad_key_rows.astype(jnp.float32), places_own, -1.0).astype(jnp.bfloat16)
    grad_qkv_local = jnp.stack(
        [
            jnp.einsum("nd,ne->de", hidden_low, grad_query_lin, preferred_element_type=jnp.float32),
            jnp.einsum("nd,ne->de", hidden_low, grad_key_lin, preferred_element_type=jnp.float32),
            jnp.einsum(
                "nd,ne->de", hidden_low, grad_value_rows, preferred_element_type=jnp.float32
            ),
        ]
    )
    grad_hidden = jnp.einsum(
        "ne,de->nd", grad_query_lin, qkv_full[0], preferred_element_type=jnp.float32
    )
    grad_hidden = grad_hidden + jnp.einsum(
        "ne,de->nd", grad_key_lin, qkv_full[1], preferred_element_type=jnp.float32
    )
    grad_hidden = grad_hidden + jnp.einsum(
        "ne,de->nd", grad_value_rows, qkv_full[2], preferred_element_type=jnp.float32
    )
    grad_input_norm, grad_shift_attn, grad_scale_attn = attn_norm_back(grad_hidden)
    input_grad = grad_mid + grad_input_norm
    grad_mod_rows = jnp.concatenate(
        [
            grad_shift_attn,
            grad_scale_attn,
            grad_gate_attn,
            grad_shift_ff,
            grad_scale_ff,
            grad_gate_ff,
        ],
        axis=1,
    )
    grad_mod_clip = butterfly_sum(
        jnp.einsum("nc,ne->ce", inside_own, grad_mod_rows, precision=precise), "seq", seq_count
    )
    grad_mod_all = doubling_gather(grad_mod_clip, ("z", "core"), dp_count, dp_rank).reshape(
        -1, grad_mod_clip.shape[1]
    )
    silu_all = doubling_gather(silu_part, ("z", "core"), dp_count, dp_rank).reshape(
        -1, silu_part.shape[1]
    )
    bias_cols = b_mod.shape[0]
    grad_bias_share = jnp.sum(
        lax.dynamic_slice_in_dim(grad_mod_all, seq_rank * bias_cols, bias_cols, 1), axis=0
    )
    grad_mod_share = jnp.einsum(
        "cd,ce->de", silu_all.astype(jnp.float32), grad_mod_all, precision=precise
    )
    grad_silu_part = jnp.einsum(
        "ce,de->cd", grad_mod_clip, mod_low.astype(jnp.float32), precision=precise
    )
    grad_silu = jnp.concatenate(
        list(doubling_gather(grad_silu_part, "seq", seq_count, seq_rank)), axis=1
    )
    time_grad = jax.vjp(jax.nn.silu, time_emb)[1](grad_silu)[0]
    qkv_piece = lax.psum_scatter(
        grad_qkv_local.astype(jnp.bfloat16), ("seq", "core"), scatter_dimension=1, tiled=True
    )
    batch_shares = reduce_batch(
        [
            grad_out_local.astype(jnp.bfloat16),
            grad_up_local.astype(jnp.bfloat16),
            grad_down_local.astype(jnp.bfloat16),
        ],
        after=qkv_piece,
    )
    grad_out, grad_up, grad_down = [share.astype(jnp.float32) for share in batch_shares]
    updated = [
        lamb_update(w_out, mom_out, var_out, grad_out, None, seq_count),
        lamb_update(w_up, mom_up, var_up, grad_up, None, seq_count),
        lamb_update(w_down, mom_down, var_down, grad_down, None, seq_count),
        lamb_update(w_mod, mom_mod, var_mod, grad_mod_share, None, seq_count),
        lamb_update(b_mod, mom_bias, var_bias, grad_bias_share, None, seq_count),
    ]
    qkv_piece = halving_sum(qkv_piece, "z", lax.axis_size("z"))
    qkv_other = lax.ppermute(qkv_piece, "core", [(0, 1), (1, 0)])
    qkv_first = lax.axis_index("core") == 0
    grad_qkv = jnp.concatenate(
        [jnp.where(qkv_first, qkv_piece, qkv_other), jnp.where(qkv_first, qkv_other, qkv_piece)],
        axis=1,
    ).astype(jnp.float32)
    updated = [lamb_update(w_qkv, mom_qkv, var_qkv, grad_qkv, (1, 2), seq_count)] + updated
    totals = (grad_qkv, grad_out, grad_up, grad_down, grad_mod_share, grad_bias_share)
    new_masters = [entry[0] for entry in updated]
    new_moments = [entry[1] for entry in updated]
    new_seconds = [entry[2] for entry in updated]
    return (
        result.astype(jnp.bfloat16),
        input_grad,
        time_grad,
        totals[0],
        new_masters[0],
        new_moments[0],
        new_seconds[0],
        totals[1],
        new_masters[1],
        new_moments[1],
        new_seconds[1],
        totals[2],
        new_masters[2],
        new_moments[2],
        new_seconds[2],
        totals[3],
        new_masters[3],
        new_moments[3],
        new_seconds[3],
        totals[4],
        new_masters[4],
        new_moments[4],
        new_seconds[4],
        totals[5],
        new_masters[5],
        new_moments[5],
        new_seconds[5],
    )


def solution(mesh):
    devices = mesh.devices
    chip_mesh = Mesh(
        devices.reshape(devices.shape[0] // 2, 2, devices.shape[1]), ("z", "core", "seq")
    )
    return jax.shard_map(
        local,
        mesh=chip_mesh,
        in_specs=(
            P(("z", "core", "seq"), None),
            P(("z", "core", "seq"), None),
            P(("z", "core"), None),
            P(("z", "core"), None),
            P(("z", "core"), None),
            P(None, "seq", None),
            P(None, "seq", None),
            P(None, "seq", None),
            P("seq", None),
            P("seq", None),
            P("seq", None),
            P("seq", None),
            P("seq", None),
            P("seq", None),
            P("seq", None),
            P("seq", None),
            P("seq", None),
            P("seq", None),
            P("seq", None),
            P("seq", None),
            P("seq"),
            P("seq"),
            P("seq"),
        ),
        out_specs=(
            P(("z", "core", "seq"), None),
            P(("z", "core", "seq"), None),
            P(("z", "core"), None),
            P(None, "seq", None),
            P(None, "seq", None),
            P(None, "seq", None),
            P(None, "seq", None),
            P("seq", None),
            P("seq", None),
            P("seq", None),
            P("seq", None),
            P("seq", None),
            P("seq", None),
            P("seq", None),
            P("seq", None),
            P("seq", None),
            P("seq", None),
            P("seq", None),
            P("seq", None),
            P("seq", None),
            P("seq", None),
            P("seq", None),
            P("seq", None),
            P("seq"),
            P("seq"),
            P("seq"),
            P("seq"),
        ),
        check_vma=False,
    )
```

```python
import jax
import jax.numpy as jnp
from jax import lax
from jax.sharding import Mesh, PartitionSpec as P


HEAD_DIM = 64


precise = lax.Precision.HIGHEST
norm_eps = 1e-06
masked_score = -1e30
beta_one = 0.9
beta_two = 0.999
adam_eps = 1e-08
weight_decay = 0.01
step_rate = 1.0
step_count = 10


def layer_norm(values):
    center = values - jnp.mean(values, axis=-1, keepdims=True)
    spread = jnp.mean(center * center, axis=-1, keepdims=True)
    return center * lax.rsqrt(spread + norm_eps)


def modulate(values, shift, scale):
    return layer_norm(values) * (1.0 + scale) + shift


def gelu_tanh(values):
    return jax.nn.gelu(values, approximate=True)


def rotate(values, places, turn_sign):
    frame_count = values.shape[0]
    half_dim = HEAD_DIM // 2
    exponent = jnp.arange(half_dim, dtype=jnp.float32) * (-2.0 / HEAD_DIM)
    frequency = jnp.power(jnp.float32(10000.0), exponent)
    angles = places.astype(jnp.float32)[:, None] * frequency[None, :]
    cos_table = jnp.cos(angles)[:, None, :]
    sin_table = turn_sign * jnp.sin(angles)[:, None, :]
    paired = values.reshape(frame_count, values.shape[1] // HEAD_DIM, half_dim, 2)
    even_part = paired[..., 0]
    odd_part = paired[..., 1]
    turned = jnp.stack(
        [
            even_part * cos_table - odd_part * sin_table,
            odd_part * cos_table + even_part * sin_table,
        ],
        axis=-1,
    )
    return turned.reshape(frame_count, values.shape[1])


def clip_tables(lengths, padding, frame_ids):
    starts = jnp.cumsum(lengths) - lengths
    finish = starts + lengths
    inside = (frame_ids[:, None] >= starts[None, :]) & (frame_ids[:, None] < finish[None, :])
    clip_ids = jnp.arange(lengths.shape[0], dtype=jnp.int32)
    owners = jnp.sum(jnp.where(inside, clip_ids[None, :], 0), axis=1)
    begins = jnp.sum(jnp.where(inside, starts[None, :], 0), axis=1)
    kept_len = jnp.maximum(lengths - padding, 1)
    limits = jnp.sum(jnp.where(inside, kept_len[None, :], 0), axis=1)
    places = frame_ids - begins
    return (inside.astype(jnp.float32), owners, places, places < limits)


def key_window(block_index, block_rows, span, frame_count):
    return jnp.clip(block_index * block_rows - (span - block_rows) // 2, 0, frame_count - span)


def block_inputs(queries, keys_all, values, owners, usable, block_index, block_rows, span):
    frame_count, columns = queries.shape
    heads_here = columns // HEAD_DIM
    row_start = block_index * block_rows
    window = key_window(block_index, block_rows, span, frame_count)
    query_rows = lax.dynamic_slice_in_dim(queries, row_start, block_rows, 0).reshape(
        block_rows, heads_here, HEAD_DIM
    )
    keys_win = keys_all.reshape(span, heads_here, HEAD_DIM)
    values_win = values.reshape(span, heads_here, HEAD_DIM)
    query_owner = lax.dynamic_slice_in_dim(owners, row_start, block_rows, 0)
    score_scale = HEAD_DIM ** (-0.5)
    scores = (
        jnp.einsum("qhd,khd->hqk", query_rows, keys_win, preferred_element_type=jnp.float32)
        * score_scale
    )
    allowed = (query_owner[:, None] == owners[None, :]) & usable[None, :]
    masked = jnp.where(allowed[None], scores, masked_score)
    return (row_start, window, query_rows, keys_win, values_win, masked)


def attend_forward(queries, keys_all, values, owners, usable, span):
    frame_count, columns = queries.shape
    block_rows = min(512, frame_count)

    def one_block(block_index):
        _, _, _, _, values_win, masked = block_inputs(
            queries, keys_all, values, owners, usable, block_index, block_rows, span
        )
        row_max = jnp.max(masked, axis=-1, keepdims=True)
        row_total = jnp.sum(jnp.exp(masked - row_max), axis=-1, keepdims=True)
        log_total = row_max + jnp.log(row_total)
        probs_low = jnp.exp(masked - log_total).astype(jnp.bfloat16)
        attended = jnp.einsum(
            "hqk,khd->qhd", probs_low, values_win, preferred_element_type=jnp.float32
        )
        return (attended.astype(jnp.bfloat16).reshape(block_rows, columns), log_total)

    outcome, log_totals = lax.map(one_block, jnp.arange(frame_count // block_rows, dtype=jnp.int32))
    return (outcome.reshape(frame_count, columns), log_totals)


def attend_backward(queries, keys_all, values, grad_attended, log_totals, owners, usable, span):
    frame_count, columns = queries.shape
    heads_here = columns // HEAD_DIM
    block_rows = min(512, frame_count)
    score_scale = HEAD_DIM ** (-0.5)

    def one_block(sums, block_data):
        key_sum, value_sum = sums
        block_index, log_total = block_data
        row_start, _, query_rows, keys_win, values_win, masked = block_inputs(
            queries, keys_all, values, owners, usable, block_index, block_rows, span
        )
        grad_rows = lax.dynamic_slice_in_dim(grad_attended, row_start, block_rows, 0).reshape(
            block_rows, heads_here, HEAD_DIM
        )
        probs_full = jnp.exp(masked - log_total)
        probs_low = probs_full.astype(jnp.bfloat16)
        grad_probs = jnp.einsum(
            "qhd,khd->hqk", grad_rows, values_win, preferred_element_type=jnp.float32
        )
        row_delta = jnp.sum(probs_full * grad_probs, axis=-1, keepdims=True)
        grad_scores = (probs_full * (grad_probs - row_delta)).astype(jnp.bfloat16)
        grad_query = (
            jnp.einsum("hqk,khd->qhd", grad_scores, keys_win, preferred_element_type=jnp.float32)
            * score_scale
        )
        grad_key = (
            jnp.einsum("hqk,qhd->khd", grad_scores, query_rows, preferred_element_type=jnp.float32)
            * score_scale
        )
        grad_value = jnp.einsum(
            "hqk,qhd->khd", probs_low, grad_rows, preferred_element_type=jnp.float32
        )
        old_keys = key_sum
        key_sum = old_keys + grad_key.reshape(span, columns)
        old_values = value_sum
        value_sum = old_values + grad_value.reshape(span, columns)
        return ((key_sum, value_sum), grad_query.astype(jnp.bfloat16).reshape(block_rows, columns))

    zeros = jnp.zeros((frame_count, columns), jnp.float32)
    indices = jnp.arange(frame_count // block_rows, dtype=jnp.int32)
    (key_sum, value_sum), grad_queries = lax.scan(one_block, (zeros, zeros), (indices, log_totals))
    return (
        grad_queries.reshape(frame_count, columns),
        key_sum.astype(jnp.bfloat16),
        value_sum.astype(jnp.bfloat16),
    )


def butterfly_sum(values, axes, size):
    step = 1
    while step < size:
        values = values + lax.ppermute(values, axes, [(i, i ^ step) for i in range(size)])
        step *= 2
    return values


def doubling_gather(values, axes, size, index):
    blocks = values[None]
    step = 1
    while step < size:
        other = lax.ppermute(blocks, axes, [(i, i ^ step) for i in range(size)])
        low_side = (index // step) % 2 == 0
        blocks = jnp.concatenate(
            [jnp.where(low_side, blocks, other), jnp.where(low_side, other, blocks)], axis=0
        )
        step *= 2
    return blocks


def gather_rows(shard, row_axis):
    half = shard.shape[row_axis] // 2
    core = lax.axis_index("core")
    piece = lax.dynamic_slice_in_dim(shard, core * half, half, row_axis)
    return lax.all_gather(piece, ("seq", "core"), axis=row_axis, tiled=True)


def halving_sum(values, axis_name, size):
    index = lax.axis_index(axis_name)
    total = values.astype(jnp.float32)
    step = 1
    while step < size:
        half = total.shape[-1] // 2
        low_side = (index // step) % 2 == 0
        keep = jnp.where(low_side, total[..., :half], total[..., half:])
        send = jnp.where(low_side, total[..., half:], total[..., :half]).astype(jnp.bfloat16)
        total = keep + lax.ppermute(send, axis_name, [(i, i ^ step) for i in range(size)]).astype(
            jnp.float32
        )
        step *= 2
    blocks = total.astype(jnp.bfloat16)
    step = size // 2
    while step >= 1:
        other = lax.ppermute(blocks, axis_name, [(i, i ^ step) for i in range(size)])
        low_side = (index // step) % 2 == 0
        blocks = jnp.concatenate(
            [jnp.where(low_side, blocks, other), jnp.where(low_side, other, blocks)], axis=-1
        )
        step //= 2
    return blocks


def gather_batch(shards):
    core = lax.axis_index("core")
    base = min(shard.shape[1] for shard in shards)
    pieces = []
    for shard in shards:
        half = shard.shape[0] // 2
        piece = lax.dynamic_slice_in_dim(shard, core * half, half, 0)
        pieces.append(piece.reshape(-1, base))
    blocks = lax.all_gather(jnp.concatenate(pieces, axis=0), ("seq", "core"), axis=0, tiled=False)
    fulls = []
    offset = 0
    for shard, piece in zip(shards, pieces):
        rows = piece.shape[0]
        fulls.append(blocks[:, offset : offset + rows].reshape(-1, shard.shape[1]))
        offset += rows
    return fulls


def reduce_batch(partials, after=None):
    groups = lax.axis_size("seq") * 2
    base = min(part.shape[1] for part in partials)
    views = [part.reshape(groups, -1, base) for part in partials]
    flat = jnp.concatenate(views, axis=1)
    piece = lax.psum_scatter(flat, ("seq", "core"), scatter_dimension=0, tiled=True)[0]
    if after is not None:
        piece, after = lax.optimization_barrier((piece, after))
    piece = lax.psum(piece, "z")
    other = lax.ppermute(piece, "core", [(0, 1), (1, 0)])
    first = lax.axis_index("core") == 0
    low = jnp.where(first, piece, other)
    high = jnp.where(first, other, piece)
    shares = []
    offset = 0
    for part, view in zip(partials, views):
        rows = view.shape[1]
        shape = (-1, part.shape[1])
        shares.append(
            jnp.concatenate(
                [
                    low[offset : offset + rows].reshape(shape),
                    high[offset : offset + rows].reshape(shape),
                ],
                axis=0,
            )
        )
        offset += rows
    return shares


def lamb_update(weight, moment, second, grad, sum_axes, seq_count):
    moment_new, second_new, direction = adam_direction(weight, moment, second, grad)
    sums = jnp.concatenate(
        [
            jnp.sum(weight * weight, axis=sum_axes, keepdims=True),
            jnp.sum(direction * direction, axis=sum_axes, keepdims=True),
        ],
        axis=-1,
    )
    sums = butterfly_sum(sums, "seq", seq_count)
    ratio = jnp.sqrt(sums[..., :1]) * lax.rsqrt(sums[..., 1:] + 1e-06)
    return (weight - step_rate * ratio * direction, moment_new, second_new)


def adam_direction(weight, moment, second, grad):
    moment_new = beta_one * moment + (1.0 - beta_one) * grad
    second_new = beta_two * second + (1.0 - beta_two) * grad * grad
    corrected = moment_new / (1.0 - beta_one**step_count)
    scaled = second_new / (1.0 - beta_two**step_count)
    direction = corrected / (jnp.sqrt(scaled) + adam_eps) + weight_decay * weight
    return (moment_new, second_new, direction)


def local(
    frames,
    out_grad,
    time_emb,
    clip_len,
    pad_len,
    w_qkv,
    mom_qkv,
    var_qkv,
    w_out,
    mom_out,
    var_out,
    w_up,
    mom_up,
    var_up,
    w_down,
    mom_down,
    var_down,
    w_mod,
    mom_mod,
    var_mod,
    b_mod,
    mom_bias,
    var_bias,
):
    seq_count = lax.axis_size("seq")
    seq_rank = lax.axis_index("seq")
    frame_rows = frames.shape[0]
    group_frames = frame_rows * seq_count
    dp_count = lax.axis_size(("z", "core"))
    dp_rank = lax.axis_index(("z", "core"))
    qkv_full = gather_rows(w_qkv.astype(jnp.bfloat16), 1)
    out_full, up_full, down_full = gather_batch(
        [w_out.astype(jnp.bfloat16), w_up.astype(jnp.bfloat16), w_down.astype(jnp.bfloat16)]
    )
    bias_full = doubling_gather(b_mod.astype(jnp.bfloat16), "seq", seq_count, seq_rank).reshape(-1)
    mod_low = w_mod.astype(jnp.bfloat16)
    mod_rows_here = w_mod.shape[0]
    mod_first = seq_rank * mod_rows_here
    inside_all, owners_all, places_all, usable_all = clip_tables(
        clip_len[0], pad_len[0], jnp.arange(group_frames, dtype=jnp.int32)
    )
    row_first = seq_rank * frame_rows
    inside_own = lax.dynamic_slice_in_dim(inside_all, row_first, frame_rows, 0)
    places_own = lax.dynamic_slice_in_dim(places_all, row_first, frame_rows, 0)
    silu_low = jax.nn.silu(time_emb).astype(jnp.bfloat16)
    silu_part = lax.dynamic_slice_in_dim(silu_low, mod_first, mod_rows_here, 1)
    modulation = butterfly_sum(
        jnp.dot(silu_part, mod_low, preferred_element_type=jnp.float32), "seq", seq_count
    ) + bias_full.astype(jnp.float32)
    mod_rows = jnp.dot(inside_own, modulation, precision=precise)
    shift_attn, scale_attn, gate_attn, shift_ff, scale_ff, gate_ff = jnp.split(mod_rows, 6, axis=1)
    inputs = frames.astype(jnp.float32)
    hidden, attn_norm_back = jax.vjp(modulate, inputs, shift_attn, scale_attn)
    hidden_low = hidden.astype(jnp.bfloat16)
    query_lin = jnp.dot(hidden_low, qkv_full[0], preferred_element_type=jnp.float32)
    key_lin = jnp.dot(hidden_low, qkv_full[1], preferred_element_type=jnp.float32)
    value_lin = jnp.dot(hidden_low, qkv_full[2], preferred_element_type=jnp.float32)
    query_send = rotate(query_lin, places_own, 1.0).astype(jnp.bfloat16)
    key_send = rotate(key_lin, places_own, 1.0).astype(jnp.bfloat16)
    value_send = value_lin.astype(jnp.bfloat16)
    query_heads, key_heads, value_heads = (
        lax.all_to_all(query_send, "seq", split_axis=1, concat_axis=0, tiled=True),
        lax.all_to_all(key_send, "seq", split_axis=1, concat_axis=0, tiled=True),
        lax.all_to_all(value_send, "seq", split_axis=1, concat_axis=0, tiled=True),
    )
    attended_heads, log_totals = attend_forward(
        query_heads, key_heads, value_heads, owners_all, usable_all, group_frames
    )
    attended = lax.all_to_all(attended_heads, "seq", split_axis=0, concat_axis=1, tiled=True)
    attn_proj = jnp.dot(attended, out_full, preferred_element_type=jnp.float32)
    mid = inputs + gate_attn * attn_proj
    hidden_ff, ff_norm_back = jax.vjp(modulate, mid, shift_ff, scale_ff)
    hidden_ff_low = hidden_ff.astype(jnp.bfloat16)
    pre_act = jnp.dot(hidden_ff_low, up_full, preferred_element_type=jnp.float32)
    active, gelu_back = jax.vjp(gelu_tanh, pre_act)
    active_low = active.astype(jnp.bfloat16)
    ff_proj = jnp.dot(active_low, down_full, preferred_element_type=jnp.float32)
    result = mid + gate_ff * ff_proj
    grad_result = out_grad.astype(jnp.float32)
    grad_gate_ff = grad_result * ff_proj
    grad_ff = (grad_result * gate_ff).astype(jnp.bfloat16)
    grad_down_local = jnp.einsum(
        "nf,nd->fd", active_low, grad_ff, preferred_element_type=jnp.float32
    )
    grad_active = jnp.einsum("nd,fd->nf", grad_ff, down_full, preferred_element_type=jnp.float32)
    (grad_pre,) = gelu_back(grad_active)
    grad_pre_low = grad_pre.astype(jnp.bfloat16)
    grad_up_local = jnp.einsum(
        "nd,nf->df", hidden_ff_low, grad_pre_low, preferred_element_type=jnp.float32
    )
    grad_hidden_ff = jnp.einsum(
        "nf,df->nd", grad_pre_low, up_full, preferred_element_type=jnp.float32
    )
    grad_mid_norm, grad_shift_ff, grad_scale_ff = ff_norm_back(grad_hidden_ff)
    grad_mid = grad_result + grad_mid_norm
    grad_gate_attn = grad_mid * attn_proj
    grad_proj = (grad_mid * gate_attn).astype(jnp.bfloat16)
    grad_out_local = jnp.einsum(
        "nd,ne->de", attended, grad_proj, preferred_element_type=jnp.float32
    )
    grad_attended = jnp.einsum(
        "ne,de->nd", grad_proj, out_full, preferred_element_type=jnp.float32
    ).astype(jnp.bfloat16)
    grad_heads = lax.all_to_all(grad_attended, "seq", split_axis=1, concat_axis=0, tiled=True)
    grad_heads, grad_out_local, grad_up_local, grad_down_local = lax.optimization_barrier(
        (grad_heads, grad_out_local, grad_up_local, grad_down_local)
    )
    grad_query_heads, grad_key_heads, grad_value_heads = attend_backward(
        query_heads,
        key_heads,
        value_heads,
        grad_heads,
        log_totals,
        owners_all,
        usable_all,
        group_frames,
    )
    grad_query_rows, grad_key_rows, grad_value_rows = (
        lax.all_to_all(grad_query_heads, "seq", split_axis=0, concat_axis=1, tiled=True),
        lax.all_to_all(grad_key_heads, "seq", split_axis=0, concat_axis=1, tiled=True),
        lax.all_to_all(grad_value_heads, "seq", split_axis=0, concat_axis=1, tiled=True),
    )
    grad_query_lin = rotate(grad_query_rows.astype(jnp.float32), places_own, -1.0).astype(
        jnp.bfloat16
    )
    grad_key_lin = rotate(grad_key_rows.astype(jnp.float32), places_own, -1.0).astype(jnp.bfloat16)
    grad_qkv_local = jnp.stack(
        [
            jnp.einsum("nd,ne->de", hidden_low, grad_query_lin, preferred_element_type=jnp.float32),
            jnp.einsum("nd,ne->de", hidden_low, grad_key_lin, preferred_element_type=jnp.float32),
            jnp.einsum(
                "nd,ne->de", hidden_low, grad_value_rows, preferred_element_type=jnp.float32
            ),
        ]
    )
    grad_hidden = jnp.einsum(
        "ne,de->nd", grad_query_lin, qkv_full[0], preferred_element_type=jnp.float32
    )
    grad_hidden = grad_hidden + jnp.einsum(
        "ne,de->nd", grad_key_lin, qkv_full[1], preferred_element_type=jnp.float32
    )
    grad_hidden = grad_hidden + jnp.einsum(
        "ne,de->nd", grad_value_rows, qkv_full[2], preferred_element_type=jnp.float32
    )
    grad_input_norm, grad_shift_attn, grad_scale_attn = attn_norm_back(grad_hidden)
    input_grad = grad_mid + grad_input_norm
    grad_mod_rows = jnp.concatenate(
        [
            grad_shift_attn,
            grad_scale_attn,
            grad_gate_attn,
            grad_shift_ff,
            grad_scale_ff,
            grad_gate_ff,
        ],
        axis=1,
    )
    grad_mod_clip = butterfly_sum(
        jnp.einsum("nc,ne->ce", inside_own, grad_mod_rows, precision=precise), "seq", seq_count
    )
    grad_mod_all = doubling_gather(grad_mod_clip, ("z", "core"), dp_count, dp_rank).reshape(
        -1, grad_mod_clip.shape[1]
    )
    silu_all = doubling_gather(silu_part, ("z", "core"), dp_count, dp_rank).reshape(
        -1, silu_part.shape[1]
    )
    bias_cols = b_mod.shape[0]
    grad_bias_share = jnp.sum(
        lax.dynamic_slice_in_dim(grad_mod_all, seq_rank * bias_cols, bias_cols, 1), axis=0
    )
    grad_mod_share = jnp.einsum(
        "cd,ce->de", silu_all.astype(jnp.float32), grad_mod_all, precision=precise
    )
    grad_silu_part = jnp.einsum(
        "ce,de->cd", grad_mod_clip, mod_low.astype(jnp.float32), precision=precise
    )
    grad_silu = jnp.concatenate(
        list(doubling_gather(grad_silu_part, "seq", seq_count, seq_rank)), axis=1
    )
    time_grad = jax.vjp(jax.nn.silu, time_emb)[1](grad_silu)[0]
    qkv_piece = lax.psum_scatter(
        grad_qkv_local.astype(jnp.bfloat16), ("seq", "core"), scatter_dimension=1, tiled=True
    )
    batch_shares = reduce_batch(
        [
            grad_out_local.astype(jnp.bfloat16),
            grad_up_local.astype(jnp.bfloat16),
            grad_down_local.astype(jnp.bfloat16),
        ],
        after=qkv_piece,
    )
    grad_out, grad_up, grad_down = [share.astype(jnp.float32) for share in batch_shares]
    updated = [
        lamb_update(w_out, mom_out, var_out, grad_out, None, seq_count),
        lamb_update(w_up, mom_up, var_up, grad_up, None, seq_count),
        lamb_update(w_down, mom_down, var_down, grad_down, None, seq_count),
    ]
    updated += [
        lamb_update(w_mod, mom_mod, var_mod, grad_mod_share, None, seq_count),
        lamb_update(b_mod, mom_bias, var_bias, grad_bias_share, None, seq_count),
    ]
    qkv_piece = halving_sum(qkv_piece, "z", lax.axis_size("z"))
    qkv_other = lax.ppermute(qkv_piece, "core", [(0, 1), (1, 0)])
    qkv_first = lax.axis_index("core") == 0
    grad_qkv = jnp.concatenate(
        [jnp.where(qkv_first, qkv_piece, qkv_other), jnp.where(qkv_first, qkv_other, qkv_piece)],
        axis=1,
    ).astype(jnp.float32)
    updated = [lamb_update(w_qkv, mom_qkv, var_qkv, grad_qkv, (1, 2), seq_count)] + updated
    totals = (grad_qkv, grad_out, grad_up, grad_down, grad_mod_share, grad_bias_share)
    new_masters = [entry[0] for entry in updated]
    new_moments = [entry[1] for entry in updated]
    new_seconds = [entry[2] for entry in updated]
    return (
        result.astype(jnp.bfloat16),
        input_grad,
        time_grad,
        totals[0],
        new_masters[0],
        new_moments[0],
        new_seconds[0],
        totals[1],
        new_masters[1],
        new_moments[1],
        new_seconds[1],
        totals[2],
        new_masters[2],
        new_moments[2],
        new_seconds[2],
        totals[3],
        new_masters[3],
        new_moments[3],
        new_seconds[3],
        totals[4],
        new_masters[4],
        new_moments[4],
        new_seconds[4],
        totals[5],
        new_masters[5],
        new_moments[5],
        new_seconds[5],
    )


def solution(mesh):
    devices = mesh.devices
    chip_mesh = Mesh(
        devices.reshape(devices.shape[0] // 2, 2, devices.shape[1]), ("z", "core", "seq")
    )
    return jax.shard_map(
        local,
        mesh=chip_mesh,
        in_specs=(
            P(("z", "core", "seq"), None),
            P(("z", "core", "seq"), None),
            P(("z", "core"), None),
            P(("z", "core"), None),
            P(("z", "core"), None),
            P(None, "seq", None),
            P(None, "seq", None),
            P(None, "seq", None),
            P("seq", None),
            P("seq", None),
            P("seq", None),
            P("seq", None),
            P("seq", None),
            P("seq", None),
            P("seq", None),
            P("seq", None),
            P("seq", None),
            P("seq", None),
            P("seq", None),
            P("seq", None),
            P("seq"),
            P("seq"),
            P("seq"),
        ),
        out_specs=(
            P(("z", "core", "seq"), None),
            P(("z", "core", "seq"), None),
            P(("z", "core"), None),
            P(None, "seq", None),
            P(None, "seq", None),
            P(None, "seq", None),
            P(None, "seq", None),
            P("seq", None),
            P("seq", None),
            P("seq", None),
            P("seq", None),
            P("seq", None),
            P("seq", None),
            P("seq", None),
            P("seq", None),
            P("seq", None),
            P("seq", None),
            P("seq", None),
            P("seq", None),
            P("seq", None),
            P("seq", None),
            P("seq", None),
            P("seq", None),
            P("seq"),
            P("seq"),
            P("seq"),
            P("seq"),
        ),
        check_vma=False,
    )
```

```python
import jax
import jax.numpy as jnp
from jax import lax
from jax.sharding import Mesh, PartitionSpec as P


HEAD_DIM = 64


precise = lax.Precision.HIGHEST
norm_eps = 1e-06
masked_score = -1e30
beta_one = 0.9
beta_two = 0.999
adam_eps = 1e-08
weight_decay = 0.01
step_rate = 1.0
step_count = 10


def layer_norm(values):
    center = values - jnp.mean(values, axis=-1, keepdims=True)
    spread = jnp.mean(center * center, axis=-1, keepdims=True)
    return center * lax.rsqrt(spread + norm_eps)


def modulate(values, shift, scale):
    return layer_norm(values) * (1.0 + scale) + shift


def gelu_tanh(values):
    return jax.nn.gelu(values, approximate=True)


def rotate(values, places, turn_sign):
    frame_count = values.shape[0]
    half_dim = HEAD_DIM // 2
    exponent = jnp.arange(half_dim, dtype=jnp.float32) * (-2.0 / HEAD_DIM)
    frequency = jnp.power(jnp.float32(10000.0), exponent)
    angles = places.astype(jnp.float32)[:, None] * frequency[None, :]
    cos_table = jnp.cos(angles)[:, None, :]
    sin_table = turn_sign * jnp.sin(angles)[:, None, :]
    paired = values.reshape(frame_count, values.shape[1] // HEAD_DIM, half_dim, 2)
    even_part = paired[..., 0]
    odd_part = paired[..., 1]
    turned = jnp.stack(
        [
            even_part * cos_table - odd_part * sin_table,
            odd_part * cos_table + even_part * sin_table,
        ],
        axis=-1,
    )
    return turned.reshape(frame_count, values.shape[1])


def clip_tables(lengths, padding, frame_ids):
    starts = jnp.cumsum(lengths) - lengths
    finish = starts + lengths
    inside = (frame_ids[:, None] >= starts[None, :]) & (frame_ids[:, None] < finish[None, :])
    clip_ids = jnp.arange(lengths.shape[0], dtype=jnp.int32)
    owners = jnp.sum(jnp.where(inside, clip_ids[None, :], 0), axis=1)
    begins = jnp.sum(jnp.where(inside, starts[None, :], 0), axis=1)
    kept_len = jnp.maximum(lengths - padding, 1)
    limits = jnp.sum(jnp.where(inside, kept_len[None, :], 0), axis=1)
    places = frame_ids - begins
    return (inside.astype(jnp.float32), owners, places, places < limits)


def key_window(block_index, block_rows, span, frame_count):
    return jnp.clip(block_index * block_rows - (span - block_rows) // 2, 0, frame_count - span)


def block_inputs(queries, keys_all, values, owners, usable, block_index, block_rows, span):
    frame_count, columns = queries.shape
    heads_here = columns // HEAD_DIM
    row_start = block_index * block_rows
    window = key_window(block_index, block_rows, span, frame_count)
    query_rows = lax.dynamic_slice_in_dim(queries, row_start, block_rows, 0).reshape(
        block_rows, heads_here, HEAD_DIM
    )
    keys_win = keys_all.reshape(span, heads_here, HEAD_DIM)
    values_win = values.reshape(span, heads_here, HEAD_DIM)
    query_owner = lax.dynamic_slice_in_dim(owners, row_start, block_rows, 0)
    score_scale = HEAD_DIM ** (-0.5)
    scores = (
        jnp.einsum("qhd,khd->hqk", query_rows, keys_win, preferred_element_type=jnp.float32)
        * score_scale
    )
    allowed = (query_owner[:, None] == owners[None, :]) & usable[None, :]
    masked = jnp.where(allowed[None], scores, masked_score)
    return (row_start, window, query_rows, keys_win, values_win, masked)


def attend_forward(queries, keys_all, values, owners, usable, span):
    frame_count, columns = queries.shape
    block_rows = min(512, frame_count)

    def one_block(block_index):
        _, _, _, _, values_win, masked = block_inputs(
            queries, keys_all, values, owners, usable, block_index, block_rows, span
        )
        row_max = jnp.max(masked, axis=-1, keepdims=True)
        row_total = jnp.sum(jnp.exp(masked - row_max), axis=-1, keepdims=True)
        log_total = row_max + jnp.log(row_total)
        probs_low = jnp.exp(masked - log_total).astype(jnp.bfloat16)
        attended = jnp.einsum(
            "hqk,khd->qhd", probs_low, values_win, preferred_element_type=jnp.float32
        )
        return (attended.astype(jnp.bfloat16).reshape(block_rows, columns), log_total)

    outcome, log_totals = lax.map(one_block, jnp.arange(frame_count // block_rows, dtype=jnp.int32))
    return (outcome.reshape(frame_count, columns), log_totals)


def attend_backward(queries, keys_all, values, grad_attended, log_totals, owners, usable, span):
    frame_count, columns = queries.shape
    heads_here = columns // HEAD_DIM
    block_rows = min(512, frame_count)
    score_scale = HEAD_DIM ** (-0.5)

    def one_block(sums, block_data):
        key_sum, value_sum = sums
        block_index, log_total = block_data
        row_start, _, query_rows, keys_win, values_win, masked = block_inputs(
            queries, keys_all, values, owners, usable, block_index, block_rows, span
        )
        grad_rows = lax.dynamic_slice_in_dim(grad_attended, row_start, block_rows, 0).reshape(
            block_rows, heads_here, HEAD_DIM
        )
        probs_full = jnp.exp(masked - log_total)
        probs_low = probs_full.astype(jnp.bfloat16)
        grad_probs = jnp.einsum(
            "qhd,khd->hqk", grad_rows, values_win, preferred_element_type=jnp.float32
        )
        row_delta = jnp.sum(probs_full * grad_probs, axis=-1, keepdims=True)
        grad_scores = (probs_full * (grad_probs - row_delta)).astype(jnp.bfloat16)
        grad_query = (
            jnp.einsum("hqk,khd->qhd", grad_scores, keys_win, preferred_element_type=jnp.float32)
            * score_scale
        )
        grad_key = (
            jnp.einsum("hqk,qhd->khd", grad_scores, query_rows, preferred_element_type=jnp.float32)
            * score_scale
        )
        grad_value = jnp.einsum(
            "hqk,qhd->khd", probs_low, grad_rows, preferred_element_type=jnp.float32
        )
        old_keys = key_sum
        key_sum = old_keys + grad_key.reshape(span, columns)
        old_values = value_sum
        value_sum = old_values + grad_value.reshape(span, columns)
        return ((key_sum, value_sum), grad_query.astype(jnp.bfloat16).reshape(block_rows, columns))

    zeros = jnp.zeros((frame_count, columns), jnp.float32)
    indices = jnp.arange(frame_count // block_rows, dtype=jnp.int32)
    (key_sum, value_sum), grad_queries = lax.scan(one_block, (zeros, zeros), (indices, log_totals))
    return (
        grad_queries.reshape(frame_count, columns),
        key_sum.astype(jnp.bfloat16),
        value_sum.astype(jnp.bfloat16),
    )


def butterfly_sum(values, axes, size):
    step = 1
    while step < size:
        values = values + lax.ppermute(values, axes, [(i, i ^ step) for i in range(size)])
        step *= 2
    return values


def doubling_gather(values, axes, size, index):
    blocks = values[None]
    step = 1
    while step < size:
        other = lax.ppermute(blocks, axes, [(i, i ^ step) for i in range(size)])
        low_side = (index // step) % 2 == 0
        blocks = jnp.concatenate(
            [jnp.where(low_side, blocks, other), jnp.where(low_side, other, blocks)], axis=0
        )
        step *= 2
    return blocks


def gather_rows(shard, row_axis):
    half = shard.shape[row_axis] // 2
    core = lax.axis_index("core")
    piece = lax.dynamic_slice_in_dim(shard, core * half, half, row_axis)
    return lax.all_gather(piece, ("seq", "core"), axis=row_axis, tiled=True)


def halving_sum(values, axis_name, size):
    index = lax.axis_index(axis_name)
    total = values.astype(jnp.float32)
    step = 1
    while step < size:
        half = total.shape[-1] // 2
        low_side = (index // step) % 2 == 0
        keep = jnp.where(low_side, total[..., :half], total[..., half:])
        send = jnp.where(low_side, total[..., half:], total[..., :half]).astype(jnp.bfloat16)
        total = keep + lax.ppermute(send, axis_name, [(i, i ^ step) for i in range(size)]).astype(
            jnp.float32
        )
        step *= 2
    blocks = total.astype(jnp.bfloat16)
    step = size // 2
    while step >= 1:
        other = lax.ppermute(blocks, axis_name, [(i, i ^ step) for i in range(size)])
        low_side = (index // step) % 2 == 0
        blocks = jnp.concatenate(
            [jnp.where(low_side, blocks, other), jnp.where(low_side, other, blocks)], axis=-1
        )
        step //= 2
    return blocks


def gather_batch(shards):
    core = lax.axis_index("core")
    base = min(shard.shape[1] for shard in shards)
    pieces = []
    for shard in shards:
        half = shard.shape[0] // 2
        piece = lax.dynamic_slice_in_dim(shard, core * half, half, 0)
        pieces.append(piece.reshape(-1, base))
    blocks = lax.all_gather(jnp.concatenate(pieces, axis=0), ("seq", "core"), axis=0, tiled=False)
    fulls = []
    offset = 0
    for shard, piece in zip(shards, pieces):
        rows = piece.shape[0]
        fulls.append(blocks[:, offset : offset + rows].reshape(-1, shard.shape[1]))
        offset += rows
    return fulls


def reduce_batch(partials, after=None):
    groups = lax.axis_size("seq") * 2
    base = min(part.shape[1] for part in partials)
    views = [part.reshape(groups, -1, base) for part in partials]
    flat = jnp.concatenate(views, axis=1)
    piece = lax.psum_scatter(flat, ("seq", "core"), scatter_dimension=0, tiled=True)[0]
    if after is not None:
        piece, after = lax.optimization_barrier((piece, after))
    piece = lax.psum(piece, "z")
    other = lax.ppermute(piece, "core", [(0, 1), (1, 0)])
    first = lax.axis_index("core") == 0
    low = jnp.where(first, piece, other)
    high = jnp.where(first, other, piece)
    shares = []
    offset = 0
    for part, view in zip(partials, views):
        rows = view.shape[1]
        shape = (-1, part.shape[1])
        shares.append(
            jnp.concatenate(
                [
                    low[offset : offset + rows].reshape(shape),
                    high[offset : offset + rows].reshape(shape),
                ],
                axis=0,
            )
        )
        offset += rows
    return shares


def lamb_group(entries, seq_count):
    steps = []
    flat = []
    for weight, moment, second, grad, sum_axes in entries:
        moment_new, second_new, direction = adam_direction(weight, moment, second, grad)
        weight_sq = jnp.sum(weight * weight, axis=sum_axes, keepdims=True)
        update_sq = jnp.sum(direction * direction, axis=sum_axes, keepdims=True)
        steps.append((weight, moment_new, second_new, direction, weight_sq.shape))
        flat += [weight_sq.reshape(-1), update_sq.reshape(-1)]
    sums = butterfly_sum(jnp.concatenate(flat), "seq", seq_count)
    results = []
    offset = 0
    for weight, moment_new, second_new, direction, shape in steps:
        count = flat[len(results) * 2].size
        weight_sq = sums[offset : offset + count].reshape(shape)
        update_sq = sums[offset + count : offset + 2 * count].reshape(shape)
        offset += 2 * count
        ratio = jnp.sqrt(weight_sq) * lax.rsqrt(update_sq + 1e-06)
        results.append((weight - step_rate * ratio * direction, moment_new, second_new))
    return results


def adam_direction(weight, moment, second, grad):
    moment_new = beta_one * moment + (1.0 - beta_one) * grad
    second_new = beta_two * second + (1.0 - beta_two) * grad * grad
    corrected = moment_new / (1.0 - beta_one**step_count)
    scaled = second_new / (1.0 - beta_two**step_count)
    direction = corrected / (jnp.sqrt(scaled) + adam_eps) + weight_decay * weight
    return (moment_new, second_new, direction)


def local(
    frames,
    out_grad,
    time_emb,
    clip_len,
    pad_len,
    w_qkv,
    mom_qkv,
    var_qkv,
    w_out,
    mom_out,
    var_out,
    w_up,
    mom_up,
    var_up,
    w_down,
    mom_down,
    var_down,
    w_mod,
    mom_mod,
    var_mod,
    b_mod,
    mom_bias,
    var_bias,
):
    seq_count = lax.axis_size("seq")
    seq_rank = lax.axis_index("seq")
    frame_rows = frames.shape[0]
    group_frames = frame_rows * seq_count
    dp_count = lax.axis_size(("z", "core"))
    dp_rank = lax.axis_index(("z", "core"))
    qkv_full = gather_rows(w_qkv.astype(jnp.bfloat16), 1)
    out_full, up_full, down_full = gather_batch(
        [w_out.astype(jnp.bfloat16), w_up.astype(jnp.bfloat16), w_down.astype(jnp.bfloat16)]
    )
    bias_full = doubling_gather(b_mod.astype(jnp.bfloat16), "seq", seq_count, seq_rank).reshape(-1)
    mod_low = w_mod.astype(jnp.bfloat16)
    mod_rows_here = w_mod.shape[0]
    mod_first = seq_rank * mod_rows_here
    inside_all, owners_all, places_all, usable_all = clip_tables(
        clip_len[0], pad_len[0], jnp.arange(group_frames, dtype=jnp.int32)
    )
    row_first = seq_rank * frame_rows
    inside_own = lax.dynamic_slice_in_dim(inside_all, row_first, frame_rows, 0)
    places_own = lax.dynamic_slice_in_dim(places_all, row_first, frame_rows, 0)
    silu_low = jax.nn.silu(time_emb).astype(jnp.bfloat16)
    silu_part = lax.dynamic_slice_in_dim(silu_low, mod_first, mod_rows_here, 1)
    modulation = butterfly_sum(
        jnp.dot(silu_part, mod_low, preferred_element_type=jnp.float32), "seq", seq_count
    ) + bias_full.astype(jnp.float32)
    mod_rows = jnp.dot(inside_own, modulation, precision=precise)
    shift_attn, scale_attn, gate_attn, shift_ff, scale_ff, gate_ff = jnp.split(mod_rows, 6, axis=1)
    inputs = frames.astype(jnp.float32)
    hidden, attn_norm_back = jax.vjp(modulate, inputs, shift_attn, scale_attn)
    hidden_low = hidden.astype(jnp.bfloat16)
    query_lin = jnp.dot(hidden_low, qkv_full[0], preferred_element_type=jnp.float32)
    key_lin = jnp.dot(hidden_low, qkv_full[1], preferred_element_type=jnp.float32)
    value_lin = jnp.dot(hidden_low, qkv_full[2], preferred_element_type=jnp.float32)
    query_send = rotate(query_lin, places_own, 1.0).astype(jnp.bfloat16)
    key_send = rotate(key_lin, places_own, 1.0).astype(jnp.bfloat16)
    value_send = value_lin.astype(jnp.bfloat16)
    query_heads, key_heads, value_heads = (
        lax.all_to_all(query_send, "seq", split_axis=1, concat_axis=0, tiled=True),
        lax.all_to_all(key_send, "seq", split_axis=1, concat_axis=0, tiled=True),
        lax.all_to_all(value_send, "seq", split_axis=1, concat_axis=0, tiled=True),
    )
    attended_heads, log_totals = attend_forward(
        query_heads, key_heads, value_heads, owners_all, usable_all, group_frames
    )
    attended = lax.all_to_all(attended_heads, "seq", split_axis=0, concat_axis=1, tiled=True)
    attn_proj = jnp.dot(attended, out_full, preferred_element_type=jnp.float32)
    mid = inputs + gate_attn * attn_proj
    hidden_ff, ff_norm_back = jax.vjp(modulate, mid, shift_ff, scale_ff)
    hidden_ff_low = hidden_ff.astype(jnp.bfloat16)
    pre_act = jnp.dot(hidden_ff_low, up_full, preferred_element_type=jnp.float32)
    active, gelu_back = jax.vjp(gelu_tanh, pre_act)
    active_low = active.astype(jnp.bfloat16)
    ff_proj = jnp.dot(active_low, down_full, preferred_element_type=jnp.float32)
    result = mid + gate_ff * ff_proj
    grad_result = out_grad.astype(jnp.float32)
    grad_gate_ff = grad_result * ff_proj
    grad_ff = (grad_result * gate_ff).astype(jnp.bfloat16)
    grad_down_local = jnp.einsum(
        "nf,nd->fd", active_low, grad_ff, preferred_element_type=jnp.float32
    )
    grad_active = jnp.einsum("nd,fd->nf", grad_ff, down_full, preferred_element_type=jnp.float32)
    (grad_pre,) = gelu_back(grad_active)
    grad_pre_low = grad_pre.astype(jnp.bfloat16)
    grad_up_local = jnp.einsum(
        "nd,nf->df", hidden_ff_low, grad_pre_low, preferred_element_type=jnp.float32
    )
    grad_hidden_ff = jnp.einsum(
        "nf,df->nd", grad_pre_low, up_full, preferred_element_type=jnp.float32
    )
    grad_mid_norm, grad_shift_ff, grad_scale_ff = ff_norm_back(grad_hidden_ff)
    grad_mid = grad_result + grad_mid_norm
    grad_gate_attn = grad_mid * attn_proj
    grad_proj = (grad_mid * gate_attn).astype(jnp.bfloat16)
    grad_out_local = jnp.einsum(
        "nd,ne->de", attended, grad_proj, preferred_element_type=jnp.float32
    )
    grad_attended = jnp.einsum(
        "ne,de->nd", grad_proj, out_full, preferred_element_type=jnp.float32
    ).astype(jnp.bfloat16)
    grad_heads = lax.all_to_all(grad_attended, "seq", split_axis=1, concat_axis=0, tiled=True)
    grad_heads, grad_out_local, grad_up_local, grad_down_local = lax.optimization_barrier(
        (grad_heads, grad_out_local, grad_up_local, grad_down_local)
    )
    grad_query_heads, grad_key_heads, grad_value_heads = attend_backward(
        query_heads,
        key_heads,
        value_heads,
        grad_heads,
        log_totals,
        owners_all,
        usable_all,
        group_frames,
    )
    grad_query_rows, grad_key_rows, grad_value_rows = (
        lax.all_to_all(grad_query_heads, "seq", split_axis=0, concat_axis=1, tiled=True),
        lax.all_to_all(grad_key_heads, "seq", split_axis=0, concat_axis=1, tiled=True),
        lax.all_to_all(grad_value_heads, "seq", split_axis=0, concat_axis=1, tiled=True),
    )
    grad_query_lin = rotate(grad_query_rows.astype(jnp.float32), places_own, -1.0).astype(
        jnp.bfloat16
    )
    grad_key_lin = rotate(grad_key_rows.astype(jnp.float32), places_own, -1.0).astype(jnp.bfloat16)
    grad_qkv_local = jnp.stack(
        [
            jnp.einsum("nd,ne->de", hidden_low, grad_query_lin, preferred_element_type=jnp.float32),
            jnp.einsum("nd,ne->de", hidden_low, grad_key_lin, preferred_element_type=jnp.float32),
            jnp.einsum(
                "nd,ne->de", hidden_low, grad_value_rows, preferred_element_type=jnp.float32
            ),
        ]
    )
    grad_hidden = jnp.einsum(
        "ne,de->nd", grad_query_lin, qkv_full[0], preferred_element_type=jnp.float32
    )
    grad_hidden = grad_hidden + jnp.einsum(
        "ne,de->nd", grad_key_lin, qkv_full[1], preferred_element_type=jnp.float32
    )
    grad_hidden = grad_hidden + jnp.einsum(
        "ne,de->nd", grad_value_rows, qkv_full[2], preferred_element_type=jnp.float32
    )
    grad_input_norm, grad_shift_attn, grad_scale_attn = attn_norm_back(grad_hidden)
    input_grad = grad_mid + grad_input_norm
    grad_mod_rows = jnp.concatenate(
        [
            grad_shift_attn,
            grad_scale_attn,
            grad_gate_attn,
            grad_shift_ff,
            grad_scale_ff,
            grad_gate_ff,
        ],
        axis=1,
    )
    grad_mod_clip = butterfly_sum(
        jnp.einsum("nc,ne->ce", inside_own, grad_mod_rows, precision=precise), "seq", seq_count
    )
    grad_mod_all = doubling_gather(grad_mod_clip, ("z", "core"), dp_count, dp_rank).reshape(
        -1, grad_mod_clip.shape[1]
    )
    silu_all = doubling_gather(silu_part, ("z", "core"), dp_count, dp_rank).reshape(
        -1, silu_part.shape[1]
    )
    bias_cols = b_mod.shape[0]
    grad_bias_share = jnp.sum(
        lax.dynamic_slice_in_dim(grad_mod_all, seq_rank * bias_cols, bias_cols, 1), axis=0
    )
    grad_mod_share = jnp.einsum(
        "cd,ce->de", silu_all.astype(jnp.float32), grad_mod_all, precision=precise
    )
    grad_silu_part = jnp.einsum(
        "ce,de->cd", grad_mod_clip, mod_low.astype(jnp.float32), precision=precise
    )
    grad_silu = jnp.concatenate(
        list(doubling_gather(grad_silu_part, "seq", seq_count, seq_rank)), axis=1
    )
    time_grad = jax.vjp(jax.nn.silu, time_emb)[1](grad_silu)[0]
    qkv_piece = lax.psum_scatter(
        grad_qkv_local.astype(jnp.bfloat16), ("seq", "core"), scatter_dimension=1, tiled=True
    )
    batch_shares = reduce_batch(
        [
            grad_out_local.astype(jnp.bfloat16),
            grad_up_local.astype(jnp.bfloat16),
            grad_down_local.astype(jnp.bfloat16),
        ],
        after=qkv_piece,
    )
    grad_out, grad_up, grad_down = [share.astype(jnp.float32) for share in batch_shares]
    updated = lamb_group(
        [
            (w_out, mom_out, var_out, grad_out, None),
            (w_up, mom_up, var_up, grad_up, None),
            (w_down, mom_down, var_down, grad_down, None),
        ],
        seq_count,
    )
    updated += lamb_group(
        [
            (w_mod, mom_mod, var_mod, grad_mod_share, None),
            (b_mod, mom_bias, var_bias, grad_bias_share, None),
        ],
        seq_count,
    )
    qkv_piece = halving_sum(qkv_piece, "z", lax.axis_size("z"))
    qkv_other = lax.ppermute(qkv_piece, "core", [(0, 1), (1, 0)])
    qkv_first = lax.axis_index("core") == 0
    grad_qkv = jnp.concatenate(
        [jnp.where(qkv_first, qkv_piece, qkv_other), jnp.where(qkv_first, qkv_other, qkv_piece)],
        axis=1,
    ).astype(jnp.float32)
    updated = lamb_group([(w_qkv, mom_qkv, var_qkv, grad_qkv, (1, 2))], seq_count) + updated
    totals = (grad_qkv, grad_out, grad_up, grad_down, grad_mod_share, grad_bias_share)
    new_masters = [entry[0] for entry in updated]
    new_moments = [entry[1] for entry in updated]
    new_seconds = [entry[2] for entry in updated]
    return (
        result.astype(jnp.bfloat16),
        input_grad,
        time_grad,
        totals[0],
        new_masters[0],
        new_moments[0],
        new_seconds[0],
        totals[1],
        new_masters[1],
        new_moments[1],
        new_seconds[1],
        totals[2],
        new_masters[2],
        new_moments[2],
        new_seconds[2],
        totals[3],
        new_masters[3],
        new_moments[3],
        new_seconds[3],
        totals[4],
        new_masters[4],
        new_moments[4],
        new_seconds[4],
        totals[5],
        new_masters[5],
        new_moments[5],
        new_seconds[5],
    )


def solution(mesh):
    devices = mesh.devices
    chip_mesh = Mesh(
        devices.reshape(devices.shape[0] // 2, 2, devices.shape[1]), ("z", "core", "seq")
    )
    return jax.shard_map(
        local,
        mesh=chip_mesh,
        in_specs=(
            P(("z", "core", "seq"), None),
            P(("z", "core", "seq"), None),
            P(("z", "core"), None),
            P(("z", "core"), None),
            P(("z", "core"), None),
            P(None, "seq", None),
            P(None, "seq", None),
            P(None, "seq", None),
            P("seq", None),
            P("seq", None),
            P("seq", None),
            P("seq", None),
            P("seq", None),
            P("seq", None),
            P("seq", None),
            P("seq", None),
            P("seq", None),
            P("seq", None),
            P("seq", None),
            P("seq", None),
            P("seq"),
            P("seq"),
            P("seq"),
        ),
        out_specs=(
            P(("z", "core", "seq"), None),
            P(("z", "core", "seq"), None),
            P(("z", "core"), None),
            P(None, "seq", None),
            P(None, "seq", None),
            P(None, "seq", None),
            P(None, "seq", None),
            P("seq", None),
            P("seq", None),
            P("seq", None),
            P("seq", None),
            P("seq", None),
            P("seq", None),
            P("seq", None),
            P("seq", None),
            P("seq", None),
            P("seq", None),
            P("seq", None),
            P("seq", None),
            P("seq", None),
            P("seq", None),
            P("seq", None),
            P("seq", None),
            P("seq"),
            P("seq"),
            P("seq"),
            P("seq"),
        ),
        check_vma=False,
    )
```

```python
import jax
import jax.numpy as jnp
from jax import lax
from jax.sharding import Mesh, PartitionSpec as P


HEAD_DIM = 64


precise = lax.Precision.HIGHEST
norm_eps = 1e-06
masked_score = -1e30
beta_one = 0.9
beta_two = 0.999
adam_eps = 1e-08
weight_decay = 0.01
step_rate = 1.0
step_count = 10


def layer_norm(values):
    center = values - jnp.mean(values, axis=-1, keepdims=True)
    spread = jnp.mean(center * center, axis=-1, keepdims=True)
    return center * lax.rsqrt(spread + norm_eps)


def modulate(values, shift, scale):
    return layer_norm(values) * (1.0 + scale) + shift


def gelu_tanh(values):
    return jax.nn.gelu(values, approximate=True)


def rotate(values, places, turn_sign):
    frame_count = values.shape[0]
    half_dim = HEAD_DIM // 2
    exponent = jnp.arange(half_dim, dtype=jnp.float32) * (-2.0 / HEAD_DIM)
    frequency = jnp.power(jnp.float32(10000.0), exponent)
    angles = places.astype(jnp.float32)[:, None] * frequency[None, :]
    cos_table = jnp.cos(angles)[:, None, :]
    sin_table = turn_sign * jnp.sin(angles)[:, None, :]
    paired = values.reshape(frame_count, values.shape[1] // HEAD_DIM, half_dim, 2)
    even_part = paired[..., 0]
    odd_part = paired[..., 1]
    turned = jnp.stack(
        [
            even_part * cos_table - odd_part * sin_table,
            odd_part * cos_table + even_part * sin_table,
        ],
        axis=-1,
    )
    return turned.reshape(frame_count, values.shape[1])


def clip_tables(lengths, padding, frame_ids):
    starts = jnp.cumsum(lengths) - lengths
    finish = starts + lengths
    inside = (frame_ids[:, None] >= starts[None, :]) & (frame_ids[:, None] < finish[None, :])
    clip_ids = jnp.arange(lengths.shape[0], dtype=jnp.int32)
    owners = jnp.sum(jnp.where(inside, clip_ids[None, :], 0), axis=1)
    begins = jnp.sum(jnp.where(inside, starts[None, :], 0), axis=1)
    kept_len = jnp.maximum(lengths - padding, 1)
    limits = jnp.sum(jnp.where(inside, kept_len[None, :], 0), axis=1)
    places = frame_ids - begins
    return (inside.astype(jnp.float32), owners, places, places < limits)


def key_window(block_index, block_rows, span, frame_count):
    return jnp.clip(block_index * block_rows - (span - block_rows) // 2, 0, frame_count - span)


def block_inputs(queries, keys_all, values, owners, usable, block_index, block_rows, span):
    frame_count, columns = queries.shape
    heads_here = columns // HEAD_DIM
    row_start = block_index * block_rows
    window = key_window(block_index, block_rows, span, frame_count)
    query_rows = lax.dynamic_slice_in_dim(queries, row_start, block_rows, 0).reshape(
        block_rows, heads_here, HEAD_DIM
    )
    keys_win = keys_all.reshape(span, heads_here, HEAD_DIM)
    values_win = values.reshape(span, heads_here, HEAD_DIM)
    query_owner = lax.dynamic_slice_in_dim(owners, row_start, block_rows, 0)
    score_scale = HEAD_DIM ** (-0.5)
    scores = (
        jnp.einsum("qhd,khd->hqk", query_rows, keys_win, preferred_element_type=jnp.float32)
        * score_scale
    )
    allowed = (query_owner[:, None] == owners[None, :]) & usable[None, :]
    masked = jnp.where(allowed[None], scores, masked_score)
    return (row_start, window, query_rows, keys_win, values_win, masked)


def attend_forward(queries, keys_all, values, owners, usable, span):
    frame_count, columns = queries.shape
    block_rows = min(512, frame_count)

    def one_block(block_index):
        _, _, _, _, values_win, masked = block_inputs(
            queries, keys_all, values, owners, usable, block_index, block_rows, span
        )
        row_max = jnp.max(masked, axis=-1, keepdims=True)
        row_total = jnp.sum(jnp.exp(masked - row_max), axis=-1, keepdims=True)
        log_total = row_max + jnp.log(row_total)
        probs_low = jnp.exp(masked - log_total).astype(jnp.bfloat16)
        attended = jnp.einsum(
            "hqk,khd->qhd", probs_low, values_win, preferred_element_type=jnp.float32
        )
        return (attended.astype(jnp.bfloat16).reshape(block_rows, columns), log_total)

    outcome, log_totals = lax.map(one_block, jnp.arange(frame_count // block_rows, dtype=jnp.int32))
    return (outcome.reshape(frame_count, columns), log_totals)


def attend_backward(queries, keys_all, values, grad_attended, log_totals, owners, usable, span):
    frame_count, columns = queries.shape
    heads_here = columns // HEAD_DIM
    block_rows = min(512, frame_count)
    score_scale = HEAD_DIM ** (-0.5)

    def one_block(sums, block_data):
        key_sum, value_sum = sums
        block_index, log_total = block_data
        row_start, _, query_rows, keys_win, values_win, masked = block_inputs(
            queries, keys_all, values, owners, usable, block_index, block_rows, span
        )
        grad_rows = lax.dynamic_slice_in_dim(grad_attended, row_start, block_rows, 0).reshape(
            block_rows, heads_here, HEAD_DIM
        )
        probs_full = jnp.exp(masked - log_total)
        probs_low = probs_full.astype(jnp.bfloat16)
        grad_probs = jnp.einsum(
            "qhd,khd->hqk", grad_rows, values_win, preferred_element_type=jnp.float32
        )
        row_delta = jnp.sum(probs_full * grad_probs, axis=-1, keepdims=True)
        grad_scores = (probs_full * (grad_probs - row_delta)).astype(jnp.bfloat16)
        grad_query = (
            jnp.einsum("hqk,khd->qhd", grad_scores, keys_win, preferred_element_type=jnp.float32)
            * score_scale
        )
        grad_key = (
            jnp.einsum("hqk,qhd->khd", grad_scores, query_rows, preferred_element_type=jnp.float32)
            * score_scale
        )
        grad_value = jnp.einsum(
            "hqk,qhd->khd", probs_low, grad_rows, preferred_element_type=jnp.float32
        )
        old_keys = key_sum
        key_sum = old_keys + grad_key.reshape(span, columns)
        old_values = value_sum
        value_sum = old_values + grad_value.reshape(span, columns)
        return ((key_sum, value_sum), grad_query.astype(jnp.bfloat16).reshape(block_rows, columns))

    zeros = jnp.zeros((frame_count, columns), jnp.float32)
    indices = jnp.arange(frame_count // block_rows, dtype=jnp.int32)
    (key_sum, value_sum), grad_queries = lax.scan(one_block, (zeros, zeros), (indices, log_totals))
    return (
        grad_queries.reshape(frame_count, columns),
        key_sum.astype(jnp.bfloat16),
        value_sum.astype(jnp.bfloat16),
    )


def butterfly_sum(values, axes, size):
    step = 1
    while step < size:
        values = values + lax.ppermute(values, axes, [(i, i ^ step) for i in range(size)])
        step *= 2
    return values


def doubling_gather(values, axes, size, index):
    blocks = values[None]
    step = 1
    while step < size:
        other = lax.ppermute(blocks, axes, [(i, i ^ step) for i in range(size)])
        low_side = (index // step) % 2 == 0
        blocks = jnp.concatenate(
            [jnp.where(low_side, blocks, other), jnp.where(low_side, other, blocks)], axis=0
        )
        step *= 2
    return blocks


def gather_rows(shard, row_axis):
    half = shard.shape[row_axis] // 2
    core = lax.axis_index("core")
    piece = lax.dynamic_slice_in_dim(shard, core * half, half, row_axis)
    return lax.all_gather(piece, ("seq", "core"), axis=row_axis, tiled=True)


def halving_sum(values, axis_name, size):
    index = lax.axis_index(axis_name)
    total = values.astype(jnp.float32)
    step = 1
    while step < size:
        half = total.shape[-1] // 2
        low_side = (index // step) % 2 == 0
        keep = jnp.where(low_side, total[..., :half], total[..., half:])
        send = jnp.where(low_side, total[..., half:], total[..., :half]).astype(jnp.bfloat16)
        total = keep + lax.ppermute(send, axis_name, [(i, i ^ step) for i in range(size)]).astype(
            jnp.float32
        )
        step *= 2
    blocks = total.astype(jnp.bfloat16)
    step = size // 2
    while step >= 1:
        other = lax.ppermute(blocks, axis_name, [(i, i ^ step) for i in range(size)])
        low_side = (index // step) % 2 == 0
        blocks = jnp.concatenate(
            [jnp.where(low_side, blocks, other), jnp.where(low_side, other, blocks)], axis=-1
        )
        step //= 2
    return blocks


def gather_batch(shards):
    core = lax.axis_index("core")
    base = min(shard.shape[1] for shard in shards)
    pieces = []
    for shard in shards:
        half = shard.shape[0] // 2
        piece = lax.dynamic_slice_in_dim(shard, core * half, half, 0)
        pieces.append(piece.reshape(-1, base))
    blocks = lax.all_gather(jnp.concatenate(pieces, axis=0), ("seq", "core"), axis=0, tiled=False)
    fulls = []
    offset = 0
    for shard, piece in zip(shards, pieces):
        rows = piece.shape[0]
        fulls.append(blocks[:, offset : offset + rows].reshape(-1, shard.shape[1]))
        offset += rows
    return fulls


def reduce_batch(partials, after=None):
    groups = lax.axis_size("seq") * 2
    base = min(part.shape[1] for part in partials)
    views = [part.reshape(groups, -1, base) for part in partials]
    flat = jnp.concatenate(views, axis=1)
    piece = lax.psum_scatter(flat, ("seq", "core"), scatter_dimension=0, tiled=True)[0]
    if after is not None:
        piece, after = lax.optimization_barrier((piece, after))
    piece = lax.psum(piece, "z")
    other = lax.ppermute(piece, "core", [(0, 1), (1, 0)])
    first = lax.axis_index("core") == 0
    low = jnp.where(first, piece, other)
    high = jnp.where(first, other, piece)
    shares = []
    offset = 0
    for part, view in zip(partials, views):
        rows = view.shape[1]
        shape = (-1, part.shape[1])
        shares.append(
            jnp.concatenate(
                [
                    low[offset : offset + rows].reshape(shape),
                    high[offset : offset + rows].reshape(shape),
                ],
                axis=0,
            )
        )
        offset += rows
    return shares


def lamb_group(entries, seq_count):
    steps = []
    flat = []
    for weight, moment, second, grad, sum_axes in entries:
        moment_new, second_new, direction = adam_direction(weight, moment, second, grad)
        weight_sq = jnp.sum(weight * weight, axis=sum_axes, keepdims=True)
        update_sq = jnp.sum(direction * direction, axis=sum_axes, keepdims=True)
        steps.append((weight, moment_new, second_new, direction, weight_sq.shape))
        flat += [weight_sq.reshape(-1), update_sq.reshape(-1)]
    sums = butterfly_sum(jnp.concatenate(flat), "seq", seq_count)
    results = []
    offset = 0
    for weight, moment_new, second_new, direction, shape in steps:
        count = flat[len(results) * 2].size
        weight_sq = sums[offset : offset + count].reshape(shape)
        update_sq = sums[offset + count : offset + 2 * count].reshape(shape)
        offset += 2 * count
        ratio = jnp.sqrt(weight_sq) * lax.rsqrt(update_sq + 1e-06)
        results.append((weight - step_rate * ratio * direction, moment_new, second_new))
    return results


def adam_direction(weight, moment, second, grad):
    moment_new = beta_one * moment + (1.0 - beta_one) * grad
    second_new = beta_two * second + (1.0 - beta_two) * grad * grad
    corrected = moment_new / (1.0 - beta_one**step_count)
    scaled = second_new / (1.0 - beta_two**step_count)
    direction = corrected / (jnp.sqrt(scaled) + adam_eps) + weight_decay * weight
    return (moment_new, second_new, direction)


def local(
    frames,
    out_grad,
    time_emb,
    clip_len,
    pad_len,
    w_qkv,
    mom_qkv,
    var_qkv,
    w_out,
    mom_out,
    var_out,
    w_up,
    mom_up,
    var_up,
    w_down,
    mom_down,
    var_down,
    w_mod,
    mom_mod,
    var_mod,
    b_mod,
    mom_bias,
    var_bias,
):
    seq_count = lax.axis_size("seq")
    seq_rank = lax.axis_index("seq")
    frame_rows = frames.shape[0]
    group_frames = frame_rows * seq_count
    dp_count = lax.axis_size(("z", "core"))
    dp_rank = lax.axis_index(("z", "core"))
    qkv_full = gather_rows(w_qkv.astype(jnp.bfloat16), 1)
    out_full, up_full, down_full = gather_batch(
        [w_out.astype(jnp.bfloat16), w_up.astype(jnp.bfloat16), w_down.astype(jnp.bfloat16)]
    )
    bias_full = doubling_gather(b_mod.astype(jnp.bfloat16), "seq", seq_count, seq_rank).reshape(-1)
    mod_low = w_mod.astype(jnp.bfloat16)
    mod_rows_here = w_mod.shape[0]
    mod_first = seq_rank * mod_rows_here
    inside_all, owners_all, places_all, usable_all = clip_tables(
        clip_len[0], pad_len[0], jnp.arange(group_frames, dtype=jnp.int32)
    )
    row_first = seq_rank * frame_rows
    inside_own = lax.dynamic_slice_in_dim(inside_all, row_first, frame_rows, 0)
    places_own = lax.dynamic_slice_in_dim(places_all, row_first, frame_rows, 0)
    silu_low = jax.nn.silu(time_emb).astype(jnp.bfloat16)
    silu_part = lax.dynamic_slice_in_dim(silu_low, mod_first, mod_rows_here, 1)
    modulation = butterfly_sum(
        jnp.dot(silu_part, mod_low, preferred_element_type=jnp.float32), "seq", seq_count
    ) + bias_full.astype(jnp.float32)
    mod_rows = jnp.dot(inside_own, modulation, precision=precise)
    shift_attn, scale_attn, gate_attn, shift_ff, scale_ff, gate_ff = jnp.split(mod_rows, 6, axis=1)
    inputs = frames.astype(jnp.float32)
    hidden, attn_norm_back = jax.vjp(modulate, inputs, shift_attn, scale_attn)
    hidden_low = hidden.astype(jnp.bfloat16)
    query_lin = jnp.dot(hidden_low, qkv_full[0], preferred_element_type=jnp.float32)
    key_lin = jnp.dot(hidden_low, qkv_full[1], preferred_element_type=jnp.float32)
    value_lin = jnp.dot(hidden_low, qkv_full[2], preferred_element_type=jnp.float32)
    query_send = rotate(query_lin, places_own, 1.0).astype(jnp.bfloat16)
    key_send = rotate(key_lin, places_own, 1.0).astype(jnp.bfloat16)
    value_send = value_lin.astype(jnp.bfloat16)
    query_heads, key_heads, value_heads = (
        lax.all_to_all(query_send, "seq", split_axis=1, concat_axis=0, tiled=True),
        lax.all_to_all(key_send, "seq", split_axis=1, concat_axis=0, tiled=True),
        lax.all_to_all(value_send, "seq", split_axis=1, concat_axis=0, tiled=True),
    )
    attended_heads, log_totals = attend_forward(
        query_heads, key_heads, value_heads, owners_all, usable_all, group_frames
    )
    attended = lax.all_to_all(attended_heads, "seq", split_axis=0, concat_axis=1, tiled=True)
    attn_proj = jnp.dot(attended, out_full, preferred_element_type=jnp.float32)
    mid = inputs + gate_attn * attn_proj
    hidden_ff, ff_norm_back = jax.vjp(modulate, mid, shift_ff, scale_ff)
    hidden_ff_low = hidden_ff.astype(jnp.bfloat16)
    pre_act = jnp.dot(hidden_ff_low, up_full, preferred_element_type=jnp.float32)
    active, gelu_back = jax.vjp(gelu_tanh, pre_act)
    active_low = active.astype(jnp.bfloat16)
    ff_proj = jnp.dot(active_low, down_full, preferred_element_type=jnp.float32)
    result = mid + gate_ff * ff_proj
    grad_result = out_grad.astype(jnp.float32)
    grad_gate_ff = grad_result * ff_proj
    grad_ff = (grad_result * gate_ff).astype(jnp.bfloat16)
    grad_down_local = jnp.einsum(
        "nf,nd->fd", active_low, grad_ff, preferred_element_type=jnp.float32
    )
    grad_active = jnp.einsum("nd,fd->nf", grad_ff, down_full, preferred_element_type=jnp.float32)
    (grad_pre,) = gelu_back(grad_active)
    grad_pre_low = grad_pre.astype(jnp.bfloat16)
    grad_up_local = jnp.einsum(
        "nd,nf->df", hidden_ff_low, grad_pre_low, preferred_element_type=jnp.float32
    )
    grad_hidden_ff = jnp.einsum(
        "nf,df->nd", grad_pre_low, up_full, preferred_element_type=jnp.float32
    )
    grad_mid_norm, grad_shift_ff, grad_scale_ff = ff_norm_back(grad_hidden_ff)
    grad_mid = grad_result + grad_mid_norm
    grad_gate_attn = grad_mid * attn_proj
    grad_proj = (grad_mid * gate_attn).astype(jnp.bfloat16)
    grad_out_local = jnp.einsum(
        "nd,ne->de", attended, grad_proj, preferred_element_type=jnp.float32
    )
    grad_attended = jnp.einsum(
        "ne,de->nd", grad_proj, out_full, preferred_element_type=jnp.float32
    ).astype(jnp.bfloat16)
    grad_heads = lax.all_to_all(grad_attended, "seq", split_axis=1, concat_axis=0, tiled=True)
    grad_heads, grad_out_local, grad_up_local, grad_down_local = lax.optimization_barrier(
        (grad_heads, grad_out_local, grad_up_local, grad_down_local)
    )
    grad_query_heads, grad_key_heads, grad_value_heads = attend_backward(
        query_heads,
        key_heads,
        value_heads,
        grad_heads,
        log_totals,
        owners_all,
        usable_all,
        group_frames,
    )
    grad_query_rows, grad_key_rows, grad_value_rows = (
        lax.all_to_all(grad_query_heads, "seq", split_axis=0, concat_axis=1, tiled=True),
        lax.all_to_all(grad_key_heads, "seq", split_axis=0, concat_axis=1, tiled=True),
        lax.all_to_all(grad_value_heads, "seq", split_axis=0, concat_axis=1, tiled=True),
    )
    grad_query_lin = rotate(grad_query_rows.astype(jnp.float32), places_own, -1.0).astype(
        jnp.bfloat16
    )
    grad_key_lin = rotate(grad_key_rows.astype(jnp.float32), places_own, -1.0).astype(jnp.bfloat16)
    grad_qkv_local = jnp.stack(
        [
            jnp.einsum("nd,ne->de", hidden_low, grad_query_lin, preferred_element_type=jnp.float32),
            jnp.einsum("nd,ne->de", hidden_low, grad_key_lin, preferred_element_type=jnp.float32),
            jnp.einsum(
                "nd,ne->de", hidden_low, grad_value_rows, preferred_element_type=jnp.float32
            ),
        ]
    )
    grad_hidden = jnp.einsum(
        "ne,de->nd", grad_query_lin, qkv_full[0], preferred_element_type=jnp.float32
    )
    grad_hidden = grad_hidden + jnp.einsum(
        "ne,de->nd", grad_key_lin, qkv_full[1], preferred_element_type=jnp.float32
    )
    grad_hidden = grad_hidden + jnp.einsum(
        "ne,de->nd", grad_value_rows, qkv_full[2], preferred_element_type=jnp.float32
    )
    grad_input_norm, grad_shift_attn, grad_scale_attn = attn_norm_back(grad_hidden)
    input_grad = grad_mid + grad_input_norm
    grad_mod_rows = jnp.concatenate(
        [
            grad_shift_attn,
            grad_scale_attn,
            grad_gate_attn,
            grad_shift_ff,
            grad_scale_ff,
            grad_gate_ff,
        ],
        axis=1,
    )
    grad_mod_clip = butterfly_sum(
        jnp.einsum("nc,ne->ce", inside_own, grad_mod_rows, precision=precise), "seq", seq_count
    )
    grad_mod_all = doubling_gather(grad_mod_clip, ("z", "core"), dp_count, dp_rank).reshape(
        -1, grad_mod_clip.shape[1]
    )
    silu_all = doubling_gather(silu_part, ("z", "core"), dp_count, dp_rank).reshape(
        -1, silu_part.shape[1]
    )
    bias_cols = b_mod.shape[0]
    grad_bias_share = jnp.sum(
        lax.dynamic_slice_in_dim(grad_mod_all, seq_rank * bias_cols, bias_cols, 1), axis=0
    )
    grad_mod_share = jnp.einsum(
        "cd,ce->de", silu_all.astype(jnp.float32), grad_mod_all, precision=precise
    )
    grad_silu_part = jnp.einsum(
        "ce,de->cd", grad_mod_clip, mod_low.astype(jnp.float32), precision=precise
    )
    grad_silu = jnp.concatenate(
        list(doubling_gather(grad_silu_part, "seq", seq_count, seq_rank)), axis=1
    )
    time_grad = jax.vjp(jax.nn.silu, time_emb)[1](grad_silu)[0]
    qkv_piece = lax.psum_scatter(
        grad_qkv_local.astype(jnp.bfloat16), ("seq", "core"), scatter_dimension=1, tiled=True
    )
    batch_shares = reduce_batch(
        [
            grad_out_local.astype(jnp.bfloat16),
            grad_up_local.astype(jnp.bfloat16),
            grad_down_local.astype(jnp.bfloat16),
        ],
        after=qkv_piece,
    )
    grad_out, grad_up, grad_down = [share.astype(jnp.float32) for share in batch_shares]
    mod_updated = lamb_group(
        [
            (w_mod, mom_mod, var_mod, grad_mod_share, None),
            (b_mod, mom_bias, var_bias, grad_bias_share, None),
        ],
        seq_count,
    )
    qkv_piece = halving_sum(qkv_piece, "z", lax.axis_size("z"))
    qkv_other = lax.ppermute(qkv_piece, "core", [(0, 1), (1, 0)])
    qkv_first = lax.axis_index("core") == 0
    grad_qkv = jnp.concatenate(
        [jnp.where(qkv_first, qkv_piece, qkv_other), jnp.where(qkv_first, qkv_other, qkv_piece)],
        axis=1,
    ).astype(jnp.float32)
    updated = (
        lamb_group(
            [
                (w_qkv, mom_qkv, var_qkv, grad_qkv, (1, 2)),
                (w_out, mom_out, var_out, grad_out, None),
                (w_up, mom_up, var_up, grad_up, None),
                (w_down, mom_down, var_down, grad_down, None),
            ],
            seq_count,
        )
        + mod_updated
    )
    totals = (grad_qkv, grad_out, grad_up, grad_down, grad_mod_share, grad_bias_share)
    new_masters = [entry[0] for entry in updated]
    new_moments = [entry[1] for entry in updated]
    new_seconds = [entry[2] for entry in updated]
    return (
        result.astype(jnp.bfloat16),
        input_grad,
        time_grad,
        totals[0],
        new_masters[0],
        new_moments[0],
        new_seconds[0],
        totals[1],
        new_masters[1],
        new_moments[1],
        new_seconds[1],
        totals[2],
        new_masters[2],
        new_moments[2],
        new_seconds[2],
        totals[3],
        new_masters[3],
        new_moments[3],
        new_seconds[3],
        totals[4],
        new_masters[4],
        new_moments[4],
        new_seconds[4],
        totals[5],
        new_masters[5],
        new_moments[5],
        new_seconds[5],
    )


def solution(mesh):
    devices = mesh.devices
    chip_mesh = Mesh(
        devices.reshape(devices.shape[0] // 2, 2, devices.shape[1]), ("z", "core", "seq")
    )
    return jax.shard_map(
        local,
        mesh=chip_mesh,
        in_specs=(
            P(("z", "core", "seq"), None),
            P(("z", "core", "seq"), None),
            P(("z", "core"), None),
            P(("z", "core"), None),
            P(("z", "core"), None),
            P(None, "seq", None),
            P(None, "seq", None),
            P(None, "seq", None),
            P("seq", None),
            P("seq", None),
            P("seq", None),
            P("seq", None),
            P("seq", None),
            P("seq", None),
            P("seq", None),
            P("seq", None),
            P("seq", None),
            P("seq", None),
            P("seq", None),
            P("seq", None),
            P("seq"),
            P("seq"),
            P("seq"),
        ),
        out_specs=(
            P(("z", "core", "seq"), None),
            P(("z", "core", "seq"), None),
            P(("z", "core"), None),
            P(None, "seq", None),
            P(None, "seq", None),
            P(None, "seq", None),
            P(None, "seq", None),
            P("seq", None),
            P("seq", None),
            P("seq", None),
            P("seq", None),
            P("seq", None),
            P("seq", None),
            P("seq", None),
            P("seq", None),
            P("seq", None),
            P("seq", None),
            P("seq", None),
            P("seq", None),
            P("seq", None),
            P("seq", None),
            P("seq", None),
            P("seq", None),
            P("seq"),
            P("seq"),
            P("seq"),
            P("seq"),
        ),
        check_vma=False,
    )
```

```python
import jax
import jax.numpy as jnp
from jax import lax
from jax.sharding import Mesh, PartitionSpec as P


HEAD_DIM = 64


precise = lax.Precision.HIGHEST
norm_eps = 1e-06
masked_score = -1e30
beta_one = 0.9
beta_two = 0.999
adam_eps = 1e-08
weight_decay = 0.01
step_rate = 1.0
step_count = 10


def layer_norm(values):
    center = values - jnp.mean(values, axis=-1, keepdims=True)
    spread = jnp.mean(center * center, axis=-1, keepdims=True)
    return center * lax.rsqrt(spread + norm_eps)


def modulate(values, shift, scale):
    return layer_norm(values) * (1.0 + scale) + shift


def gelu_tanh(values):
    return jax.nn.gelu(values, approximate=True)


def rotate(values, places, turn_sign):
    frame_count = values.shape[0]
    half_dim = HEAD_DIM // 2
    exponent = jnp.arange(half_dim, dtype=jnp.float32) * (-2.0 / HEAD_DIM)
    frequency = jnp.power(jnp.float32(10000.0), exponent)
    angles = places.astype(jnp.float32)[:, None] * frequency[None, :]
    cos_table = jnp.cos(angles)[:, None, :]
    sin_table = turn_sign * jnp.sin(angles)[:, None, :]
    paired = values.reshape(frame_count, values.shape[1] // HEAD_DIM, half_dim, 2)
    even_part = paired[..., 0]
    odd_part = paired[..., 1]
    turned = jnp.stack(
        [
            even_part * cos_table - odd_part * sin_table,
            odd_part * cos_table + even_part * sin_table,
        ],
        axis=-1,
    )
    return turned.reshape(frame_count, values.shape[1])


def clip_tables(lengths, padding, frame_ids):
    starts = jnp.cumsum(lengths) - lengths
    finish = starts + lengths
    inside = (frame_ids[:, None] >= starts[None, :]) & (frame_ids[:, None] < finish[None, :])
    clip_ids = jnp.arange(lengths.shape[0], dtype=jnp.int32)
    owners = jnp.sum(jnp.where(inside, clip_ids[None, :], 0), axis=1)
    begins = jnp.sum(jnp.where(inside, starts[None, :], 0), axis=1)
    kept_len = jnp.maximum(lengths - padding, 1)
    limits = jnp.sum(jnp.where(inside, kept_len[None, :], 0), axis=1)
    places = frame_ids - begins
    return (inside.astype(jnp.float32), owners, places, places < limits)


def key_window(block_index, block_rows, span, frame_count):
    return jnp.clip(block_index * block_rows - (span - block_rows) // 2, 0, frame_count - span)


def block_inputs(queries, keys_all, values, owners, usable, block_index, block_rows, span):
    frame_count, columns = queries.shape
    heads_here = columns // HEAD_DIM
    row_start = block_index * block_rows
    window = key_window(block_index, block_rows, span, frame_count)
    query_rows = lax.dynamic_slice_in_dim(queries, row_start, block_rows, 0).reshape(
        block_rows, heads_here, HEAD_DIM
    )
    keys_win = keys_all.reshape(span, heads_here, HEAD_DIM)
    values_win = values.reshape(span, heads_here, HEAD_DIM)
    query_owner = lax.dynamic_slice_in_dim(owners, row_start, block_rows, 0)
    score_scale = HEAD_DIM ** (-0.5)
    scores = (
        jnp.einsum("qhd,khd->hqk", query_rows, keys_win, preferred_element_type=jnp.float32)
        * score_scale
    )
    allowed = (query_owner[:, None] == owners[None, :]) & usable[None, :]
    masked = jnp.where(allowed[None], scores, masked_score)
    return (row_start, window, query_rows, keys_win, values_win, masked)


def attend_forward(queries, keys_all, values, owners, usable, span):
    frame_count, columns = queries.shape
    block_rows = min(512, frame_count)

    def one_block(block_index):
        _, _, _, _, values_win, masked = block_inputs(
            queries, keys_all, values, owners, usable, block_index, block_rows, span
        )
        row_max = jnp.max(masked, axis=-1, keepdims=True)
        row_total = jnp.sum(jnp.exp(masked - row_max), axis=-1, keepdims=True)
        log_total = row_max + jnp.log(row_total)
        probs_low = jnp.exp(masked - log_total).astype(jnp.bfloat16)
        attended = jnp.einsum(
            "hqk,khd->qhd", probs_low, values_win, preferred_element_type=jnp.float32
        )
        return (attended.astype(jnp.bfloat16).reshape(block_rows, columns), log_total)

    outcome, log_totals = lax.map(one_block, jnp.arange(frame_count // block_rows, dtype=jnp.int32))
    return (outcome.reshape(frame_count, columns), log_totals)


def attend_backward(queries, keys_all, values, grad_attended, log_totals, owners, usable, span):
    frame_count, columns = queries.shape
    heads_here = columns // HEAD_DIM
    block_rows = min(512, frame_count)
    score_scale = HEAD_DIM ** (-0.5)

    def one_block(sums, block_data):
        key_sum, value_sum = sums
        block_index, log_total = block_data
        row_start, _, query_rows, keys_win, values_win, masked = block_inputs(
            queries, keys_all, values, owners, usable, block_index, block_rows, span
        )
        grad_rows = lax.dynamic_slice_in_dim(grad_attended, row_start, block_rows, 0).reshape(
            block_rows, heads_here, HEAD_DIM
        )
        probs_full = jnp.exp(masked - log_total)
        probs_low = probs_full.astype(jnp.bfloat16)
        grad_probs = jnp.einsum(
            "qhd,khd->hqk", grad_rows, values_win, preferred_element_type=jnp.float32
        )
        row_delta = jnp.sum(probs_full * grad_probs, axis=-1, keepdims=True)
        grad_scores = (probs_full * (grad_probs - row_delta)).astype(jnp.bfloat16)
        grad_query = (
            jnp.einsum("hqk,khd->qhd", grad_scores, keys_win, preferred_element_type=jnp.float32)
            * score_scale
        )
        grad_key = (
            jnp.einsum("hqk,qhd->khd", grad_scores, query_rows, preferred_element_type=jnp.float32)
            * score_scale
        )
        grad_value = jnp.einsum(
            "hqk,qhd->khd", probs_low, grad_rows, preferred_element_type=jnp.float32
        )
        old_keys = key_sum
        key_sum = old_keys + grad_key.reshape(span, columns)
        old_values = value_sum
        value_sum = old_values + grad_value.reshape(span, columns)
        return ((key_sum, value_sum), grad_query.astype(jnp.bfloat16).reshape(block_rows, columns))

    zeros = jnp.zeros((frame_count, columns), jnp.float32)
    indices = jnp.arange(frame_count // block_rows, dtype=jnp.int32)
    (key_sum, value_sum), grad_queries = lax.scan(one_block, (zeros, zeros), (indices, log_totals))
    return (
        grad_queries.reshape(frame_count, columns),
        key_sum.astype(jnp.bfloat16),
        value_sum.astype(jnp.bfloat16),
    )


def butterfly_sum(values, axes, size):
    step = 1
    while step < size:
        values = values + lax.ppermute(values, axes, [(i, i ^ step) for i in range(size)])
        step *= 2
    return values


def doubling_gather(values, axes, size, index):
    blocks = values[None]
    step = 1
    while step < size:
        other = lax.ppermute(blocks, axes, [(i, i ^ step) for i in range(size)])
        low_side = (index // step) % 2 == 0
        blocks = jnp.concatenate(
            [jnp.where(low_side, blocks, other), jnp.where(low_side, other, blocks)], axis=0
        )
        step *= 2
    return blocks


def gather_rows(shard, row_axis):
    half = shard.shape[row_axis] // 2
    core = lax.axis_index("core")
    piece = lax.dynamic_slice_in_dim(shard, core * half, half, row_axis)
    return lax.all_gather(piece, ("seq", "core"), axis=row_axis, tiled=True)


def halving_sum(values, axis_name, size):
    index = lax.axis_index(axis_name)
    total = values.astype(jnp.float32)
    step = 1
    while step < size:
        half = total.shape[-1] // 2
        low_side = (index // step) % 2 == 0
        keep = jnp.where(low_side, total[..., :half], total[..., half:])
        send = jnp.where(low_side, total[..., half:], total[..., :half]).astype(jnp.bfloat16)
        total = keep + lax.ppermute(send, axis_name, [(i, i ^ step) for i in range(size)]).astype(
            jnp.float32
        )
        step *= 2
    blocks = total.astype(jnp.bfloat16)
    step = size // 2
    while step >= 1:
        other = lax.ppermute(blocks, axis_name, [(i, i ^ step) for i in range(size)])
        low_side = (index // step) % 2 == 0
        blocks = jnp.concatenate(
            [jnp.where(low_side, blocks, other), jnp.where(low_side, other, blocks)], axis=-1
        )
        step //= 2
    return blocks


def gather_batch(shards):
    core = lax.axis_index("core")
    base = min(shard.shape[1] for shard in shards)
    pieces = []
    for shard in shards:
        half = shard.shape[0] // 2
        piece = lax.dynamic_slice_in_dim(shard, core * half, half, 0)
        pieces.append(piece.reshape(-1, base))
    blocks = lax.all_gather(jnp.concatenate(pieces, axis=0), ("seq", "core"), axis=0, tiled=False)
    fulls = []
    offset = 0
    for shard, piece in zip(shards, pieces):
        rows = piece.shape[0]
        fulls.append(blocks[:, offset : offset + rows].reshape(-1, shard.shape[1]))
        offset += rows
    return fulls


def reduce_batch(partials, after=None):
    groups = lax.axis_size("seq") * 2
    base = min(part.shape[1] for part in partials)
    views = [part.reshape(groups, -1, base) for part in partials]
    flat = jnp.concatenate(views, axis=1)
    piece = lax.psum_scatter(flat, ("seq", "core"), scatter_dimension=0, tiled=True)[0]
    if after is not None:
        piece, after = lax.optimization_barrier((piece, after))
    piece = lax.psum(piece, "z")
    other = lax.ppermute(piece, "core", [(0, 1), (1, 0)])
    first = lax.axis_index("core") == 0
    shares = []
    offset = 0
    for part, view in zip(partials, views):
        rows = view.shape[1]
        shape = (-1, part.shape[1])
        mine = piece[offset : offset + rows].reshape(shape)
        theirs = other[offset : offset + rows].reshape(shape)
        shares.append(
            jnp.where(
                first,
                jnp.concatenate([mine, theirs], axis=0),
                jnp.concatenate([theirs, mine], axis=0),
            )
        )
        offset += rows
    return shares


def lamb_group(entries, seq_count):
    steps = []
    flat = []
    for weight, moment, second, grad, sum_axes in entries:
        moment_new, second_new, direction = adam_direction(weight, moment, second, grad)
        weight_sq = jnp.sum(weight * weight, axis=sum_axes, keepdims=True)
        update_sq = jnp.sum(direction * direction, axis=sum_axes, keepdims=True)
        steps.append((weight, moment_new, second_new, direction, weight_sq.shape))
        flat += [weight_sq.reshape(-1), update_sq.reshape(-1)]
    sums = butterfly_sum(jnp.concatenate(flat), "seq", seq_count)
    results = []
    offset = 0
    for weight, moment_new, second_new, direction, shape in steps:
        count = flat[len(results) * 2].size
        weight_sq = sums[offset : offset + count].reshape(shape)
        update_sq = sums[offset + count : offset + 2 * count].reshape(shape)
        offset += 2 * count
        ratio = jnp.sqrt(weight_sq) * lax.rsqrt(update_sq + 1e-06)
        results.append((weight - step_rate * ratio * direction, moment_new, second_new))
    return results


def adam_direction(weight, moment, second, grad):
    moment_new = beta_one * moment + (1.0 - beta_one) * grad
    second_new = beta_two * second + (1.0 - beta_two) * grad * grad
    corrected = moment_new / (1.0 - beta_one**step_count)
    scaled = second_new / (1.0 - beta_two**step_count)
    direction = corrected / (jnp.sqrt(scaled) + adam_eps) + weight_decay * weight
    return (moment_new, second_new, direction)


def local(
    frames,
    out_grad,
    time_emb,
    clip_len,
    pad_len,
    w_qkv,
    mom_qkv,
    var_qkv,
    w_out,
    mom_out,
    var_out,
    w_up,
    mom_up,
    var_up,
    w_down,
    mom_down,
    var_down,
    w_mod,
    mom_mod,
    var_mod,
    b_mod,
    mom_bias,
    var_bias,
):
    seq_count = lax.axis_size("seq")
    seq_rank = lax.axis_index("seq")
    frame_rows = frames.shape[0]
    group_frames = frame_rows * seq_count
    dp_count = lax.axis_size(("z", "core"))
    dp_rank = lax.axis_index(("z", "core"))
    qkv_full = gather_rows(w_qkv.astype(jnp.bfloat16), 1)
    out_full, up_full, down_full = gather_batch(
        [w_out.astype(jnp.bfloat16), w_up.astype(jnp.bfloat16), w_down.astype(jnp.bfloat16)]
    )
    bias_full = doubling_gather(b_mod.astype(jnp.bfloat16), "seq", seq_count, seq_rank).reshape(-1)
    mod_low = w_mod.astype(jnp.bfloat16)
    mod_rows_here = w_mod.shape[0]
    mod_first = seq_rank * mod_rows_here
    inside_all, owners_all, places_all, usable_all = clip_tables(
        clip_len[0], pad_len[0], jnp.arange(group_frames, dtype=jnp.int32)
    )
    row_first = seq_rank * frame_rows
    inside_own = lax.dynamic_slice_in_dim(inside_all, row_first, frame_rows, 0)
    places_own = lax.dynamic_slice_in_dim(places_all, row_first, frame_rows, 0)
    silu_low = jax.nn.silu(time_emb).astype(jnp.bfloat16)
    silu_part = lax.dynamic_slice_in_dim(silu_low, mod_first, mod_rows_here, 1)
    modulation = butterfly_sum(
        jnp.dot(silu_part, mod_low, preferred_element_type=jnp.float32), "seq", seq_count
    ) + bias_full.astype(jnp.float32)
    mod_rows = jnp.dot(inside_own, modulation, precision=precise)
    shift_attn, scale_attn, gate_attn, shift_ff, scale_ff, gate_ff = jnp.split(mod_rows, 6, axis=1)
    inputs = frames.astype(jnp.float32)
    hidden, attn_norm_back = jax.vjp(modulate, inputs, shift_attn, scale_attn)
    hidden_low = hidden.astype(jnp.bfloat16)
    query_lin = jnp.dot(hidden_low, qkv_full[0], preferred_element_type=jnp.float32)
    key_lin = jnp.dot(hidden_low, qkv_full[1], preferred_element_type=jnp.float32)
    value_lin = jnp.dot(hidden_low, qkv_full[2], preferred_element_type=jnp.float32)
    query_send = rotate(query_lin, places_own, 1.0).astype(jnp.bfloat16)
    key_send = rotate(key_lin, places_own, 1.0).astype(jnp.bfloat16)
    value_send = value_lin.astype(jnp.bfloat16)
    query_heads, key_heads, value_heads = (
        lax.all_to_all(query_send, "seq", split_axis=1, concat_axis=0, tiled=True),
        lax.all_to_all(key_send, "seq", split_axis=1, concat_axis=0, tiled=True),
        lax.all_to_all(value_send, "seq", split_axis=1, concat_axis=0, tiled=True),
    )
    attended_heads, log_totals = attend_forward(
        query_heads, key_heads, value_heads, owners_all, usable_all, group_frames
    )
    attended = lax.all_to_all(attended_heads, "seq", split_axis=0, concat_axis=1, tiled=True)
    attn_proj = jnp.dot(attended, out_full, preferred_element_type=jnp.float32)
    mid = inputs + gate_attn * attn_proj
    hidden_ff, ff_norm_back = jax.vjp(modulate, mid, shift_ff, scale_ff)
    hidden_ff_low = hidden_ff.astype(jnp.bfloat16)
    pre_act = jnp.dot(hidden_ff_low, up_full, preferred_element_type=jnp.float32)
    active, gelu_back = jax.vjp(gelu_tanh, pre_act)
    active_low = active.astype(jnp.bfloat16)
    ff_proj = jnp.dot(active_low, down_full, preferred_element_type=jnp.float32)
    result = mid + gate_ff * ff_proj
    grad_result = out_grad.astype(jnp.float32)
    grad_gate_ff = grad_result * ff_proj
    grad_ff = (grad_result * gate_ff).astype(jnp.bfloat16)
    grad_down_local = jnp.einsum(
        "nf,nd->fd", active_low, grad_ff, preferred_element_type=jnp.float32
    )
    grad_active = jnp.einsum("nd,fd->nf", grad_ff, down_full, preferred_element_type=jnp.float32)
    (grad_pre,) = gelu_back(grad_active)
    grad_pre_low = grad_pre.astype(jnp.bfloat16)
    grad_up_local = jnp.einsum(
        "nd,nf->df", hidden_ff_low, grad_pre_low, preferred_element_type=jnp.float32
    )
    grad_hidden_ff = jnp.einsum(
        "nf,df->nd", grad_pre_low, up_full, preferred_element_type=jnp.float32
    )
    grad_mid_norm, grad_shift_ff, grad_scale_ff = ff_norm_back(grad_hidden_ff)
    grad_mid = grad_result + grad_mid_norm
    grad_gate_attn = grad_mid * attn_proj
    grad_proj = (grad_mid * gate_attn).astype(jnp.bfloat16)
    grad_out_local = jnp.einsum(
        "nd,ne->de", attended, grad_proj, preferred_element_type=jnp.float32
    )
    grad_attended = jnp.einsum(
        "ne,de->nd", grad_proj, out_full, preferred_element_type=jnp.float32
    ).astype(jnp.bfloat16)
    grad_heads = lax.all_to_all(grad_attended, "seq", split_axis=1, concat_axis=0, tiled=True)
    grad_heads, grad_out_local, grad_up_local, grad_down_local = lax.optimization_barrier(
        (grad_heads, grad_out_local, grad_up_local, grad_down_local)
    )
    grad_query_heads, grad_key_heads, grad_value_heads = attend_backward(
        query_heads,
        key_heads,
        value_heads,
        grad_heads,
        log_totals,
        owners_all,
        usable_all,
        group_frames,
    )
    grad_query_rows, grad_key_rows, grad_value_rows = (
        lax.all_to_all(grad_query_heads, "seq", split_axis=0, concat_axis=1, tiled=True),
        lax.all_to_all(grad_key_heads, "seq", split_axis=0, concat_axis=1, tiled=True),
        lax.all_to_all(grad_value_heads, "seq", split_axis=0, concat_axis=1, tiled=True),
    )
    grad_query_lin = rotate(grad_query_rows.astype(jnp.float32), places_own, -1.0).astype(
        jnp.bfloat16
    )
    grad_key_lin = rotate(grad_key_rows.astype(jnp.float32), places_own, -1.0).astype(jnp.bfloat16)
    grad_qkv_local = jnp.stack(
        [
            jnp.einsum("nd,ne->de", hidden_low, grad_query_lin, preferred_element_type=jnp.float32),
            jnp.einsum("nd,ne->de", hidden_low, grad_key_lin, preferred_element_type=jnp.float32),
            jnp.einsum(
                "nd,ne->de", hidden_low, grad_value_rows, preferred_element_type=jnp.float32
            ),
        ]
    )
    grad_hidden = jnp.einsum(
        "ne,de->nd", grad_query_lin, qkv_full[0], preferred_element_type=jnp.float32
    )
    grad_hidden = grad_hidden + jnp.einsum(
        "ne,de->nd", grad_key_lin, qkv_full[1], preferred_element_type=jnp.float32
    )
    grad_hidden = grad_hidden + jnp.einsum(
        "ne,de->nd", grad_value_rows, qkv_full[2], preferred_element_type=jnp.float32
    )
    grad_input_norm, grad_shift_attn, grad_scale_attn = attn_norm_back(grad_hidden)
    input_grad = grad_mid + grad_input_norm
    grad_mod_rows = jnp.concatenate(
        [
            grad_shift_attn,
            grad_scale_attn,
            grad_gate_attn,
            grad_shift_ff,
            grad_scale_ff,
            grad_gate_ff,
        ],
        axis=1,
    )
    grad_mod_clip = butterfly_sum(
        jnp.einsum("nc,ne->ce", inside_own, grad_mod_rows, precision=precise), "seq", seq_count
    )
    grad_mod_all = doubling_gather(grad_mod_clip, ("z", "core"), dp_count, dp_rank).reshape(
        -1, grad_mod_clip.shape[1]
    )
    silu_all = doubling_gather(silu_part, ("z", "core"), dp_count, dp_rank).reshape(
        -1, silu_part.shape[1]
    )
    bias_cols = b_mod.shape[0]
    grad_bias_share = jnp.sum(
        lax.dynamic_slice_in_dim(grad_mod_all, seq_rank * bias_cols, bias_cols, 1), axis=0
    )
    grad_mod_share = jnp.einsum(
        "cd,ce->de", silu_all.astype(jnp.float32), grad_mod_all, precision=precise
    )
    grad_silu_part = jnp.einsum(
        "ce,de->cd", grad_mod_clip, mod_low.astype(jnp.float32), precision=precise
    )
    grad_silu = jnp.concatenate(
        list(doubling_gather(grad_silu_part, "seq", seq_count, seq_rank)), axis=1
    )
    time_grad = jax.vjp(jax.nn.silu, time_emb)[1](grad_silu)[0]
    qkv_piece = lax.psum_scatter(
        grad_qkv_local.astype(jnp.bfloat16), ("seq", "core"), scatter_dimension=1, tiled=True
    )
    batch_shares = reduce_batch(
        [
            grad_out_local.astype(jnp.bfloat16),
            grad_up_local.astype(jnp.bfloat16),
            grad_down_local.astype(jnp.bfloat16),
        ],
        after=qkv_piece,
    )
    grad_out, grad_up, grad_down = [share.astype(jnp.float32) for share in batch_shares]
    updated = lamb_group(
        [
            (w_out, mom_out, var_out, grad_out, None),
            (w_up, mom_up, var_up, grad_up, None),
            (w_down, mom_down, var_down, grad_down, None),
        ],
        seq_count,
    )
    updated += lamb_group(
        [
            (w_mod, mom_mod, var_mod, grad_mod_share, None),
            (b_mod, mom_bias, var_bias, grad_bias_share, None),
        ],
        seq_count,
    )
    qkv_piece = halving_sum(qkv_piece, "z", lax.axis_size("z"))
    qkv_other = lax.ppermute(qkv_piece, "core", [(0, 1), (1, 0)])
    qkv_first = lax.axis_index("core") == 0
    grad_qkv = jnp.concatenate(
        [jnp.where(qkv_first, qkv_piece, qkv_other), jnp.where(qkv_first, qkv_other, qkv_piece)],
        axis=1,
    ).astype(jnp.float32)
    updated = lamb_group([(w_qkv, mom_qkv, var_qkv, grad_qkv, (1, 2))], seq_count) + updated
    totals = (grad_qkv, grad_out, grad_up, grad_down, grad_mod_share, grad_bias_share)
    new_masters = [entry[0] for entry in updated]
    new_moments = [entry[1] for entry in updated]
    new_seconds = [entry[2] for entry in updated]
    return (
        result.astype(jnp.bfloat16),
        input_grad,
        time_grad,
        totals[0],
        new_masters[0],
        new_moments[0],
        new_seconds[0],
        totals[1],
        new_masters[1],
        new_moments[1],
        new_seconds[1],
        totals[2],
        new_masters[2],
        new_moments[2],
        new_seconds[2],
        totals[3],
        new_masters[3],
        new_moments[3],
        new_seconds[3],
        totals[4],
        new_masters[4],
        new_moments[4],
        new_seconds[4],
        totals[5],
        new_masters[5],
        new_moments[5],
        new_seconds[5],
    )


def solution(mesh):
    devices = mesh.devices
    chip_mesh = Mesh(
        devices.reshape(devices.shape[0] // 2, 2, devices.shape[1]), ("z", "core", "seq")
    )
    return jax.shard_map(
        local,
        mesh=chip_mesh,
        in_specs=(
            P(("z", "core", "seq"), None),
            P(("z", "core", "seq"), None),
            P(("z", "core"), None),
            P(("z", "core"), None),
            P(("z", "core"), None),
            P(None, "seq", None),
            P(None, "seq", None),
            P(None, "seq", None),
            P("seq", None),
            P("seq", None),
            P("seq", None),
            P("seq", None),
            P("seq", None),
            P("seq", None),
            P("seq", None),
            P("seq", None),
            P("seq", None),
            P("seq", None),
            P("seq", None),
            P("seq", None),
            P("seq"),
            P("seq"),
            P("seq"),
        ),
        out_specs=(
            P(("z", "core", "seq"), None),
            P(("z", "core", "seq"), None),
            P(("z", "core"), None),
            P(None, "seq", None),
            P(None, "seq", None),
            P(None, "seq", None),
            P(None, "seq", None),
            P("seq", None),
            P("seq", None),
            P("seq", None),
            P("seq", None),
            P("seq", None),
            P("seq", None),
            P("seq", None),
            P("seq", None),
            P("seq", None),
            P("seq", None),
            P("seq", None),
            P("seq", None),
            P("seq", None),
            P("seq", None),
            P("seq", None),
            P("seq", None),
            P("seq"),
            P("seq"),
            P("seq"),
            P("seq"),
        ),
        check_vma=False,
    )
```
